1024 devices in a mesh: dp: 4 (over x), cp: 16 (over z), tensor: 16 (over y, core).
Axes of the slice: x: 4, y: 8, z: 16, core: 2. Of those that a mesh axis runs over, the one named last changes fastest.
Arguments:
- x_in: bfloat16 [8192, 16384], P('tensor', ('dp', 'cp')), parts along dimension 1, may hold values from -6 to 6
- z_gate: bfloat16 [8192, 16384], P('tensor', ('dp', 'cp')), parts along dimension 1, may hold values from -6 to 6
- bc_in: bfloat16 [8, 256, 16384], P(None, None, ('dp', 'cp')), parts along dimension 2, may hold values from -6 to 6
- dt_raw: bfloat16 [128, 16384], P('tensor', ('dp', 'cp')), parts along dimension 1, may hold values from -3 to 13
- conv_x_w: float32 [8192, 4], P('tensor'), may hold values from -3 to 3
- conv_x_b: float32 [8192], P('tensor'), may hold values from -1.7 to 0.3
- conv_bc_w: float32 [8, 256, 4], replicated, may hold values from -3 to 3
- conv_bc_b: float32 [8, 256], replicated, may hold values from -1.7 to 0.3
- dt_bias: float32 [128], P('tensor'), may hold values from -10 to -1.5
- a_log: float32 [128], P('tensor'), may hold values from -4.6 to -2
- d_skip: float32 [128], P('tensor'), may hold values from 0.5 to 2
Outputs:
- y_out: bfloat16 [8192, 16384], P('tensor', ('dp', 'cp')), parts along dimension 1
The draws below stay inside these ranges and needn't reach their ends.
There are 4 independent parts, one for each index of `dp`. The reference program is written for one: setup_inputs(seed, part) draws one part's arguments, and reference() takes and returns one part's arrays. A program takes and returns all parts, laid end to end along the dimension named above; an argument that names none is the same for every part. Nothing has to cross between parts.
All inputs are finite; a program needn't handle non-finite values.
Results may differ from the reference program's by a relative error of at most 0.0085.
Values may be sent and summed in bfloat16 or wider, within the bound.
No kernel may reach another device: no remote copies, remote signals or barrier semaphores. Data moves between devices by JAX's collectives and lax.ppermute only.
A program may use at most 32 MiB of HBM per device.

```python
import math
import jax
import jax.numpy as jnp
from jax import lax

HEADS = 128
HEAD_DIM = 64
STATE = 128
GROUPS = 8
KERNEL = 4
BLOCK = 256
SEQUENCE_LENGTH = 4096
CHANNELS = 8192


lift_share = 0.1875


raise_elevation = 3.8


surge_start = 1.4


def head_law(key):
    base_key = jax.random.fold_in(key, 7)
    subkeys = jax.random.split(base_key, 4)
    slow_share = 0.5
    nodes = jnp.array([-0.866, 0.0, 0.866], jnp.float32)
    node_weights = jnp.array([1.0 / 6.0, 2.0 / 3.0, 1.0 / 6.0], jnp.float32)
    is_slow = jax.random.uniform(subkeys[0], (HEADS,)) < slow_share
    spread = jax.random.uniform(subkeys[1], (HEADS,), minval=-0.2, maxval=0.2)
    slow_rate = jax.random.uniform(subkeys[2], (HEADS,), minval=0.4, maxval=0.8) / SEQUENCE_LENGTH
    fast_rate = jax.random.uniform(subkeys[3], (HEADS,), minval=1.0 / 50, maxval=1.0 / 30)
    start_delta = jnp.where(is_slow, 2.0 / SEQUENCE_LENGTH * jnp.exp(spread), 0.1 * jnp.exp(2.5 * spread))
    decay_rate = jnp.where(is_slow, slow_rate, fast_rate)
    base_raw = jnp.log(jnp.expm1(start_delta))
    drawn_mean = jnp.sum(jax.nn.softplus(base_raw[:, None] + nodes[None, :]) * node_weights[None, :], axis=1)
    lifted_mean = jnp.sum(jax.nn.softplus(base_raw[:, None] + raise_elevation + nodes[None, :]) * node_weights[None, :], axis=1)
    mean_delta = (1.0 - lift_share) * drawn_mean + lift_share * lifted_mean
    return (start_delta, decay_rate / mean_delta)


def draw_dt_bias(key, part):
    start_delta, magnitude = head_law(key)
    return jnp.log(jnp.expm1(start_delta)).astype(jnp.float32)


def draw_a_log(key, part):
    start_delta, magnitude = head_law(key)
    return jnp.log(magnitude).astype(jnp.float32)


def draw_dt_raw(key, part):
    jitter_key, lift_key, place_key, elevation_key = jax.random.split(jax.random.fold_in(key, 3), 4)
    jitter = jnp.clip(0.5 * jax.random.normal(jitter_key, (HEADS, SEQUENCE_LENGTH)), -2.5, 2.5)
    raised_values = jax.random.uniform(lift_key, (HEADS, SEQUENCE_LENGTH)) < lift_share
    stretch_width = max(1, BLOCK // 8)
    places = jax.random.randint(place_key, (3,), 0, SEQUENCE_LENGTH - stretch_width + 1)
    elevation_values = jnp.log(SEQUENCE_LENGTH / stretch_width) + surge_start + jax.random.uniform(elevation_key, (3,), minval=-0.3, maxval=0.3)
    positions = jnp.arange(SEQUENCE_LENGTH)
    contained_flag = (positions[None, :] >= places[:, None]) & (positions[None, :] < places[:, None] + stretch_width)
    surge_spans = jnp.max(jnp.where(contained_flag, elevation_values[:, None], 0.0), axis=0)
    within_surge = jnp.any(contained_flag, axis=0)
    raise_amount = jnp.where(within_surge[None, :], surge_spans[None, :], jnp.where(raised_values, raise_elevation, 0.0))
    return (jitter + raise_amount).astype(jnp.bfloat16)


def levels(stream_key, extent, shards, smallest, top_value):
    def one(axis_at, blocks):
        steps = jax.random.uniform(jax.random.fold_in(jax.random.fold_in(stream_key, 6), axis_at), (blocks,), jnp.float32, smallest / len(shards), top_value / len(shards))
        return jnp.repeat(jnp.exp(steps), extent[axis_at] // blocks).reshape((-1,) + (1,) * (len(extent) - axis_at - 1))

    level = one(*shards[0])
    for cut in shards[1:]:
        level = level * one(*cut)
    return level


def centred(rng, extent, scale, most, cuts=(), dtype=jnp.bfloat16):
    level = levels(rng, extent, cuts, -0.22, 0.18) if cuts else 1.0
    values = jax.random.normal(rng, extent, jnp.float32) * scale * level
    return jnp.minimum(jnp.maximum(values, -most), most).astype(dtype)


def setup_inputs(seed: int = 0, part: int = 0) -> dict:
    key_of = jax.random.split(jax.random.key(seed), 12)
    own_keys = jax.random.split(jax.random.fold_in(key_of[11], part), 12)
    return {
        "x_in": centred(own_keys[0], (CHANNELS, SEQUENCE_LENGTH), 1.0, 6.0, ((0, 16), (1, 16))),
        "z_gate": centred(own_keys[1], (CHANNELS, SEQUENCE_LENGTH), 1.0, 6.0, ((0, 16), (1, 16))),
        "bc_in": centred(own_keys[2], (GROUPS, 2 * STATE, SEQUENCE_LENGTH), 1.0, 6.0, ((2, 16),)),
        "dt_raw": draw_dt_raw(jax.random.fold_in(jax.random.fold_in(key_of[11], part), 71), part),
        "conv_x_w": centred(key_of[4], (CHANNELS, KERNEL), KERNEL ** -0.5, 3.0, ((0, 16),), jnp.float32),
        "conv_x_b": jnp.clip(-1.7 + 2 * jax.random.uniform(key_of[5], (CHANNELS,), jnp.float32) ** levels(key_of[5], (CHANNELS,), ((0, 16),), -0.2, 0.2), -1.7, 0.3),
        "conv_bc_w": centred(key_of[6], (GROUPS, 2 * STATE, KERNEL), KERNEL ** -0.5, 3.0, (), jnp.float32),
        "conv_bc_b": jnp.clip(jax.random.uniform(key_of[7], (GROUPS, 2 * STATE), jnp.float32, -1.7, 0.3), -1.7, 0.3),
        "dt_bias": draw_dt_bias(jax.random.fold_in(key_of[11], 71), part),
        "a_log": draw_a_log(jax.random.fold_in(key_of[11], 71), part),
        "d_skip": jnp.clip(jnp.exp(math.log(2.0) - 1.3862944 * jax.random.uniform(key_of[10], (HEADS,), jnp.float32) ** levels(key_of[10], (HEADS,), ((0, 16),), -0.2, 0.2)), 0.5, 2.0),
    }


def causal_filter(series, taps, offsets):
    kernel_size = taps.shape[-1]
    length = series.shape[-1]
    history = jnp.zeros(series.shape[:-1] + (kernel_size - 1,), jnp.float32)
    padded = jnp.concatenate([history, series], axis=-1)
    summed = jnp.broadcast_to(offsets[..., None], series.shape)
    for tap_index in range(kernel_size):
        summed = summed + taps[..., tap_index:tap_index + 1] * padded[..., tap_index:tap_index + length]
    return jax.nn.silu(summed)


def group_output(x_values, step_size, rates, skip, b_rows, c_rows):
    unit_count, channels, length = x_values.shape
    state_dim = b_rows.shape[0]
    nblocks = length // BLOCK
    cumulative = jnp.cumsum((step_size * rates[:, None]).reshape(unit_count, nblocks, BLOCK), axis=2)
    block_ends = cumulative[:, :, BLOCK - 1]
    input_gain = step_size.reshape(unit_count, nblocks, BLOCK) * jnp.exp(block_ends[:, :, None] - cumulative)
    x_wide = x_values.astype(jnp.float32)
    weighted = (x_wide.reshape(unit_count, channels, nblocks, BLOCK) * input_gain[:, None]).astype(jnp.bfloat16)
    b_wide = b_rows.astype(jnp.float32).reshape(state_dim, nblocks, BLOCK)
    c_wide = c_rows.astype(jnp.float32).reshape(state_dim, nblocks, BLOCK)
    fresh = jnp.einsum("ucbs,nbs->ubcn", weighted.astype(jnp.float32), b_wide)

    def advance(carried, inputs):
        decay, new_state = inputs
        return jnp.exp(decay)[:, None, None] * carried + new_state, carried

    unused, entering = lax.scan(advance, jnp.zeros((unit_count, channels, state_dim), jnp.float32),
                                (block_ends.T, jnp.moveaxis(fresh, 1, 0)))
    rounded = lax.optimization_barrier(entering.astype(jnp.bfloat16)).astype(jnp.float32)
    from_state = jnp.einsum("bucn,nbt->ucbt", rounded, c_wide) * jnp.exp(cumulative)[:, None]

    step_blocks = math.gcd(nblocks, max(1, 1024 // BLOCK))
    rows_step = step_blocks * BLOCK
    causal = lax.broadcasted_iota(jnp.int32, (BLOCK, BLOCK), 0) >= lax.broadcasted_iota(jnp.int32, (BLOCK, BLOCK), 1)

    def one_step(index, result):
        index = jnp.asarray(index).astype(jnp.int32)
        start = index * rows_step
        x_part = lax.dynamic_slice_in_dim(x_wide, start, rows_step, 2).reshape(unit_count, channels, step_blocks, BLOCK)
        d_part = lax.dynamic_slice_in_dim(step_size, start, rows_step, 1).reshape(unit_count, step_blocks, BLOCK)
        cum_part = lax.dynamic_slice_in_dim(cumulative, index * step_blocks, step_blocks, 1)
        b_part = lax.dynamic_slice_in_dim(b_wide, index * step_blocks, step_blocks, 1)
        c_part = lax.dynamic_slice_in_dim(c_wide, index * step_blocks, step_blocks, 1)
        gram = jnp.einsum("nbt,nbs->bts", c_part, b_part)
        spread = cum_part[:, :, :, None] - cum_part[:, :, None, :]
        decayed = jnp.where(causal, jnp.exp(jnp.where(causal, spread, 0.0)), 0.0)
        mixing = (gram[None] * decayed * d_part[:, :, None, :]).astype(jnp.bfloat16)
        mixing = lax.optimization_barrier(mixing).astype(jnp.float32)
        y_part = jnp.einsum("ucbs,ubts->ucbt", x_part, mixing)
        return lax.dynamic_update_slice_in_dim(result, y_part.reshape(unit_count, channels, rows_step), start, 2)

    intra = lax.fori_loop(0, nblocks // step_blocks, one_step,
                          jnp.zeros((unit_count, channels, length), jnp.float32))
    summed = intra + from_state.reshape(unit_count, channels, length) + skip[:, None, None] * x_wide
    return summed.astype(jnp.bfloat16)


def reference(x_in, z_gate, bc_in, dt_raw, conv_x_w, conv_x_b, conv_bc_w, conv_bc_b, dt_bias, a_log, d_skip):
    length = x_in.shape[1]
    group_heads = HEADS // GROUPS
    x_conv = causal_filter(x_in.astype(jnp.float32), conv_x_w, conv_x_b).astype(jnp.bfloat16)
    bc_conv = causal_filter(bc_in.astype(jnp.float32), conv_bc_w, conv_bc_b).astype(jnp.bfloat16)
    step_size = jax.nn.softplus(dt_raw.astype(jnp.float32) + dt_bias[:, None])
    rates = -jnp.exp(a_log)

    def group_work(operands):
        x_group, d_group, r_group, s_group, bc_group = operands
        return group_output(x_group.reshape(group_heads, HEAD_DIM, length), d_group, r_group, s_group,
                            bc_group[:STATE], bc_group[STATE:])

    mixed_out = lax.map(group_work, (x_conv.reshape(GROUPS, group_heads * HEAD_DIM, length),
                                     step_size.reshape(GROUPS, group_heads, length),
                                     rates.reshape(GROUPS, group_heads),
                                     d_skip.reshape(GROUPS, group_heads), bc_conv))
    mixed_out = lax.optimization_barrier(mixed_out.reshape(HEADS * HEAD_DIM, length))
    return (mixed_out.astype(jnp.float32) * jax.nn.silu(z_gate.astype(jnp.float32))).astype(jnp.bfloat16)
```

```python
import jax
import jax.numpy as jnp
from jax import lax
from jax.experimental import pallas as pl
from jax.experimental.pallas import tpu as pltpu
from jax.sharding import Mesh, PartitionSpec as P

HEADS = 128
GROUPS = 8
GROUP_HEADS = HEADS // GROUPS
LO = 4
META = 16

F32 = jnp.float32
BF16 = jnp.bfloat16


def dot(a, b, ca, cb):
    return lax.dot_general(a, b, (((ca,), (cb,)), ((), ())), preferred_element_type=F32)


def silu(v):
    return v / (1.0 + jnp.exp(-v))


def log1p(u):
    return jnp.where(u < 1e-3, u * (1.0 - u * (0.5 - u * (1.0 / 3.0))), jnp.log(1.0 + u))


def softplus(v):
    return jnp.maximum(v, 0.0) + log1p(jnp.exp(-jnp.abs(v)))


def tails_kernel(group, x, bc, out):
    rows = lax.broadcasted_iota(jnp.int32, (8, 128), 0)
    lanes = lax.broadcasted_iota(jnp.int32, (8, 128), 1)
    pick = jnp.where(jnp.logical_and(lanes == rows + 125, rows < 3), 1.0, 0.0).astype(BF16)
    channels = x.shape[0]
    out[:, :channels] = dot(pick, x[...], 1, 1).astype(BF16)
    out[:, channels:] = dot(pick, bc[0], 1, 1).astype(BF16)


def filtered(series, rim, taps):
    lanes = lax.broadcasted_iota(jnp.int32, rim.shape, 1)
    first, second = series[:, :128].astype(F32), series[:, 128:].astype(F32)
    a = taps[:, 4:5] + taps[:, 3:4] * first
    b = taps[:, 4:5] + taps[:, 3:4] * second
    for back in (1, 2, 3):
        moved = pltpu.roll(first, back, 1)
        tap = taps[:, 3 - back : 4 - back]
        a = a + tap * jnp.where(lanes < back, pltpu.roll(rim, back, 1), moved)
        b = b + tap * jnp.where(lanes < back, moved, pltpu.roll(second, back, 1))
    return jnp.concatenate([silu(a), silu(b)], axis=1).astype(BF16)


def columns(taps, offsets):
    width = offsets.shape[1]
    rows = jnp.concatenate([taps, offsets, jnp.zeros((3, width), F32)], axis=0)
    return rows.T


def state_kernel(group, x, bc, rims, dt, xw, xb, bw, bb, bias, a_log, pay, xc, bcc, cum_out, delta_out):
    channels = x.shape[0]
    heads = dt.shape[0]
    width = channels // heads
    states = bc.shape[1] // 2
    rows = lax.broadcasted_iota(jnp.int32, (8, 128), 0)
    lanes = lax.broadcasted_iota(jnp.int32, (8, 128), 1)
    place = jnp.where(jnp.logical_and(lanes == rows + 125, rows < 3), 1.0, 0.0).astype(BF16)
    rim = dot(rims[...], place, 0, 0)

    delta = softplus(dt[...].astype(F32) + bias[...])
    delta_out[...] = delta
    scaled = delta * -jnp.exp(a_log[...])
    high = scaled.astype(BF16)
    rest = scaled - high.astype(F32)
    mid = rest.astype(BF16)
    low = (rest - mid.astype(F32)).astype(BF16)
    size = scaled.shape[1]
    upto = jnp.where(
        lax.broadcasted_iota(jnp.int32, (size, size), 0) <= lax.broadcasted_iota(jnp.int32, (size, size), 1), 1.0, 0.0
    ).astype(BF16)
    cum = dot(low, upto, 1, 0) + dot(mid, upto, 1, 0) + dot(high, upto, 1, 0)
    cum_out[...] = cum
    end = cum[:, size - 1 :]
    gain = delta * jnp.exp(end - cum)
    total = jnp.exp(end)
    total_high = total.astype(BF16).astype(F32)
    total_low = (total - total_high).astype(BF16).astype(F32)

    bcc[...] = filtered(bc[0], rim[channels:], columns(bw[0], bb[0]))
    b_rows = bcc[:states, :]
    x_taps = columns(xw[...], xb[...])
    meta = lax.broadcasted_iota(jnp.int32, (META, 128), 0)
    per = heads // LO
    for quarter in range(LO):
        tail = jnp.zeros((META, 128), F32)
        for j in range(per):
            h = quarter * per + j
            at = pl.ds(h * width, width)
            values = filtered(x[at, :], rim[h * width : (h + 1) * width], x_taps[h * width : (h + 1) * width])
            xc[at, :] = values
            weighted = (values.astype(F32) * gain[h : h + 1]).astype(BF16)
            pay[quarter, pl.ds(j * width, width), :] = dot(weighted, b_rows, 1, 1).astype(BF16)
            tail = jnp.where(meta == 2 * j, total_high[h : h + 1], tail)
            tail = jnp.where(meta == 2 * j + 1, total_low[h : h + 1], tail)
        pay[quarter, pl.ds(per * width, META), :] = tail.astype(BF16)


def unpack(block, per):
    size = block.shape[0] - META
    width = size // per
    tail = block[size:].astype(F32)
    decays = jnp.concatenate(
        [jnp.broadcast_to(tail[2 * j : 2 * j + 1] + tail[2 * j + 1 : 2 * j + 2], (width, 128)) for j in range(per)], axis=0
    )
    return block[:size].astype(F32), decays


def group_kernel(got, out, *, per):
    size = out.shape[0] - META
    width = size // per
    state, decay = unpack(got[0], per)
    for r in range(1, LO):
        fresh, d = unpack(got[r], per)
        state = fresh + d * state
        decay = decay * d
    out[:size, :] = state.astype(BF16)
    meta = lax.broadcasted_iota(jnp.int32, (META, 128), 0)
    tail = jnp.zeros((META, 128), F32)
    for j in range(per):
        d = decay[j * width : j * width + 1]
        high = d.astype(BF16).astype(F32)
        tail = jnp.where(meta == 2 * j, high, tail)
        tail = jnp.where(meta == 2 * j + 1, d - high, tail)
    out[size:, :] = tail.astype(BF16)


def entering_kernel(got, near, middle, far, out, *, per):
    last, last_decay = unpack(near[...], per)
    second, second_decay = unpack(middle[...], per)
    third, unused = unpack(far[...], per)
    state = last + last_decay * (second + second_decay * third)
    out[0] = state.astype(BF16)
    for r in range(1, LO):
        fresh, d = unpack(got[r - 1], per)
        state = fresh + d * state
        out[r] = state.astype(BF16)


def intra_kernel(xc, bcc, cum_in, delta, skip, out):
    heads = cum_in.shape[0]
    width = xc.shape[0] // heads
    states = bcc.shape[0] // 2
    cum = cum_in[...]
    less = cum - jnp.log(delta[...])
    less_cols = jnp.concatenate([less[:, :128].T, less[:, 128:].T], axis=0)
    gram = dot(bcc[:states, :], bcc[states:, :], 0, 0)
    keep = lax.broadcasted_iota(jnp.int32, (128, 128), 0) <= lax.broadcasted_iota(jnp.int32, (128, 128), 1)
    for h in range(heads):
        at = pl.ds(h * width, width)
        values = xc[at, :]
        row = cum[h : h + 1]
        col = less_cols[:, h : h + 1]

        def mix(s, t, masked):
            spread = row[:, t : t + 128] - col[s : s + 128]
            if masked:
                spread = jnp.where(keep, spread, -1e30)
            return (gram[s : s + 128, t : t + 128] * jnp.exp(spread)).astype(BF16)

        early = dot(values[:, :128], mix(0, 0, True), 1, 0)
        late = dot(values, jnp.concatenate([mix(0, 128, False), mix(128, 128, True)], axis=0), 1, 0)
        out[at, :] = jnp.concatenate([early, late], axis=1) + skip[h : h + 1] * values.astype(F32)


def output_kernel(inner, bcc, cum, state, z, out):
    heads = cum.shape[0]
    width = inner.shape[0] // heads
    states = bcc.shape[0] // 2
    c_rows = bcc[states:, :]
    grown = jnp.exp(cum[...])
    for h in range(heads):
        at = pl.ds(h * width, width)
        y = inner[at, :] + grown[h : h + 1] * dot(state[at, :], c_rows, 1, 0)
        y = y.astype(BF16).astype(F32)
        out[at, :] = (y * silu(z[at, :].astype(F32))).astype(BF16)


def shape(*dims, dtype=F32):
    return jax.ShapeDtypeStruct(dims, dtype)


def whole(array):
    return pl.BlockSpec(array.shape, lambda i, g: (0,) * array.ndim)


def local(x_in, z_gate, bc_in, dt_raw, conv_x_w, conv_x_b, conv_bc_w, conv_bc_b, dt_bias, a_log, d_skip):
    heads, length = dt_raw.shape
    channels = x_in.shape[0]
    rows = bc_in.shape[1]
    states = rows // 2
    per = heads // LO
    quarter = channels // LO
    group = (lax.axis_index("tensor") * heads // GROUP_HEADS).astype(jnp.int32).reshape(1)
    xw = conv_x_w.T
    bw = jnp.swapaxes(conv_bc_w, 1, 2)
    cp = ("far", "near")
    count = lax.axis_size(cp)

    def moved(block, distance):
        return lax.ppermute(block, cp, [(i, i + distance) for i in range(count - distance)])

    tails = pl.pallas_call(
        tails_kernel,
        grid_spec=pltpu.PrefetchScalarGridSpec(
            num_scalar_prefetch=1,
            grid=(1,),
            in_specs=[
                pl.BlockSpec((channels, 128), lambda i, g: (0, length // 128 - 1)),
                pl.BlockSpec((1, rows, 128), lambda i, g: (g[0], 0, length // 128 - 1)),
            ],
            out_specs=pl.BlockSpec((8, channels + rows), lambda i, g: (0, 0)),
        ),
        out_shape=shape(8, channels + rows, dtype=BF16),
        name="tails",
    )(group, x_in, bc_in)
    rims = moved(tails, 1)
    bb = conv_bc_b[:, None, :]
    args = [x_in, bc_in, rims, dt_raw, xw, conv_x_b[None], bw, bb, dt_bias[:, None], a_log[:, None]]
    specs = [whole(a) for a in args]
    specs[1] = pl.BlockSpec((1, rows, length), lambda i, g: (g[0], 0, 0))
    specs[6] = pl.BlockSpec((1,) + bw.shape[1:], lambda i, g: (g[0], 0, 0))
    specs[7] = pl.BlockSpec((1,) + bb.shape[1:], lambda i, g: (g[0], 0, 0))
    outs = [
        shape(LO, quarter + META, states, dtype=BF16),
        shape(channels, length, dtype=BF16),
        shape(rows, length, dtype=BF16),
        shape(heads, length),
        shape(heads, length),
    ]
    pay, xc, bcc, cum, delta = pl.pallas_call(
        state_kernel,
        grid_spec=pltpu.PrefetchScalarGridSpec(
            num_scalar_prefetch=1, grid=(1,), in_specs=specs, out_specs=[whole(o) for o in outs]
        ),
        out_shape=outs,
        name="states",
    )(group, *args)
    got = lax.all_to_all(pay, "near", 0, 0, tiled=True)
    inner = pl.pallas_call(intra_kernel, out_shape=shape(channels, length), name="intra")(
        xc, bcc, cum, delta, d_skip[:, None]
    )
    block = pl.pallas_call(
        lambda *refs: group_kernel(*refs, per=per), out_shape=shape(quarter + META, states, dtype=BF16), name="totals"
    )(got)
    parts = [moved(block, LO * k) for k in range(1, count // LO)]
    entering = pl.pallas_call(
        lambda *refs: entering_kernel(*refs, per=per), out_shape=shape(LO, quarter, states, dtype=BF16), name="entering"
    )(got, *parts)
    state = lax.all_to_all(entering, "near", 0, 0, tiled=True).reshape(channels, states)
    return pl.pallas_call(output_kernel, out_shape=shape(channels, length, dtype=BF16), name="gated")(
        inner, bcc, cum, state, z_gate
    )


def solution(mesh):
    dp, cp, tensor = mesh.devices.shape
    finer = Mesh(mesh.devices.reshape(dp, cp // LO, LO, tensor), ("dp", "far", "near", "tensor"))
    along = ("dp", "far", "near")
    return jax.shard_map(
        local,
        mesh=finer,
        in_specs=(
            P("tensor", along),
            P("tensor", along),
            P(None, None, along),
            P("tensor", along),
            P("tensor", None),
            P("tensor"),
            P(),
            P(),
            P("tensor"),
            P("tensor"),
            P("tensor"),
        ),
        out_specs=P("tensor", along),
        check_vma=False,
    )
```

```python
import jax
import jax.numpy as jnp
from jax import lax
from jax.experimental import pallas as pl
from jax.experimental.pallas import tpu as pltpu
from jax.sharding import Mesh, PartitionSpec as P

HEADS = 128
GROUPS = 8
GROUP_HEADS = HEADS // GROUPS
LO = 4
META = 16

F32 = jnp.float32
BF16 = jnp.bfloat16


def dot(a, b, ca, cb):
    return lax.dot_general(a, b, (((ca,), (cb,)), ((), ())), preferred_element_type=F32)


def silu(v):
    return v / (1.0 + jnp.exp(-v))


def log1p(u):
    return jnp.where(u < 1e-3, u * (1.0 - u * (0.5 - u * (1.0 / 3.0))), jnp.log(1.0 + u))


def softplus(v):
    return jnp.maximum(v, 0.0) + log1p(jnp.exp(-jnp.abs(v)))


def picks(first_lane):
    rows = lax.broadcasted_iota(jnp.int32, (8, 128), 0)
    lanes = lax.broadcasted_iota(jnp.int32, (8, 128), 1)
    return jnp.where(jnp.logical_and(lanes == rows + first_lane, rows < 3), 1.0, 0.0).astype(BF16)


def tails_kernel(group, x, bc, last, first, bc_mine):
    channels = x.shape[0]
    begin, finish = picks(0), picks(125)
    mine = bc[0]
    bc_mine[...] = mine
    last[:, :channels] = dot(finish, x[:, 128:], 1, 1).astype(BF16)
    last[:, channels:] = dot(finish, mine[:, 128:], 1, 1).astype(BF16)
    first[:, :channels] = dot(begin, x[:, :128], 1, 1).astype(BF16)
    first[:, channels:] = dot(begin, mine[:, :128], 1, 1).astype(BF16)


def filtered(series, taps):
    lanes = lax.broadcasted_iota(jnp.int32, (series.shape[0], 128), 1)
    first, second = series[:, :128].astype(F32), series[:, 128:].astype(F32)
    a = taps[:, 4:5] + taps[:, 3:4] * first
    b = taps[:, 4:5] + taps[:, 3:4] * second
    for back in (1, 2, 3):
        moved = pltpu.roll(first, back, 1)
        tap = taps[:, 3 - back : 4 - back]
        a = a + tap * moved
        b = b + tap * jnp.where(lanes < back, moved, pltpu.roll(second, back, 1))
    return jnp.concatenate([silu(a), silu(b)], axis=1).astype(BF16)


def columns(taps, offsets):
    width = offsets.shape[1]
    rows = jnp.concatenate([taps, offsets, jnp.zeros((3, width), F32)], axis=0)
    return rows.T


def column(row):
    size = row.shape[1]
    same = lax.broadcasted_iota(jnp.int32, (size, size), 0) == lax.broadcasted_iota(jnp.int32, (size, size), 1)
    return jnp.sum(jnp.where(same, row, 0.0), axis=1, keepdims=True)


def chosen(table, group):
    rows = lax.broadcasted_iota(jnp.int32, table.shape, 0)
    return jnp.sum(jnp.where(rows == group, table, 0.0), axis=0, keepdims=True)


def split(value):
    high = value.astype(BF16)
    return high, (value - high.astype(F32)).astype(BF16)


def state_kernel(group, bw, x, bc, dt, xw, xb, bb, bias, a_log, fresh, tails, gains, taps_out, xc, bcc, cum_out, less_out):
    channels = x.shape[0]
    heads = dt.shape[0]
    width = channels // heads
    states = bc.shape[0] // 2

    delta = softplus(dt[...].astype(F32) + column(bias[...]))
    scaled = delta * -jnp.exp(column(a_log[...]))
    high = scaled.astype(BF16)
    mid, low = split(scaled - high.astype(F32))
    size = scaled.shape[1]
    upto = jnp.where(
        lax.broadcasted_iota(jnp.int32, (size, size), 0) <= lax.broadcasted_iota(jnp.int32, (size, size), 1), 1.0, 0.0
    ).astype(BF16)
    cum = dot(low, upto, 1, 0) + dot(mid, upto, 1, 0) + dot(high, upto, 1, 0)
    cum_out[...] = cum
    less_out[...] = cum - jnp.log(delta)
    end = cum[:, size - 1 :]
    gain = delta * jnp.exp(end - cum)
    total_high, total_low = split(jnp.exp(end))
    total_high, total_low = total_high.astype(F32), total_low.astype(F32)

    spread = jnp.where(
        lax.broadcasted_iota(jnp.int32, (heads, channels), 1) // width
        == lax.broadcasted_iota(jnp.int32, (heads, channels), 0),
        1.0,
        0.0,
    ).astype(BF16)
    gain_high, gain_low = split(gain[:, :128])
    gains[...] = (dot(gain_high, spread, 0, 0) + dot(gain_low, spread, 0, 0))[:8]

    offsets = chosen(bb[...], group[0])
    taps_out[...] = jnp.concatenate([bw[0], offsets, jnp.zeros((3, offsets.shape[1]), F32)], axis=0)
    bcc[...] = filtered(bc[...], columns(bw[0], offsets))
    b_rows = bcc[:states, :]
    x_taps = columns(xw[...], xb[...])
    late = jnp.where(lax.broadcasted_iota(jnp.int32, gain.shape, 1) < 3, 0.0, gain)
    meta = lax.broadcasted_iota(jnp.int32, (META, 128), 0)
    per = heads // LO
    for quarter in range(LO):
        tail = jnp.zeros((META, 128), F32)
        for j in range(per):
            h = quarter * per + j
            at = pl.ds(h * width, width)
            values = filtered(x[at, :], x_taps[h * width : (h + 1) * width])
            xc[at, :] = values
            weighted = (values.astype(F32) * late[h : h + 1]).astype(BF16)
            fresh[at, :] = dot(weighted, b_rows, 1, 1)
            tail = jnp.where(meta == 2 * j, total_high[h : h + 1], tail)
            tail = jnp.where(meta == 2 * j + 1, total_low[h : h + 1], tail)
        tails[quarter] = tail.astype(BF16)


def early(rims, first, taps, offsets):
    rows = lax.broadcasted_iota(jnp.int32, rims.shape, 0)
    series = jnp.where(rows < 3, rims, pltpu.roll(first, 3, 0))
    total = offsets + taps[0:1] * series
    for k in (1, 2, 3):
        total = total + taps[k : k + 1] * pltpu.roll(series, 8 - k, 0)
    return jnp.where(rows < 3, silu(total), 0.0).astype(BF16)


def rim_kernel(rims, first, xw, xb, bc_taps, fresh, tails, gains, pay, begun):
    channels = fresh.shape[0]
    states = fresh.shape[1]
    quarter = channels // LO
    r, f = rims[...].astype(F32), first[...].astype(F32)
    x_rows = early(r[:, :channels], f[:, :channels], xw[...], xb[...])
    bc_rows = early(r[:, channels:], f[:, channels:], bc_taps[:4], bc_taps[4:5])
    begun[:, :channels] = x_rows
    begun[:, channels:] = bc_rows
    weighted = (x_rows.astype(F32) * gains[...]).astype(BF16)
    state = fresh[...] + dot(weighted, bc_rows[:, :states], 0, 0)
    for q in range(LO):
        pay[q, :quarter, :] = state[q * quarter : (q + 1) * quarter].astype(BF16)
        pay[q, quarter:, :] = tails[q]


def unpack(block, per):
    size = block.shape[0] - META
    width = size // per
    tail = block[size:].astype(F32)
    decays = jnp.concatenate(
        [jnp.broadcast_to(tail[2 * j : 2 * j + 1] + tail[2 * j + 1 : 2 * j + 2], (width, 128)) for j in range(per)], axis=0
    )
    return block[:size].astype(F32), decays


def group_kernel(got, out, *, per):
    size = out.shape[0] - META
    width = size // per
    state, decay = unpack(got[0], per)
    for r in range(1, LO):
        fresh, d = unpack(got[r], per)
        state = fresh + d * state
        decay = decay * d
    out[:size, :] = state.astype(BF16)
    meta = lax.broadcasted_iota(jnp.int32, (META, 128), 0)
    tail = jnp.zeros((META, 128), F32)
    for j in range(per):
        d = decay[j * width : j * width + 1]
        high = d.astype(BF16).astype(F32)
        tail = jnp.where(meta == 2 * j, high, tail)
        tail = jnp.where(meta == 2 * j + 1, d - high, tail)
    out[size:, :] = tail.astype(BF16)


def entering_kernel(got, near, middle, far, out, *, per):
    last, last_decay = unpack(near[...], per)
    second, second_decay = unpack(middle[...], per)
    third, unused = unpack(far[...], per)
    state = last + last_decay * (second + second_decay * third)
    out[0] = state.astype(BF16)
    for r in range(1, LO):
        fresh, d = unpack(got[r - 1], per)
        state = fresh + d * state
        out[r] = state.astype(BF16)


def intra_kernel(xc, bcc, begun, cum_in, less_in, skip, out, c_out):
    heads = cum_in.shape[0]
    channels = xc.shape[0]
    width = channels // heads
    states = bcc.shape[0] // 2
    cum, less = cum_in[...], less_in[...]
    less_cols = jnp.concatenate([less[:, :128].T, less[:, 128:].T], axis=0)
    skips = column(skip[...])
    placed = dot(begun[...], picks(0), 0, 0).astype(BF16)

    def mended(values, rows):
        lanes = lax.broadcasted_iota(jnp.int32, rows.shape, 1)
        return jnp.concatenate([jnp.where(lanes < 3, rows, values[:, :128]), values[:, 128:]], axis=1)

    both = mended(bcc[...], placed[channels:])
    c_out[...] = both[states:]
    gram = dot(both[:states], both[states:], 0, 0)
    keep = lax.broadcasted_iota(jnp.int32, (128, 128), 0) <= lax.broadcasted_iota(jnp.int32, (128, 128), 1)
    for h in range(heads):
        at = pl.ds(h * width, width)
        values = mended(xc[at, :], placed[h * width : (h + 1) * width])
        row = cum[h : h + 1]
        col = less_cols[:, h : h + 1]

        def mix(s, t, masked):
            spread = row[:, t : t + 128] - col[s : s + 128]
            if masked:
                spread = jnp.where(keep, spread, -1e30)
            return (gram[s : s + 128, t : t + 128] * jnp.exp(spread)).astype(BF16)

        near = dot(values[:, :128], mix(0, 0, True), 1, 0)
        late = dot(values, jnp.concatenate([mix(0, 128, False), mix(128, 128, True)], axis=0), 1, 0)
        out[at, :] = jnp.concatenate([near, late], axis=1) + skips[h : h + 1] * values.astype(F32)


def output_kernel(inner, c_rows, cum, state, z, out):
    heads = cum.shape[0]
    width = inner.shape[0] // heads
    grown = jnp.exp(cum[...])
    for h in range(heads):
        at = pl.ds(h * width, width)
        y = inner[at, :] + grown[h : h + 1] * dot(state[at, :], c_rows[...], 1, 0)
        y = y.astype(BF16).astype(F32)
        out[at, :] = (y * silu(z[at, :].astype(F32))).astype(BF16)


def shape(*dims, dtype=F32):
    return pltpu.VMEM(dims, dtype)


VMEM = pl.BlockSpec(memory_space=pltpu.VMEM)


def run(kernel, name, outs, *args, table=None, group=None):
    args = [pltpu.with_memory_space_constraint(a, pltpu.VMEM) for a in args]
    specs = [VMEM] * len(args)
    out_specs = [VMEM] * len(outs)
    if group is None:
        return pl.pallas_call(kernel, out_shape=outs, in_specs=specs, out_specs=out_specs, name=name)(*args)
    picked = pl.BlockSpec((1,) + table.shape[1:], lambda i, g: (g[0], 0, 0))
    grid = pltpu.PrefetchScalarGridSpec(
        num_scalar_prefetch=1, grid=(1,), in_specs=[picked] + specs, out_specs=out_specs
    )
    return pl.pallas_call(kernel, grid_spec=grid, out_shape=outs, name=name)(group, table, *args)


def local(x_in, z_gate, bc_in, dt_raw, conv_x_w, conv_x_b, conv_bc_w, conv_bc_b, dt_bias, a_log, d_skip):
    heads, length = dt_raw.shape
    channels = x_in.shape[0]
    rows = bc_in.shape[1]
    states = rows // 2
    per = heads // LO
    quarter = channels // LO
    group = (lax.axis_index("tensor") // (GROUP_HEADS // heads)).astype(jnp.int32).reshape(1)
    xw = conv_x_w.T
    bw = jnp.swapaxes(conv_bc_w, 1, 2)
    xb, bias, rate, skip = conv_x_b[None], dt_bias[None], a_log[None], d_skip[None]
    cp = ("far", "near")
    count = lax.axis_size(cp)

    def moved(block, distance):
        return lax.ppermute(block, cp, [(i, i + distance) for i in range(count - distance)])

    strip = shape(8, channels + rows, dtype=BF16)
    last, first, bc = run(
        lambda g, bc, x, *outs: tails_kernel(g, x, bc, *outs),
        "tails",
        [strip, strip, shape(rows, length, dtype=BF16)],
        x_in,
        table=bc_in,
        group=group,
    )
    rims = moved(last, 1)
    fresh, tails, gains, bc_taps, xc, bcc, cum, less = run(
        state_kernel,
        "states",
        [
            shape(channels, states),
            shape(LO, META, 128, dtype=BF16),
            shape(8, channels),
            shape(8, rows),
            shape(channels, length, dtype=BF16),
            shape(rows, length, dtype=BF16),
            shape(heads, length),
            shape(heads, length),
        ],
        x_in,
        bc,
        dt_raw,
        xw,
        xb,
        conv_bc_b,
        bias,
        rate,
        table=bw,
        group=group,
    )
    pay, begun = run(
        rim_kernel,
        "rims",
        [shape(LO, quarter + META, states, dtype=BF16), strip],
        rims,
        first,
        xw,
        xb,
        bc_taps,
        fresh,
        tails,
        gains,
    )
    got = lax.all_to_all(pay, "near", 0, 0, tiled=True)
    inner, c_rows = run(
        intra_kernel,
        "intra",
        [shape(channels, length), shape(states, length, dtype=BF16)],
        xc,
        bcc,
        begun,
        cum,
        less,
        skip,
    )
    (block,) = run(
        lambda *refs: group_kernel(*refs, per=per), "totals", [shape(quarter + META, states, dtype=BF16)], got
    )
    middle = moved(block, 2 * LO)
    far = moved(block, 3 * LO)
    near = moved(block, LO)
    near, inner, c_rows = lax.optimization_barrier((near, inner, c_rows))
    (entering,) = run(
        lambda *refs: entering_kernel(*refs, per=per),
        "entering",
        [shape(LO, quarter, states, dtype=BF16)],
        got,
        near,
        middle,
        far,
    )
    state = lax.all_to_all(entering, "near", 0, 0, tiled=True).reshape(channels, states)
    (out,) = run(
        output_kernel, "gated", [jax.ShapeDtypeStruct((channels, length), BF16)], inner, c_rows, cum, state, z_gate
    )
    return out


def solution(mesh):
    dp, cp, tensor = mesh.devices.shape
    finer = Mesh(mesh.devices.reshape(dp, cp // LO, LO, tensor), ("dp", "far", "near", "tensor"))
    along = ("dp", "far", "near")
    return jax.shard_map(
        local,
        mesh=finer,
        in_specs=(
            P("tensor", along),
            P("tensor", along),
            P(None, None, along),
            P("tensor", along),
            P("tensor", None),
            P("tensor"),
            P(),
            P(),
            P("tensor"),
            P("tensor"),
            P("tensor"),
        ),
        out_specs=P("tensor", along),
        check_vma=False,
    )
```

```python
import jax
import jax.numpy as jnp
from jax import lax
from jax.experimental import pallas as pl
from jax.experimental.pallas import tpu as pltpu
from jax.sharding import Mesh, PartitionSpec as P


HEADS = 128
GROUPS = 8
GROUP_HEADS = HEADS // GROUPS
LO = 4
META = 16

F32 = jnp.float32
BF16 = jnp.bfloat16


def dot(a, b, ca, cb):
    return lax.dot_general(a, b, (((ca,), (cb,)), ((), ())), preferred_element_type=F32)


def silu(v):
    return v / (1.0 + jnp.exp(-v))


def log1p(u):
    return jnp.where(u < 1e-3, u * (1.0 - u * (0.5 - u * (1.0 / 3.0))), jnp.log(1.0 + u))


def softplus(v):
    return jnp.maximum(v, 0.0) + log1p(jnp.exp(-jnp.abs(v)))


def picks(first_lane):
    rows = lax.broadcasted_iota(jnp.int32, (8, 128), 0)
    lanes = lax.broadcasted_iota(jnp.int32, (8, 128), 1)
    return jnp.where(jnp.logical_and(lanes == rows + first_lane, rows < 3), 1.0, 0.0).astype(BF16)


def load_kernel(
    group, bc, bw, x, dt, xw, xb, bb, bias, a_log, skip, last, first, x_out, bc_out, dt_out, x_taps, bc_taps, per_head
):
    channels = x.shape[0]
    heads = dt.shape[0]
    begin, finish = picks(0), picks(125)
    series, mine = x[...], bc[0]
    last[:, :channels] = dot(finish, series[:, 128:], 1, 1).astype(BF16)
    last[:, channels:] = dot(finish, mine[:, 128:], 1, 1).astype(BF16)
    first[:, :channels] = dot(begin, series[:, :128], 1, 1).astype(BF16)
    first[:, channels:] = dot(begin, mine[:, :128], 1, 1).astype(BF16)
    x_out[...] = series
    bc_out[...] = mine
    dt_out[...] = dt[...]
    x_taps[:4, :] = xw[...]
    x_taps[4:, :] = jnp.broadcast_to(xb[...], (4, channels))
    bc_taps[:4, :] = bw[0]
    bc_taps[4:, :] = jnp.broadcast_to(chosen(bb[...], group[0]), (4, mine.shape[0]))
    for i, row in enumerate((bias, a_log, skip)):
        per_head[i] = jnp.broadcast_to(column(row[...]), (heads, 128))


def filtered(series, taps):
    lanes = lax.broadcasted_iota(jnp.int32, (series.shape[0], 128), 1)
    first, second = series[:, :128].astype(F32), series[:, 128:].astype(F32)
    a = taps[:, 4:5] + taps[:, 3:4] * first
    b = taps[:, 4:5] + taps[:, 3:4] * second
    for back in (1, 2, 3):
        moved = pltpu.roll(first, back, 1)
        tap = taps[:, 3 - back : 4 - back]
        a = a + tap * moved
        b = b + tap * jnp.where(lanes < back, moved, pltpu.roll(second, back, 1))
    return jnp.concatenate([silu(a), silu(b)], axis=1).astype(BF16)


def column(row):
    size = row.shape[1]
    same = lax.broadcasted_iota(jnp.int32, (size, size), 0) == lax.broadcasted_iota(jnp.int32, (size, size), 1)
    return jnp.sum(jnp.where(same, row, 0.0), axis=1, keepdims=True)


def chosen(table, group):
    rows = lax.broadcasted_iota(jnp.int32, table.shape, 0)
    return jnp.sum(jnp.where(rows == group, table, 0.0), axis=0, keepdims=True)


def split(value):
    high = value.astype(BF16)
    return high, (value - high.astype(F32)).astype(BF16)


def state_kernel(x, bc, dt, x_taps, bc_taps, per_head, fresh, tails, gains, xc, bcc, cum_out, less_out):
    channels = x.shape[0]
    heads = dt.shape[0]
    width = channels // heads
    states = bc.shape[0] // 2

    delta = softplus(dt[...].astype(F32) + per_head[0][:, :1])
    scaled = delta * -jnp.exp(per_head[1][:, :1])
    high = scaled.astype(BF16)
    mid, low = split(scaled - high.astype(F32))
    size = scaled.shape[1]
    upto = jnp.where(
        lax.broadcasted_iota(jnp.int32, (size, size), 0) <= lax.broadcasted_iota(jnp.int32, (size, size), 1), 1.0, 0.0
    ).astype(BF16)
    cum = dot(low, upto, 1, 0) + dot(mid, upto, 1, 0) + dot(high, upto, 1, 0)
    cum_out[...] = cum
    less_out[...] = cum - jnp.log(delta)
    end = cum[:, size - 1 :]
    gain = delta * jnp.exp(end - cum)
    total_high, total_low = split(jnp.exp(end))
    total_high, total_low = total_high.astype(F32), total_low.astype(F32)

    spread = jnp.where(
        lax.broadcasted_iota(jnp.int32, (heads, channels), 1) // width
        == lax.broadcasted_iota(jnp.int32, (heads, channels), 0),
        1.0,
        0.0,
    ).astype(BF16)
    gain_high, gain_low = split(gain[:, :128])
    gains[...] = (dot(gain_high, spread, 0, 0) + dot(gain_low, spread, 0, 0))[:8]

    bcc[...] = filtered(bc[...], bc_taps[...].T)
    b_rows = bcc[:states, :]
    x_cols = x_taps[...].T
    late = jnp.where(lax.broadcasted_iota(jnp.int32, gain.shape, 1) < 3, 0.0, gain)
    meta = lax.broadcasted_iota(jnp.int32, (META, 128), 0)
    per = heads // LO
    for quarter in range(LO):
        tail = jnp.zeros((META, 128), F32)
        for j in range(per):
            h = quarter * per + j
            at = pl.ds(h * width, width)
            values = filtered(x[at, :], x_cols[h * width : (h + 1) * width])
            xc[at, :] = values
            weighted = (values.astype(F32) * late[h : h + 1]).astype(BF16)
            fresh[at, :] = dot(weighted, b_rows, 1, 1)
            tail = jnp.where(meta == 2 * j, total_high[h : h + 1], tail)
            tail = jnp.where(meta == 2 * j + 1, total_low[h : h + 1], tail)
        tails[quarter] = tail.astype(BF16)


def early(rims, first, taps):
    rows = lax.broadcasted_iota(jnp.int32, rims.shape, 0)
    series = jnp.where(rows < 3, rims, pltpu.roll(first, 3, 0))
    total = taps[4:5] + taps[0:1] * series
    for k in (1, 2, 3):
        total = total + taps[k : k + 1] * pltpu.roll(series, 8 - k, 0)
    return jnp.where(rows < 3, silu(total), 0.0).astype(BF16)


def rim_kernel(rims, first, x_taps, bc_taps, fresh, tails, gains, pay, begun):
    channels = fresh.shape[0]
    states = fresh.shape[1]
    quarter = channels // LO
    r, f = rims[...].astype(F32), first[...].astype(F32)
    x_rows = early(r[:, :channels], f[:, :channels], x_taps[...])
    bc_rows = early(r[:, channels:], f[:, channels:], bc_taps[...])
    begun[:, :channels] = x_rows
    begun[:, channels:] = bc_rows
    weighted = (x_rows.astype(F32) * gains[...]).astype(BF16)
    state = fresh[...] + dot(weighted, bc_rows[:, :states], 0, 0)
    for q in range(LO):
        pay[q, :quarter, :] = state[q * quarter : (q + 1) * quarter].astype(BF16)
        pay[q, quarter:, :] = tails[q]


def unpack(block, per):
    size = block.shape[0] - META
    width = size // per
    tail = block[size:].astype(F32)
    decays = jnp.concatenate(
        [jnp.broadcast_to(tail[2 * j : 2 * j + 1] + tail[2 * j + 1 : 2 * j + 2], (width, 128)) for j in range(per)], axis=0
    )
    return block[:size].astype(F32), decays


def packed(state, decay, out, per):
    size = out.shape[0] - META
    width = size // per
    out[:size, :] = state.astype(BF16)
    meta = lax.broadcasted_iota(jnp.int32, (META, 128), 0)
    tail = jnp.zeros((META, 128), F32)
    for j in range(per):
        d = decay[j * width : j * width + 1]
        high = d.astype(BF16).astype(F32)
        tail = jnp.where(meta == 2 * j, high, tail)
        tail = jnp.where(meta == 2 * j + 1, d - high, tail)
    out[size:, :] = tail.astype(BF16)


def group_kernel(got, kept, out, *, per):
    kept[...] = got[...]
    state, decay = unpack(got[0], per)
    for r in range(1, LO):
        fresh, d = unpack(got[r], per)
        state = fresh + d * state
        decay = decay * d
    packed(state, decay, out, per)


def join_kernel(earlier, later, out, *, per):
    before, decay_before = unpack(earlier[...], per)
    after, decay = unpack(later[...], per)
    packed(after + decay * before, decay * decay_before, out, per)


def entering_kernel(got, *refs, per):
    *given, out = refs
    if given:
        near, next_one, over, between = given
        last, last_decay = unpack(between[...], per)
        state = last + last_decay * unpack(over[...], per)[0]
        state = state + unpack(near[...], per)[0] + unpack(next_one[...], per)[0]
    else:
        state = jnp.zeros(out.shape[1:], F32)
    out[0] = state.astype(BF16)
    for r in range(1, LO):
        fresh, d = unpack(got[r - 1], per)
        state = fresh + d * state
        out[r] = state.astype(BF16)


def copy_kernel(*refs):
    half = len(refs) // 2
    for source, target in zip(refs[:half], refs[half:]):
        target[...] = source[...]


def blank_kernel(*refs):
    for ref in refs:
        ref[...] = jnp.zeros(ref.shape, ref.dtype)


def intra_kernel(xc, bcc, begun, cum_in, less_in, per_head, out, c_out):
    heads = cum_in.shape[0]
    channels = xc.shape[0]
    width = channels // heads
    states = bcc.shape[0] // 2
    cum, less = cum_in[...], less_in[...]
    less_cols = jnp.concatenate([less[:, :128].T, less[:, 128:].T], axis=0)
    skips = per_head[2][:, :1]
    placed = dot(begun[...], picks(0), 0, 0).astype(BF16)

    def mended(values, rows):
        lanes = lax.broadcasted_iota(jnp.int32, rows.shape, 1)
        return jnp.concatenate([jnp.where(lanes < 3, rows, values[:, :128]), values[:, 128:]], axis=1)

    both = mended(bcc[...], placed[channels:])
    c_out[...] = both[states:]
    gram = dot(both[:states], both[states:], 0, 0)
    keep = lax.broadcasted_iota(jnp.int32, (128, 128), 0) <= lax.broadcasted_iota(jnp.int32, (128, 128), 1)
    for h in range(heads):
        at = pl.ds(h * width, width)
        values = mended(xc[at, :], placed[h * width : (h + 1) * width])
        row = cum[h : h + 1]
        col = less_cols[:, h : h + 1]

        def mix(s, t, masked):
            spread = row[:, t : t + 128] - col[s : s + 128]
            if masked:
                spread = jnp.where(keep, spread, -1e30)
            return (gram[s : s + 128, t : t + 128] * jnp.exp(spread)).astype(BF16)

        near = dot(values[:, :128], mix(0, 0, True), 1, 0)
        late = dot(values, jnp.concatenate([mix(0, 128, False), mix(128, 128, True)], axis=0), 1, 0)
        out[at, :] = jnp.concatenate([near, late], axis=1) + skips[h : h + 1] * values.astype(F32)


def output_kernel(inner, c_rows, cum, state, z, out):
    heads = cum.shape[0]
    width = inner.shape[0] // heads
    grown = jnp.exp(cum[...])
    for h in range(heads):
        at = pl.ds(h * width, width)
        y = inner[at, :] + grown[h : h + 1] * dot(state[at, :], c_rows[...], 1, 0)
        y = y.astype(BF16).astype(F32)
        out[at, :] = (y * silu(z[at, :].astype(F32))).astype(BF16)


def shape(*dims, dtype=F32):
    return pltpu.VMEM(dims, dtype)


VMEM = pl.BlockSpec(memory_space=pltpu.VMEM)


def run(kernel, outs, *args):
    args = [pltpu.with_memory_space_constraint(a, pltpu.VMEM) for a in args]
    return pl.pallas_call(kernel, out_shape=outs, in_specs=[VMEM] * len(args), out_specs=[VMEM] * len(outs))(*args)


def local(x_in, z_gate, bc_in, dt_raw, conv_x_w, conv_x_b, conv_bc_w, conv_bc_b, dt_bias, a_log, d_skip):
    heads, length = dt_raw.shape
    channels = x_in.shape[0]
    rows = bc_in.shape[1]
    states = rows // 2
    per = heads // LO
    quarter = channels // LO
    group = (lax.axis_index("tensor") // (GROUP_HEADS // heads)).astype(jnp.int32).reshape(1)
    far = lax.axis_index("far")
    cp = ("far", "near")

    strip = shape(8, channels + rows, dtype=BF16)
    block_shape = shape(quarter + META, states, dtype=BF16)
    kept_shape = shape(LO, quarter + META, states, dtype=BF16)
    series = shape(channels, length, dtype=BF16)
    taps = jnp.swapaxes(conv_bc_w, 1, 2)
    small = [dt_raw, conv_x_w.T, conv_x_b[None], conv_bc_b, dt_bias[None], a_log[None], d_skip[None]]
    last, first, x, bc, dt, x_taps, bc_taps, per_head = pl.pallas_call(
        load_kernel,
        grid_spec=pltpu.PrefetchScalarGridSpec(
            num_scalar_prefetch=1,
            grid=(1,),
            in_specs=[pl.BlockSpec((1,) + a.shape[1:], lambda i, g: (g[0], 0, 0)) for a in (bc_in, taps)]
            + [pl.BlockSpec(a.shape, lambda i, g: (0, 0)) for a in [x_in] + small],
            out_specs=[VMEM] * 8,
        ),
        out_shape=[
            strip,
            strip,
            series,
            shape(rows, length, dtype=BF16),
            shape(heads, length, dtype=BF16),
            shape(8, channels),
            shape(8, rows),
            shape(3, heads, 128),
        ],
        name="load",
    )(group, bc_in, taps, x_in, *small)
    count = lax.axis_size(cp)
    rims = lax.ppermute(last, cp, [(i, i + 1) for i in range(count - 1)])
    fresh, tails, gains, xc, bcc, cum, less = run(
        state_kernel,
        [
            shape(channels, states),
            shape(LO, META, 128, dtype=BF16),
            shape(8, channels),
            series,
            shape(rows, length, dtype=BF16),
            shape(heads, length),
            shape(heads, length),
        ],
        x,
        bc,
        dt,
        x_taps,
        bc_taps,
        per_head,
    )
    pay, begun = run(rim_kernel, [kept_shape, strip], rims, first, x_taps, bc_taps, fresh, tails, gains)

    def gather():
        got = lax.all_to_all(pay, "near", 0, 0, tiled=True)
        return tuple(run(lambda *refs: group_kernel(*refs, per=per), [kept_shape, block_shape], got))

    def blank(*outs):
        return tuple(run(blank_kernel, list(outs)))

    def inside():
        return run(
            intra_kernel,
            [shape(channels, length), shape(states, length, dtype=BF16)],
            xc,
            bcc,
            begun,
            cum,
            less,
            per_head,
        )

    def finish(target, inner, c_rows, kept, *given):
        (entering,) = run(
            lambda *refs: entering_kernel(*refs, per=per), [shape(LO, quarter, states, dtype=BF16)], kept, *given
        )
        state = lax.all_to_all(entering, "near", 0, 0, tiled=True).reshape(channels, states)
        return run(output_kernel, [target], inner, c_rows, cum, state, z_gate)[0]

    def sent(block, source, target):
        pairs = [(source * LO + i, target * LO + i) for i in range(LO)]
        return lax.ppermute(block, cp, pairs)

    def first_branch(kept, block):
        return blank(kept_shape, block_shape) + (finish(series, *inside(), kept),)

    def second_branch(kept, block):
        return gather() + blank(series)

    kept, block = lax.cond(far == 0, gather, lambda: blank(kept_shape, block_shape))
    near = sent(block, 0, 1)
    kept, block, begin = lax.switch(
        jnp.minimum(far, 2),
        [first_branch, second_branch, lambda kept, block: blank(kept_shape, block_shape, series)],
        kept,
        block,
    )
    (joined,) = run(lambda *refs: join_kernel(*refs, per=per), [block_shape], near, block)
    next_one = sent(joined, 1, 2)
    over = sent(joined, 1, 3)
    kept, block = lax.cond(
        far >= 2,
        lambda kept, block: gather(),
        lambda kept, block: tuple(run(copy_kernel, [kept_shape, block_shape], kept, block)),
        kept,
        block,
    )
    between = sent(block, 2, 3)
    inner, c_rows = inside()
    out = jax.ShapeDtypeStruct((channels, length), BF16)
    return lax.cond(
        far == 0,
        lambda begin, *unused: run(copy_kernel, [out], begin)[0],
        lambda begin, *given: finish(out, *given),
        begin,
        inner,
        c_rows,
        kept,
        near,
        next_one,
        over,
        between,
    )


def solution(mesh):
    dp, cp, tensor = mesh.devices.shape
    finer = Mesh(mesh.devices.reshape(dp, cp // LO, LO, tensor), ("dp", "far", "near", "tensor"))
    along = ("dp", "far", "near")
    return jax.shard_map(
        local,
        mesh=finer,
        in_specs=(
            P("tensor", along),
            P("tensor", along),
            P(None, None, along),
            P("tensor", along),
            P("tensor", None),
            P("tensor"),
            P(),
            P(),
            P("tensor"),
            P("tensor"),
            P("tensor"),
        ),
        out_specs=P("tensor", along),
        check_vma=False,
    )
```

```python
import jax
import jax.numpy as jnp
from jax import lax
from jax.experimental import pallas as pl
from jax.experimental.pallas import tpu as pltpu
from jax.sharding import Mesh, PartitionSpec as P


HEADS = 128
GROUPS = 8
GROUP_HEADS = HEADS // GROUPS
LO = 4
META = 32

F32 = jnp.float32
BF16 = jnp.bfloat16


def dot(a, b, ca, cb):
    return lax.dot_general(a, b, (((ca,), (cb,)), ((), ())), preferred_element_type=F32)


def silu(v):
    return v / (1.0 + jnp.exp(-v))


def log1p(u):
    return jnp.where(u < 1e-3, u * (1.0 - u * (0.5 - u * (1.0 / 3.0))), jnp.log(1.0 + u))


def softplus(v):
    return jnp.maximum(v, 0.0) + log1p(jnp.exp(-jnp.abs(v)))


def picks(first_lane):
    rows = lax.broadcasted_iota(jnp.int32, (8, 128), 0)
    lanes = lax.broadcasted_iota(jnp.int32, (8, 128), 1)
    return jnp.where(jnp.logical_and(lanes == rows + first_lane, rows < 3), 1.0, 0.0).astype(BF16)


def load_kernel(
    group, member, bc, bw, x, dt, xw, xb, bb, bias, a_log, skip,
    last, first, x_out, bc_out, dt_out, x_taps, bc_taps, own_taps, per_head,
):
    channels = x.shape[0]
    heads = dt.shape[0]
    begin, finish = picks(0), picks(125)
    series, mine = x[...], bc[0]
    last[:, :channels] = dot(finish, series[:, 128:], 1, 1).astype(BF16)
    last[:, channels:] = dot(finish, mine[:, 128:], 1, 1).astype(BF16)
    first[:, :channels] = dot(begin, series[:, :128], 1, 1).astype(BF16)
    first[:, channels:] = dot(begin, mine[:, :128], 1, 1).astype(BF16)
    x_out[...] = series
    bc_out[...] = mine
    dt_out[...] = dt[...]
    x_taps[:4, :] = xw[...]
    x_taps[4:, :] = jnp.broadcast_to(xb[...], (4, channels))
    own = jnp.zeros(own_taps.shape[1:], F32)
    for q in range(LO):
        own = jnp.where(member[0] == q, x_taps[:, q * 128 : (q + 1) * 128], own)
    own_taps[0] = own
    bc_taps[:4, :] = bw[0]
    bc_taps[4:, :] = jnp.broadcast_to(chosen(bb[...], group[0]), (4, mine.shape[0]))
    own_taps[1] = bc_taps[:, :128]
    for i, row in enumerate((bias, a_log, skip)):
        per_head[i] = jnp.broadcast_to(column(row[...]), (heads, 128))


def filtered(series, taps):
    lanes = lax.broadcasted_iota(jnp.int32, (series.shape[0], 128), 1)
    first, second = series[:, :128].astype(F32), series[:, 128:].astype(F32)
    a = taps[:, 4:5] + taps[:, 3:4] * first
    b = taps[:, 4:5] + taps[:, 3:4] * second
    for back in (1, 2, 3):
        moved = pltpu.roll(first, back, 1)
        tap = taps[:, 3 - back : 4 - back]
        a = a + tap * moved
        b = b + tap * jnp.where(lanes < back, moved, pltpu.roll(second, back, 1))
    return jnp.concatenate([silu(a), silu(b)], axis=1).astype(BF16)


def column(row):
    size = row.shape[1]
    same = lax.broadcasted_iota(jnp.int32, (size, size), 0) == lax.broadcasted_iota(jnp.int32, (size, size), 1)
    return jnp.sum(jnp.where(same, row, 0.0), axis=1, keepdims=True)


def chosen(table, group):
    rows = lax.broadcasted_iota(jnp.int32, table.shape, 0)
    return jnp.sum(jnp.where(rows == group, table, 0.0), axis=0, keepdims=True)


def split(value):
    high = value.astype(BF16)
    return high, (value - high.astype(F32)).astype(BF16)


def state_kernel(x, bc, dt, x_taps, bc_taps, per_head, last, first, pay, xc, bcc, cum_out, less_out):
    channels = x.shape[0]
    heads = dt.shape[0]
    width = channels // heads
    states = bc.shape[0] // 2

    delta = softplus(dt[...].astype(F32) + per_head[0][:, :1])
    scaled = delta * -jnp.exp(per_head[1][:, :1])
    high = scaled.astype(BF16)
    mid, low = split(scaled - high.astype(F32))
    size = scaled.shape[1]
    upto = jnp.where(
        lax.broadcasted_iota(jnp.int32, (size, size), 0) <= lax.broadcasted_iota(jnp.int32, (size, size), 1), 1.0, 0.0
    ).astype(BF16)
    cum = dot(low, upto, 1, 0) + dot(mid, upto, 1, 0) + dot(high, upto, 1, 0)
    cum_out[...] = cum
    less_out[...] = cum - jnp.log(delta)
    end = cum[:, size - 1 :]
    gain = delta * jnp.exp(end - cum)
    total_high, total_low = split(jnp.exp(end))
    total_high, total_low = total_high.astype(F32), total_low.astype(F32)

    spread = jnp.where(
        lax.broadcasted_iota(jnp.int32, (heads, channels), 1) // width
        == lax.broadcasted_iota(jnp.int32, (heads, channels), 0),
        1.0,
        0.0,
    ).astype(BF16)
    gain_high, gain_low = split(gain[:, :128])
    lines = lax.broadcasted_iota(jnp.int32, (8, channels), 0)
    gains = jnp.where(lines < 4, dot(gain_high, spread, 0, 0)[:8], pltpu.roll(dot(gain_low, spread, 0, 0)[:8], 4, 0))
    lines = lax.broadcasted_iota(jnp.int32, last.shape, 0)
    edges = jnp.where(lines < 3, last[...].astype(F32), pltpu.roll(first[...].astype(F32), 3, 0))

    bcc[...] = filtered(bc[...], bc_taps[...].T)
    b_rows = bcc[:states, :]
    x_cols = x_taps[...].T
    late = jnp.where(lax.broadcasted_iota(jnp.int32, gain.shape, 1) < 3, 0.0, gain)
    lines = lax.broadcasted_iota(jnp.int32, (8, 128), 0)
    per = heads // LO
    for quarter in range(LO):
        tail = jnp.zeros((8, 128), F32)
        for j in range(per):
            h = quarter * per + j
            at = pl.ds(h * width, width)
            values = filtered(x[at, :], x_cols[h * width : (h + 1) * width])
            xc[at, :] = values
            weighted = (values.astype(F32) * late[h : h + 1]).astype(BF16)
            pay[quarter, pl.ds(j * width, width), :] = dot(weighted, b_rows, 1, 1).astype(BF16)
            tail = jnp.where(lines == 2 * j, total_high[h : h + 1], tail)
            tail = jnp.where(lines == 2 * j + 1, total_low[h : h + 1], tail)
        here = slice(quarter * 128, (quarter + 1) * 128)
        rows = jnp.concatenate([tail, edges[:, here], edges[:, channels : channels + 128], gains[:, here]], axis=0)
        pay[quarter, pl.ds(per * width, META), :] = rows.astype(BF16)


def early(series, taps):
    rows = lax.broadcasted_iota(jnp.int32, series.shape, 0)
    total = taps[4:5] + taps[0:1] * series
    for k in (1, 2, 3):
        total = total + taps[k : k + 1] * pltpu.roll(series, 8 - k, 0)
    return jnp.where(rows < 3, silu(total), 0.0).astype(BF16)


def rim_state(before, after, taps):
    rows = lax.broadcasted_iota(jnp.int32, (8, 128), 0)
    x_rows = early(jnp.where(rows < 3, before[8:16], after[8:16]), taps[0])
    b_rows = early(jnp.where(rows < 3, before[16:24], after[16:24]), taps[1])
    gains = after[24:32] + pltpu.roll(after[24:32], 4, 0)
    return dot((x_rows.astype(F32) * gains).astype(BF16), b_rows, 0, 0)


def spread_rows(rows, start, per, size):
    width = size // per
    values = [rows[start + 2 * j : start + 2 * j + 1] + rows[start + 2 * j + 1 : start + 2 * j + 2] for j in range(per)]
    return jnp.concatenate([jnp.broadcast_to(v, (width, 128)) for v in values], axis=0)


def unpack(block):
    size = block.shape[0] - META
    return block[:size].astype(F32), block[size:].astype(F32)


def packed_rows(decay, start, rows, per):
    width = decay.shape[0] // per
    lines = lax.broadcasted_iota(jnp.int32, (8, 128), 0)
    for j in range(per):
        d = decay[j * width : j * width + 1]
        high = d.astype(BF16).astype(F32)
        rows = jnp.where(lines == start + 2 * j, high, rows)
        rows = jnp.where(lines == start + 2 * j + 1, d - high, rows)
    return rows


def group_kernel(got, taps, kept, meta, out, *, per, opening):
    size = out.shape[0] - META
    members = [unpack(got[r]) for r in range(LO)]
    lines = lax.broadcasted_iota(jnp.int32, (META, 128), 0)
    state, rows = members[0]
    if opening:
        state = state + rim_state(jnp.zeros_like(rows), rows, taps)
    kept[0] = state
    decay = spread_rows(rows, 0, per, size)
    suffix = jnp.ones_like(decay)
    for r in range(1, LO):
        fresh, now = members[r]
        fresh = fresh + rim_state(members[r - 1][1], now, taps)
        kept[r] = fresh
        d = spread_rows(now, 0, per, size)
        state = fresh + d * state
        decay, suffix = decay * d, suffix * d
    meta[...] = got[:, size:, :]
    out[:size, :] = state.astype(BF16)
    head = packed_rows(suffix, 4, packed_rows(decay, 0, jnp.zeros((8, 128), F32), per), per)
    edge = lax.broadcasted_iota(jnp.int32, (16, 128), 0) % 8 < 3
    edges = jnp.where(edge, members[LO - 1][1][8:24], rows[8:24])
    out[size:, :] = jnp.concatenate([head, edges, rows[24:32]], axis=0).astype(BF16)


def join_kernel(earlier, later, taps, out, *, per):
    size = out.shape[0] - META
    before, rows_before = unpack(earlier[...])
    after, rows = unpack(later[...])
    opening = rim_state(rows_before, rows, taps)
    state = after + spread_rows(rows, 4, per, size) * opening + spread_rows(rows, 0, per, size) * before
    out[:size, :] = state.astype(BF16)
    out[size:, :] = later[size:, :]


def entering_kernel(kept, meta, *refs, per):
    *given, out = refs
    size = kept.shape[1]
    own = meta[0].astype(F32)
    fresh = kept[0]
    state = jnp.zeros(out.shape[1:], F32)
    if given:
        taps, near, next_one, over, between = given
        (near, rows_near), (next_one, rows_next) = unpack(near[...]), unpack(next_one[...])
        (over, rows_over), (between, rows) = unpack(over[...]), unpack(between[...])
        opening = rim_state(rows_over, rows, taps)
        state = between + spread_rows(rows, 4, per, size) * opening + spread_rows(rows, 0, per, size) * over
        state = state + near + next_one
        fresh = fresh + rim_state(rows_near + rows_next + rows, own, taps)
    out[0] = state.astype(BF16)
    for r in range(1, LO):
        state = fresh + spread_rows(meta[r - 1].astype(F32), 0, per, size) * state
        out[r] = state.astype(BF16)
        fresh = kept[r]


def copy_kernel(*refs):
    half = len(refs) // 2
    for source, target in zip(refs[:half], refs[half:]):
        target[...] = source[...]


def blank_kernel(*refs):
    for ref in refs:
        ref[...] = jnp.zeros(ref.shape, ref.dtype)


def intra_kernel(xc, bcc, rims, first, x_taps, bc_taps, cum_in, less_in, per_head, out, c_out):
    heads = cum_in.shape[0]
    channels = xc.shape[0]
    width = channels // heads
    states = bcc.shape[0] // 2
    cum, less = cum_in[...], less_in[...]
    less_cols = jnp.concatenate([less[:, :128].T, less[:, 128:].T], axis=0)
    skips = per_head[2][:, :1]
    lines = lax.broadcasted_iota(jnp.int32, rims.shape, 0)
    edges = jnp.where(lines < 3, rims[...].astype(F32), pltpu.roll(first[...].astype(F32), 3, 0))
    begun = [early(edges[:, :channels], x_taps[...]), early(edges[:, channels:], bc_taps[...])]
    placed = dot(jnp.concatenate(begun, axis=1), picks(0), 0, 0).astype(BF16)

    def mended(values, rows):
        lanes = lax.broadcasted_iota(jnp.int32, rows.shape, 1)
        return jnp.concatenate([jnp.where(lanes < 3, rows, values[:, :128]), values[:, 128:]], axis=1)

    both = mended(bcc[...], placed[channels:])
    c_out[...] = both[states:]
    gram = dot(both[:states], both[states:], 0, 0)
    keep = lax.broadcasted_iota(jnp.int32, (128, 128), 0) <= lax.broadcasted_iota(jnp.int32, (128, 128), 1)
    for h in range(heads):
        at = pl.ds(h * width, width)
        values = mended(xc[at, :], placed[h * width : (h + 1) * width])
        row = cum[h : h + 1]
        col = less_cols[:, h : h + 1]

        def mix(s, t, masked):
            spread = row[:, t : t + 128] - col[s : s + 128]
            if masked:
                spread = jnp.where(keep, spread, -1e30)
            return (gram[s : s + 128, t : t + 128] * jnp.exp(spread)).astype(BF16)

        near = dot(values[:, :128], mix(0, 0, True), 1, 0)
        late = dot(values, jnp.concatenate([mix(0, 128, False), mix(128, 128, True)], axis=0), 1, 0)
        out[at, :] = jnp.concatenate([near, late], axis=1) + skips[h : h + 1] * values.astype(F32)


def output_kernel(inner, c_rows, cum, state, z, out):
    heads = cum.shape[0]
    width = inner.shape[0] // heads
    grown = jnp.exp(cum[...])
    for h in range(heads):
        at = pl.ds(h * width, width)
        y = inner[at, :] + grown[h : h + 1] * dot(state[at, :], c_rows[...], 1, 0)
        y = y.astype(BF16).astype(F32)
        out[at, :] = (y * silu(z[at, :].astype(F32))).astype(BF16)


def shape(*dims, dtype=F32):
    return pltpu.VMEM(dims, dtype)


VMEM = pl.BlockSpec(memory_space=pltpu.VMEM)


def run(kernel, outs, *args):
    args = [pltpu.with_memory_space_constraint(a, pltpu.VMEM) for a in args]
    return pl.pallas_call(kernel, out_shape=outs, in_specs=[VMEM] * len(args), out_specs=[VMEM] * len(outs))(*args)


def local(x_in, z_gate, bc_in, dt_raw, conv_x_w, conv_x_b, conv_bc_w, conv_bc_b, dt_bias, a_log, d_skip):
    heads, length = dt_raw.shape
    channels = x_in.shape[0]
    rows = bc_in.shape[1]
    states = rows // 2
    per = heads // LO
    quarter = channels // LO
    group = (lax.axis_index("tensor") // (GROUP_HEADS // heads)).astype(jnp.int32).reshape(1)
    member = lax.axis_index("near").astype(jnp.int32).reshape(1)
    far = lax.axis_index("far")
    cp = ("far", "near")
    count = lax.axis_size(cp)

    strip = shape(8, channels + rows, dtype=BF16)
    block_shape = shape(quarter + META, states, dtype=BF16)
    kept_shapes = [shape(LO, quarter, states), shape(LO, META, states, dtype=BF16)]
    state_shape = shape(LO, quarter, states, dtype=BF16)
    series = shape(channels, length, dtype=BF16)
    pairs = shape(rows, length, dtype=BF16)
    taps = jnp.swapaxes(conv_bc_w, 1, 2)
    small = [dt_raw, conv_x_w.T, conv_x_b[None], conv_bc_b, dt_bias[None], a_log[None], d_skip[None]]
    outs = [strip, strip, series, pairs, shape(heads, length, dtype=BF16), shape(8, channels), shape(8, rows)]
    outs += [shape(2, 8, 128), shape(3, heads, 128)]
    last, first, x, bc, dt, x_taps, bc_taps, own_taps, per_head = pl.pallas_call(
        load_kernel,
        grid_spec=pltpu.PrefetchScalarGridSpec(
            num_scalar_prefetch=2,
            grid=(1,),
            in_specs=[pl.BlockSpec((1,) + a.shape[1:], lambda i, g, m: (g[0], 0, 0)) for a in (bc_in, taps)]
            + [pl.BlockSpec(a.shape, lambda i, g, m: (0, 0)) for a in [x_in] + small],
            out_specs=[VMEM] * len(outs),
        ),
        out_shape=outs,
        name="load",
    )(group, member, bc_in, taps, x_in, *small)
    pay, xc, bcc, cum, less = run(
        state_kernel,
        [shape(LO, quarter + META, states, dtype=BF16), series, pairs, shape(heads, length), shape(heads, length)],
        x,
        bc,
        dt,
        x_taps,
        bc_taps,
        per_head,
        last,
        first,
    )

    def gather(opening=False):
        got = lax.all_to_all(pay, "near", 0, 0, tiled=True)
        kernel = lambda *refs: group_kernel(*refs, per=per, opening=opening)
        return tuple(run(kernel, kept_shapes + [block_shape], got, own_taps))

    def blank(*outs):
        return tuple(run(blank_kernel, list(outs)))

    def exchange(*given):
        (entering,) = run(lambda *refs: entering_kernel(*refs, per=per), [state_shape], *given)
        return lax.all_to_all(entering, "near", 0, 0, tiled=True)

    def sent(block, source, target):
        route = [(source * LO + i, target * LO + i) for i in range(LO)]
        return lax.ppermute(block, cp, route)

    def kept_on(*arrays):
        return tuple(run(copy_kernel, kept_shapes + [block_shape], *arrays))

    kept = lax.cond(far == 0, lambda: gather(True), lambda: blank(*kept_shapes, block_shape))
    near = sent(kept[2], 0, 1)
    *kept, begin = lax.switch(
        jnp.minimum(far, 2),
        [
            lambda *kept: blank(*kept_shapes, block_shape) + (exchange(*kept[:2]),),
            lambda *kept: gather() + blank(state_shape),
            lambda *kept: blank(*kept_shapes, block_shape, state_shape),
        ],
        *kept,
    )
    (joined,) = run(lambda *refs: join_kernel(*refs, per=per), [block_shape], near, kept[2], own_taps)
    next_one = sent(joined, 1, 2)
    over = sent(joined, 1, 3)
    kept = lax.cond(far >= 2, lambda *kept: gather(), kept_on, *kept)
    between = sent(kept[2], 2, 3)
    rims = lax.ppermute(last, cp, [(i, i + 1) for i in range(count - 1)])
    inner, c_rows = run(
        intra_kernel,
        [shape(channels, length), shape(states, length, dtype=BF16)],
        xc,
        bcc,
        rims,
        first,
        x_taps,
        bc_taps,
        cum,
        less,
        per_head,
    )
    state = lax.cond(
        far == 0,
        lambda begin, *unused: run(copy_kernel, [state_shape], begin)[0],
        lambda begin, *given: exchange(*given),
        begin,
        *kept[:2],
        own_taps,
        near,
        next_one,
        over,
        between,
    ).reshape(channels, states)
    out = jax.ShapeDtypeStruct((channels, length), BF16)
    return run(output_kernel, [out], inner, c_rows, cum, state, z_gate)[0]


def solution(mesh):
    dp, cp, tensor = mesh.devices.shape
    finer = Mesh(mesh.devices.reshape(dp, cp // LO, LO, tensor), ("dp", "far", "near", "tensor"))
    along = ("dp", "far", "near")
    return jax.shard_map(
        local,
        mesh=finer,
        in_specs=(
            P("tensor", along),
            P("tensor", along),
            P(None, None, along),
            P("tensor", along),
            P("tensor", None),
            P("tensor"),
            P(),
            P(),
            P("tensor"),
            P("tensor"),
            P("tensor"),
        ),
        out_specs=P("tensor", along),
        check_vma=False,
    )
```

```python
import jax
import jax.numpy as jnp
from jax import lax
from jax.experimental import pallas as pl
from jax.experimental.pallas import tpu as pltpu
from jax.sharding import Mesh, PartitionSpec as P


HEADS = 128
GROUPS = 8
GROUP_HEADS = HEADS // GROUPS
LO = 4
META = 32

F32 = jnp.float32
BF16 = jnp.bfloat16


def dot(a, b, ca, cb):
    return lax.dot_general(a, b, (((ca,), (cb,)), ((), ())), preferred_element_type=F32)


def silu(v):
    return v / (1.0 + jnp.exp(-v))


def log1p(u):
    return jnp.where(u < 1e-3, u * (1.0 - u * (0.5 - u * (1.0 / 3.0))), jnp.log(1.0 + u))


def softplus(v):
    return jnp.maximum(v, 0.0) + log1p(jnp.exp(-jnp.abs(v)))


def picks(first_lane):
    rows = lax.broadcasted_iota(jnp.int32, (8, 128), 0)
    lanes = lax.broadcasted_iota(jnp.int32, (8, 128), 1)
    return jnp.where(jnp.logical_and(lanes == rows + first_lane, rows < 3), 1.0, 0.0).astype(BF16)


def load_kernel(
    group, member, bc, bw, x, dt, xw, xb, bb, bias, a_log, skip,
    last, first, x_out, bc_out, dt_out, x_taps, bc_taps, own_taps, per_head,
):
    channels = x.shape[0]
    heads = dt.shape[0]
    begin, finish = picks(0), picks(125)
    series, mine = x[...], bc[0]
    last[:, :channels] = dot(finish, series[:, 128:], 1, 1).astype(BF16)
    last[:, channels:] = dot(finish, mine[:, 128:], 1, 1).astype(BF16)
    first[:, :channels] = dot(begin, series[:, :128], 1, 1).astype(BF16)
    first[:, channels:] = dot(begin, mine[:, :128], 1, 1).astype(BF16)
    x_out[...] = series
    bc_out[...] = mine
    dt_out[...] = dt[...]
    x_taps[:4, :] = xw[...]
    x_taps[4:, :] = jnp.broadcast_to(xb[...], (4, channels))
    own = jnp.zeros(own_taps.shape[1:], F32)
    for q in range(LO):
        own = jnp.where(member[0] == q, x_taps[:, q * 128 : (q + 1) * 128], own)
    own_taps[0] = own
    bc_taps[:4, :] = bw[0]
    bc_taps[4:, :] = jnp.broadcast_to(chosen(bb[...], group[0]), (4, mine.shape[0]))
    own_taps[1] = bc_taps[:, :128]
    for i, row in enumerate((bias, a_log, skip)):
        per_head[i] = jnp.broadcast_to(column(row[...]), (heads, 128))


def filtered(series, taps):
    lanes = lax.broadcasted_iota(jnp.int32, (series.shape[0], 128), 1)
    first, second = series[:, :128].astype(F32), series[:, 128:].astype(F32)
    a = taps[:, 4:5] + taps[:, 3:4] * first
    b = taps[:, 4:5] + taps[:, 3:4] * second
    for back in (1, 2, 3):
        moved = pltpu.roll(first, back, 1)
        tap = taps[:, 3 - back : 4 - back]
        a = a + tap * moved
        b = b + tap * jnp.where(lanes < back, moved, pltpu.roll(second, back, 1))
    return jnp.concatenate([silu(a), silu(b)], axis=1).astype(BF16)


def column(row):
    size = row.shape[1]
    same = lax.broadcasted_iota(jnp.int32, (size, size), 0) == lax.broadcasted_iota(jnp.int32, (size, size), 1)
    return jnp.sum(jnp.where(same, row, 0.0), axis=1, keepdims=True)


def chosen(table, group):
    rows = lax.broadcasted_iota(jnp.int32, table.shape, 0)
    return jnp.sum(jnp.where(rows == group, table, 0.0), axis=0, keepdims=True)


def split(value):
    high = value.astype(BF16)
    return high, (value - high.astype(F32)).astype(BF16)


def state_kernel(
    z, x, bc, dt, x_taps, bc_taps, per_head, last, first, pay, xc, bcc, cum_out, less_out, z_out, done
):
    fetch = pltpu.make_async_copy(z, z_out, done)
    fetch.start()
    channels = x.shape[0]
    heads = dt.shape[0]
    width = channels // heads
    states = bc.shape[0] // 2

    delta = softplus(dt[...].astype(F32) + per_head[0][:, :1])
    scaled = delta * -jnp.exp(per_head[1][:, :1])
    high = scaled.astype(BF16)
    mid, low = split(scaled - high.astype(F32))
    size = scaled.shape[1]
    upto = jnp.where(
        lax.broadcasted_iota(jnp.int32, (size, size), 0) <= lax.broadcasted_iota(jnp.int32, (size, size), 1), 1.0, 0.0
    ).astype(BF16)
    cum = dot(low, upto, 1, 0) + dot(mid, upto, 1, 0) + dot(high, upto, 1, 0)
    cum_out[...] = cum
    less_out[...] = cum - jnp.log(delta)
    end = cum[:, size - 1 :]
    gain = delta * jnp.exp(end - cum)
    total_high, total_low = split(jnp.exp(end))
    total_high, total_low = total_high.astype(F32), total_low.astype(F32)

    spread = jnp.where(
        lax.broadcasted_iota(jnp.int32, (heads, channels), 1) // width
        == lax.broadcasted_iota(jnp.int32, (heads, channels), 0),
        1.0,
        0.0,
    ).astype(BF16)
    gain_high, gain_low = split(gain[:, :128])
    lines = lax.broadcasted_iota(jnp.int32, (8, channels), 0)
    gains = jnp.where(lines < 4, dot(gain_high, spread, 0, 0)[:8], pltpu.roll(dot(gain_low, spread, 0, 0)[:8], 4, 0))
    lines = lax.broadcasted_iota(jnp.int32, last.shape, 0)
    edges = jnp.where(lines < 3, last[...].astype(F32), pltpu.roll(first[...].astype(F32), 3, 0))

    bcc[...] = filtered(bc[...], bc_taps[...].T)
    b_rows = bcc[:states, :]
    x_cols = x_taps[...].T
    late = jnp.where(lax.broadcasted_iota(jnp.int32, gain.shape, 1) < 3, 0.0, gain)
    lines = lax.broadcasted_iota(jnp.int32, (8, 128), 0)
    per = heads // LO
    for quarter in range(LO):
        tail = jnp.zeros((8, 128), F32)
        for j in range(per):
            h = quarter * per + j
            at = pl.ds(h * width, width)
            values = filtered(x[at, :], x_cols[h * width : (h + 1) * width])
            xc[at, :] = values
            weighted = (values.astype(F32) * late[h : h + 1]).astype(BF16)
            pay[quarter, pl.ds(j * width, width), :] = dot(weighted, b_rows, 1, 1).astype(BF16)
            tail = jnp.where(lines == 2 * j, total_high[h : h + 1], tail)
            tail = jnp.where(lines == 2 * j + 1, total_low[h : h + 1], tail)
        here = slice(quarter * 128, (quarter + 1) * 128)
        rows = jnp.concatenate([tail, edges[:, here], edges[:, channels : channels + 128], gains[:, here]], axis=0)
        pay[quarter, pl.ds(per * width, META), :] = rows.astype(BF16)
    fetch.wait()


def early(series, taps):
    rows = lax.broadcasted_iota(jnp.int32, series.shape, 0)
    total = taps[4:5] + taps[0:1] * series
    for k in (1, 2, 3):
        total = total + taps[k : k + 1] * pltpu.roll(series, 8 - k, 0)
    return jnp.where(rows < 3, silu(total), 0.0).astype(BF16)


def rim_state(before, after, taps):
    rows = lax.broadcasted_iota(jnp.int32, (8, 128), 0)
    x_rows = early(jnp.where(rows < 3, before[8:16], after[8:16]), taps[0])
    b_rows = early(jnp.where(rows < 3, before[16:24], after[16:24]), taps[1])
    gains = after[24:32] + pltpu.roll(after[24:32], 4, 0)
    return dot((x_rows.astype(F32) * gains).astype(BF16), b_rows, 0, 0)


def spread_rows(rows, start, per, size):
    width = size // per
    values = [rows[start + 2 * j : start + 2 * j + 1] + rows[start + 2 * j + 1 : start + 2 * j + 2] for j in range(per)]
    return jnp.concatenate([jnp.broadcast_to(v, (width, 128)) for v in values], axis=0)


def unpack(block):
    size = block.shape[0] - META
    return block[:size].astype(F32), block[size:].astype(F32)


def packed_rows(decay, start, rows, per):
    width = decay.shape[0] // per
    lines = lax.broadcasted_iota(jnp.int32, (8, 128), 0)
    for j in range(per):
        d = decay[j * width : j * width + 1]
        high = d.astype(BF16).astype(F32)
        rows = jnp.where(lines == start + 2 * j, high, rows)
        rows = jnp.where(lines == start + 2 * j + 1, d - high, rows)
    return rows


def group_kernel(got, taps, kept, meta, out, *blanks, per, opening):
    blank_kernel(*blanks)
    size = out.shape[0] - META
    members = [unpack(got[r]) for r in range(LO)]
    lines = lax.broadcasted_iota(jnp.int32, (META, 128), 0)
    state, rows = members[0]
    if opening:
        state = state + rim_state(jnp.zeros_like(rows), rows, taps)
    kept[0] = state
    decay = spread_rows(rows, 0, per, size)
    suffix = jnp.ones_like(decay)
    for r in range(1, LO):
        fresh, now = members[r]
        fresh = fresh + rim_state(members[r - 1][1], now, taps)
        kept[r] = fresh
        d = spread_rows(now, 0, per, size)
        state = fresh + d * state
        decay, suffix = decay * d, suffix * d
    meta[...] = got[:, size:, :]
    out[:size, :] = state.astype(BF16)
    head = packed_rows(suffix, 4, packed_rows(decay, 0, jnp.zeros((8, 128), F32), per), per)
    edge = lax.broadcasted_iota(jnp.int32, (16, 128), 0) % 8 < 3
    edges = jnp.where(edge, members[LO - 1][1][8:24], rows[8:24])
    out[size:, :] = jnp.concatenate([head, edges, rows[24:32]], axis=0).astype(BF16)


def join_kernel(earlier, later, taps, out, *, per):
    size = out.shape[0] - META
    before, rows_before = unpack(earlier[...])
    after, rows = unpack(later[...])
    opening = rim_state(rows_before, rows, taps)
    state = after + spread_rows(rows, 4, per, size) * opening + spread_rows(rows, 0, per, size) * before
    out[:size, :] = state.astype(BF16)
    out[size:, :] = later[size:, :]


def entering_kernel(kept, meta, *refs, per, blanks):
    blank_kernel(*refs[len(refs) - blanks :])
    *given, out = refs[: len(refs) - blanks]
    size = kept.shape[1]
    own = meta[0].astype(F32)
    fresh = kept[0]
    state = jnp.zeros(out.shape[1:], F32)
    if given:
        taps, near, next_one, over, between = given
        (near, rows_near), (next_one, rows_next) = unpack(near[...]), unpack(next_one[...])
        (over, rows_over), (between, rows) = unpack(over[...]), unpack(between[...])
        opening = rim_state(rows_over, rows, taps)
        state = between + spread_rows(rows, 4, per, size) * opening + spread_rows(rows, 0, per, size) * over
        state = state + near + next_one
        fresh = fresh + rim_state(rows_near + rows_next + rows, own, taps)
    out[0] = state.astype(BF16)
    for r in range(1, LO):
        state = fresh + spread_rows(meta[r - 1].astype(F32), 0, per, size) * state
        out[r] = state.astype(BF16)
        fresh = kept[r]


def copy_kernel(*refs):
    half = len(refs) // 2
    for source, target in zip(refs[:half], refs[half:]):
        target[...] = source[...]


def blank_kernel(*refs):
    for ref in refs:
        ref[...] = jnp.zeros(ref.shape, ref.dtype)


def intra_kernel(xc, bcc, rims, rims_high, first, x_taps, bc_taps, cum_in, less_in, per_head, out, c_out):
    heads = cum_in.shape[0]
    channels = xc.shape[0]
    width = channels // heads
    states = bcc.shape[0] // 2
    cum, less = cum_in[...], less_in[...]
    less_cols = jnp.concatenate([less[:, :128].T, less[:, 128:].T], axis=0)
    skips = per_head[2][:, :1]
    lines = lax.broadcasted_iota(jnp.int32, rims.shape, 0)
    given = rims[...].astype(F32) + rims_high[...].astype(F32)
    edges = jnp.where(lines < 3, given, pltpu.roll(first[...].astype(F32), 3, 0))
    begun = [early(edges[:, :channels], x_taps[...]), early(edges[:, channels:], bc_taps[...])]
    placed = dot(jnp.concatenate(begun, axis=1), picks(0), 0, 0).astype(BF16)

    def mended(values, rows):
        lanes = lax.broadcasted_iota(jnp.int32, rows.shape, 1)
        return jnp.concatenate([jnp.where(lanes < 3, rows, values[:, :128]), values[:, 128:]], axis=1)

    both = mended(bcc[...], placed[channels:])
    c_out[...] = both[states:]
    gram = dot(both[:states], both[states:], 0, 0)
    keep = lax.broadcasted_iota(jnp.int32, (128, 128), 0) <= lax.broadcasted_iota(jnp.int32, (128, 128), 1)
    for h in range(heads):
        at = pl.ds(h * width, width)
        values = mended(xc[at, :], placed[h * width : (h + 1) * width])
        row = cum[h : h + 1]
        col = less_cols[:, h : h + 1]

        def mix(s, t, masked):
            spread = row[:, t : t + 128] - col[s : s + 128]
            if masked:
                spread = jnp.where(keep, spread, -1e30)
            return (gram[s : s + 128, t : t + 128] * jnp.exp(spread)).astype(BF16)

        near = dot(values[:, :128], mix(0, 0, True), 1, 0)
        late = dot(values, jnp.concatenate([mix(0, 128, False), mix(128, 128, True)], axis=0), 1, 0)
        out[at, :] = jnp.concatenate([near, late], axis=1) + skips[h : h + 1] * values.astype(F32)


def output_kernel(inner, c_rows, cum, state, z, out, held, done):
    heads = cum.shape[0]
    width = inner.shape[0] // heads
    per = heads // LO
    grown = jnp.exp(cum[...])
    copies = []
    for h in range(heads):
        at = pl.ds(h * width, width)
        y = inner[at, :] + grown[h : h + 1] * dot(state[at, :], c_rows[...], 1, 0)
        y = y.astype(BF16).astype(F32)
        held[at, :] = (y * silu(z[at, :].astype(F32))).astype(BF16)
        if h % per == per - 1:
            part = pl.ds((h + 1 - per) * width, per * width)
            copies.append(pltpu.make_async_copy(held.at[part], out.at[part], done.at[h // per]))
            copies[-1].start()
    for copy in copies:
        copy.wait()


def shape(*dims, dtype=F32):
    return pltpu.VMEM(dims, dtype)


VMEM = pl.BlockSpec(memory_space=pltpu.VMEM)


def run(kernel, outs, *args):
    args = [pltpu.with_memory_space_constraint(a, pltpu.VMEM) for a in args]
    return pl.pallas_call(kernel, out_shape=outs, in_specs=[VMEM] * len(args), out_specs=[VMEM] * len(outs))(*args)


def local(x_in, z_gate, bc_in, dt_raw, conv_x_w, conv_x_b, conv_bc_w, conv_bc_b, dt_bias, a_log, d_skip):
    heads, length = dt_raw.shape
    channels = x_in.shape[0]
    rows = bc_in.shape[1]
    states = rows // 2
    per = heads // LO
    quarter = channels // LO
    group = (lax.axis_index("tensor") // (GROUP_HEADS // heads)).astype(jnp.int32).reshape(1)
    member = lax.axis_index("near").astype(jnp.int32).reshape(1)
    far = lax.axis_index("far")
    cp = ("far", "near")
    count = lax.axis_size(cp)

    strip = shape(8, channels + rows, dtype=BF16)
    block_shape = shape(quarter + META, states, dtype=BF16)
    kept_shapes = [shape(LO, quarter, states), shape(LO, META, states, dtype=BF16)]
    state_shape = shape(LO, quarter, states, dtype=BF16)
    series = shape(channels, length, dtype=BF16)
    pairs = shape(rows, length, dtype=BF16)
    taps = jnp.swapaxes(conv_bc_w, 1, 2)
    small = [dt_raw, conv_x_w.T, conv_x_b[None], conv_bc_b, dt_bias[None], a_log[None], d_skip[None]]
    outs = [strip, strip, series, pairs, shape(heads, length, dtype=BF16), shape(8, channels), shape(8, rows)]
    outs += [shape(2, 8, 128), shape(3, heads, 128)]
    last, first, x, bc, dt, x_taps, bc_taps, own_taps, per_head = pl.pallas_call(
        load_kernel,
        grid_spec=pltpu.PrefetchScalarGridSpec(
            num_scalar_prefetch=2,
            grid=(1,),
            in_specs=[pl.BlockSpec((1,) + a.shape[1:], lambda i, g, m: (g[0], 0, 0)) for a in (bc_in, taps)]
            + [pl.BlockSpec(a.shape, lambda i, g, m: (0, 0)) for a in [x_in] + small],
            out_specs=[VMEM] * len(outs),
        ),
        out_shape=outs,
        name="load",
    )(group, member, bc_in, taps, x_in, *small)
    inputs = [pltpu.with_memory_space_constraint(a, pltpu.VMEM) for a in (x, bc, dt, x_taps, bc_taps, per_head, last, first)]
    outs = [shape(LO, quarter + META, states, dtype=BF16), series, pairs]
    outs += [shape(heads, length), shape(heads, length), series]
    pay, xc, bcc, cum, less, z = pl.pallas_call(
        state_kernel,
        out_shape=outs,
        in_specs=[pl.BlockSpec(memory_space=pl.ANY)] + [VMEM] * len(inputs),
        out_specs=[VMEM] * len(outs),
        scratch_shapes=[pltpu.SemaphoreType.DMA],
        name="states",
    )(z_gate, *inputs)

    def gather(*blanks, opening=False):
        got = lax.all_to_all(pay, "near", 0, 0, tiled=True)
        kernel = lambda *refs: group_kernel(*refs, per=per, opening=opening)
        return tuple(run(kernel, kept_shapes + [block_shape, *blanks], got, own_taps))

    def blank(*outs):
        return tuple(run(blank_kernel, list(outs)))

    def exchange(*given, blanks=()):
        kernel = lambda *refs: entering_kernel(*refs, per=per, blanks=len(blanks))
        entering, *rest = run(kernel, [state_shape, *blanks], *given)
        return tuple(rest) + (lax.all_to_all(entering, "near", 0, 0, tiled=True),)

    def sent(block, source, target):
        route = [(source * LO + i, target * LO + i) for i in range(LO)]
        return lax.ppermute(block, cp, route)

    def kept_on(*arrays):
        return tuple(run(copy_kernel, [shape(*a.shape, dtype=a.dtype) for a in arrays], *arrays))

    kept = lax.cond(far == 0, lambda: gather(opening=True), lambda: blank(*kept_shapes, block_shape))
    near = sent(kept[2], 0, 1)
    rims_low = lax.ppermute(last, cp, [(i, i + 1) for i in range(2 * LO - 1)])
    *kept, begin = lax.switch(
        jnp.minimum(far, 2),
        [
            lambda *kept: exchange(*kept[:2], blanks=(*kept_shapes, block_shape)),
            lambda *kept: gather(state_shape),
            lambda *kept: blank(*kept_shapes, block_shape, state_shape),
        ],
        *kept,
    )
    (joined,) = run(lambda *refs: join_kernel(*refs, per=per), [block_shape], near, kept[2], own_taps)
    over = sent(joined, 1, 3)
    next_one = sent(joined, 1, 2)
    kept = lax.cond(far == 2, lambda *kept: gather(), kept_on, *kept)
    between = sent(kept[2], 2, 3)
    kept = lax.cond(far == 3, lambda *kept: gather()[:2], kept_on, *kept[:2])
    *kept, last = lax.optimization_barrier((*kept, last))
    rims_high = lax.ppermute(last, cp, [(i, i + 1) for i in range(2 * LO - 1, count - 1)])
    inner, c_rows = run(
        intra_kernel,
        [shape(channels, length), shape(states, length, dtype=BF16)],
        xc,
        bcc,
        rims_low,
        rims_high,
        first,
        x_taps,
        bc_taps,
        cum,
        less,
        per_head,
    )
    (state,) = lax.cond(
        far == 0,
        lambda begin, *unused: tuple(run(copy_kernel, [state_shape], begin)),
        lambda begin, *given: exchange(*given),
        begin,
        *kept,
        own_taps,
        near,
        next_one,
        over,
        between,
    )
    inputs = [inner, c_rows, cum, state.reshape(channels, states), z]
    return pl.pallas_call(
        output_kernel,
        out_shape=jax.ShapeDtypeStruct((channels, length), BF16),
        in_specs=[VMEM] * len(inputs),
        out_specs=pl.BlockSpec(memory_space=pl.ANY),
        scratch_shapes=[pltpu.VMEM((channels, length), BF16), pltpu.SemaphoreType.DMA((LO,))],
        name="gated",
    )(*[pltpu.with_memory_space_constraint(a, pltpu.VMEM) for a in inputs])


def solution(mesh):
    dp, cp, tensor = mesh.devices.shape
    finer = Mesh(mesh.devices.reshape(dp, cp // LO, LO, tensor), ("dp", "far", "near", "tensor"))
    along = ("dp", "far", "near")
    return jax.shard_map(
        local,
        mesh=finer,
        in_specs=(
            P("tensor", along),
            P("tensor", along),
            P(None, None, along),
            P("tensor", along),
            P("tensor", None),
            P("tensor"),
            P(),
            P(),
            P("tensor"),
            P("tensor"),
            P("tensor"),
        ),
        out_specs=P("tensor", along),
        check_vma=False,
    )
```

```python
import jax
import jax.numpy as jnp
from jax import lax
from jax.experimental import pallas as pl
from jax.experimental.pallas import tpu as pltpu
from jax.sharding import Mesh, PartitionSpec as P


HEADS = 128
GROUPS = 8
GROUP_HEADS = HEADS // GROUPS
LO = 4
META = 32

F32 = jnp.float32
BF16 = jnp.bfloat16


def dot(a, b, ca, cb):
    return lax.dot_general(a, b, (((ca,), (cb,)), ((), ())), preferred_element_type=F32)


def silu(v):
    return v / (1.0 + jnp.exp(-v))


def log1p(u):
    return jnp.where(u < 1e-3, u * (1.0 - u * (0.5 - u * (1.0 / 3.0))), jnp.log(1.0 + u))


def softplus(v):
    return jnp.maximum(v, 0.0) + log1p(jnp.exp(-jnp.abs(v)))


def picks(first_lane):
    rows = lax.broadcasted_iota(jnp.int32, (8, 128), 0)
    lanes = lax.broadcasted_iota(jnp.int32, (8, 128), 1)
    return jnp.where(jnp.logical_and(lanes == rows + first_lane, rows < 3), 1.0, 0.0).astype(BF16)


def load_kernel(
    group, member, bc, bw, x, dt, xw, xb, bb, bias, a_log, skip,
    last, first, x_out, bc_out, dt_out, x_taps, bc_taps, own_taps, per_head,
):
    channels = x.shape[0]
    heads = dt.shape[0]
    begin, finish = picks(0), picks(125)
    series, mine = x[...], bc[0]
    last[:, :channels] = dot(finish, series[:, 128:], 1, 1).astype(BF16)
    last[:, channels:] = dot(finish, mine[:, 128:], 1, 1).astype(BF16)
    first[:, :channels] = dot(begin, series[:, :128], 1, 1).astype(BF16)
    first[:, channels:] = dot(begin, mine[:, :128], 1, 1).astype(BF16)
    x_out[...] = series
    bc_out[...] = mine
    dt_out[...] = dt[...]
    x_taps[:4, :] = xw[...]
    x_taps[4:, :] = jnp.broadcast_to(xb[...], (4, channels))
    own = jnp.zeros(own_taps.shape[1:], F32)
    for q in range(LO):
        own = jnp.where(member[0] == q, x_taps[:, q * 128 : (q + 1) * 128], own)
    own_taps[0] = own
    bc_taps[:4, :] = bw[0]
    bc_taps[4:, :] = jnp.broadcast_to(chosen(bb[...], group[0]), (4, mine.shape[0]))
    own_taps[1] = bc_taps[:, :128]
    for i, row in enumerate((bias, a_log, skip)):
        per_head[i] = jnp.broadcast_to(column(row[...]), (heads, 128))


def filtered(series, taps):
    lanes = lax.broadcasted_iota(jnp.int32, (series.shape[0], 128), 1)
    first, second = series[:, :128].astype(F32), series[:, 128:].astype(F32)
    a = taps[:, 4:5] + taps[:, 3:4] * first
    b = taps[:, 4:5] + taps[:, 3:4] * second
    for back in (1, 2, 3):
        moved = pltpu.roll(first, back, 1)
        tap = taps[:, 3 - back : 4 - back]
        a = a + tap * moved
        b = b + tap * jnp.where(lanes < back, moved, pltpu.roll(second, back, 1))
    return jnp.concatenate([silu(a), silu(b)], axis=1).astype(BF16)


def column(row):
    size = row.shape[1]
    same = lax.broadcasted_iota(jnp.int32, (size, size), 0) == lax.broadcasted_iota(jnp.int32, (size, size), 1)
    return jnp.sum(jnp.where(same, row, 0.0), axis=1, keepdims=True)


def chosen(table, group):
    rows = lax.broadcasted_iota(jnp.int32, table.shape, 0)
    return jnp.sum(jnp.where(rows == group, table, 0.0), axis=0, keepdims=True)


def split(value):
    high = value.astype(BF16)
    return high, (value - high.astype(F32)).astype(BF16)


def state_kernel(
    z, x, bc, dt, x_taps, bc_taps, per_head, last, first, pay, xc, bcc, cum_out, less_out, z_out, done
):
    fetch = pltpu.make_async_copy(z, z_out, done)
    fetch.start()
    channels = x.shape[0]
    heads = dt.shape[0]
    width = channels // heads
    states = bc.shape[0] // 2

    delta = softplus(dt[...].astype(F32) + per_head[0][:, :1])
    scaled = delta * -jnp.exp(per_head[1][:, :1])
    high = scaled.astype(BF16)
    mid, low = split(scaled - high.astype(F32))
    size = scaled.shape[1]
    upto = jnp.where(
        lax.broadcasted_iota(jnp.int32, (size, size), 0) <= lax.broadcasted_iota(jnp.int32, (size, size), 1), 1.0, 0.0
    ).astype(BF16)
    cum = dot(low, upto, 1, 0) + dot(mid, upto, 1, 0) + dot(high, upto, 1, 0)
    cum_out[...] = cum
    less_out[...] = cum - jnp.log(delta)
    end = cum[:, size - 1 :]
    gain = delta * jnp.exp(end - cum)
    total_high, total_low = split(jnp.exp(end))
    total_high, total_low = total_high.astype(F32), total_low.astype(F32)

    spread = jnp.where(
        lax.broadcasted_iota(jnp.int32, (heads, channels), 1) // width
        == lax.broadcasted_iota(jnp.int32, (heads, channels), 0),
        1.0,
        0.0,
    ).astype(BF16)
    gain_high, gain_low = split(gain[:, :128])
    lines = lax.broadcasted_iota(jnp.int32, (8, channels), 0)
    gains = jnp.where(lines < 4, dot(gain_high, spread, 0, 0)[:8], pltpu.roll(dot(gain_low, spread, 0, 0)[:8], 4, 0))
    lines = lax.broadcasted_iota(jnp.int32, last.shape, 0)
    edges = jnp.where(lines < 3, last[...].astype(F32), pltpu.roll(first[...].astype(F32), 3, 0))

    bcc[...] = filtered(bc[...], bc_taps[...].T)
    b_rows = bcc[:states, :]
    x_cols = x_taps[...].T
    late = jnp.where(lax.broadcasted_iota(jnp.int32, gain.shape, 1) < 3, 0.0, gain)
    lines = lax.broadcasted_iota(jnp.int32, (8, 128), 0)
    per = heads // LO
    for quarter in range(LO):
        tail = jnp.zeros((8, 128), F32)
        for j in range(per):
            h = quarter * per + j
            at = pl.ds(h * width, width)
            values = filtered(x[at, :], x_cols[h * width : (h + 1) * width])
            xc[at, :] = values
            weighted = (values.astype(F32) * late[h : h + 1]).astype(BF16)
            pay[quarter, pl.ds(j * width, width), :] = dot(weighted, b_rows, 1, 1).astype(BF16)
            tail = jnp.where(lines == 2 * j, total_high[h : h + 1], tail)
            tail = jnp.where(lines == 2 * j + 1, total_low[h : h + 1], tail)
        here = slice(quarter * 128, (quarter + 1) * 128)
        rows = jnp.concatenate([tail, edges[:, here], edges[:, channels : channels + 128], gains[:, here]], axis=0)
        pay[quarter, pl.ds(per * width, META), :] = rows.astype(BF16)
    fetch.wait()


def early(series, taps):
    rows = lax.broadcasted_iota(jnp.int32, series.shape, 0)
    total = taps[4:5] + taps[0:1] * series
    for k in (1, 2, 3):
        total = total + taps[k : k + 1] * pltpu.roll(series, 8 - k, 0)
    return jnp.where(rows < 3, silu(total), 0.0).astype(BF16)


def rim_state(before, after, taps):
    rows = lax.broadcasted_iota(jnp.int32, (8, 128), 0)
    x_rows = early(jnp.where(rows < 3, before[8:16], after[8:16]), taps[0])
    b_rows = early(jnp.where(rows < 3, before[16:24], after[16:24]), taps[1])
    gains = after[24:32] + pltpu.roll(after[24:32], 4, 0)
    return dot((x_rows.astype(F32) * gains).astype(BF16), b_rows, 0, 0)


def spread_rows(rows, start, per, size):
    width = size // per
    values = [rows[start + 2 * j : start + 2 * j + 1] + rows[start + 2 * j + 1 : start + 2 * j + 2] for j in range(per)]
    return jnp.concatenate([jnp.broadcast_to(v, (width, 128)) for v in values], axis=0)


def unpack(block):
    size = block.shape[0] - META
    return block[:size].astype(F32), block[size:].astype(F32)


def packed_rows(decay, start, rows, per):
    width = decay.shape[0] // per
    lines = lax.broadcasted_iota(jnp.int32, (8, 128), 0)
    for j in range(per):
        d = decay[j * width : j * width + 1]
        high = d.astype(BF16).astype(F32)
        rows = jnp.where(lines == start + 2 * j, high, rows)
        rows = jnp.where(lines == start + 2 * j + 1, d - high, rows)
    return rows


def group_kernel(got, taps, kept, meta, *refs, per, opening):
    blank_kernel(*refs[1:])
    size = kept.shape[1]
    members = [unpack(got[r]) for r in range(LO)]
    lines = lax.broadcasted_iota(jnp.int32, (META, 128), 0)
    state, rows = members[0]
    if opening:
        state = state + rim_state(jnp.zeros_like(rows), rows, taps)
    kept[0] = state
    decay = spread_rows(rows, 0, per, size)
    suffix = jnp.ones_like(decay)
    for r in range(1, LO):
        fresh, now = members[r]
        fresh = fresh + rim_state(members[r - 1][1], now, taps)
        kept[r] = fresh
        d = spread_rows(now, 0, per, size)
        state = fresh + d * state
        decay, suffix = decay * d, suffix * d
    meta[...] = got[:, size:, :]
    if not refs:
        return
    out = refs[0]
    out[:size, :] = state.astype(BF16)
    head = packed_rows(suffix, 4, packed_rows(decay, 0, jnp.zeros((8, 128), F32), per), per)
    edge = lax.broadcasted_iota(jnp.int32, (16, 128), 0) % 8 < 3
    edges = jnp.where(edge, members[LO - 1][1][8:24], rows[8:24])
    out[size:, :] = jnp.concatenate([head, edges, rows[24:32]], axis=0).astype(BF16)


def join_kernel(earlier, later, taps, out, *, per):
    size = out.shape[0] - META
    before, rows_before = unpack(earlier[...])
    after, rows = unpack(later[...])
    opening = rim_state(rows_before, rows, taps)
    state = after + spread_rows(rows, 4, per, size) * opening + spread_rows(rows, 0, per, size) * before
    out[:size, :] = state.astype(BF16)
    out[size:, :] = later[size:, :]


def entering_kernel(kept, meta, *refs, per, blanks):
    blank_kernel(*refs[len(refs) - blanks :])
    *given, out = refs[: len(refs) - blanks]
    size = kept.shape[1]
    own = meta[0].astype(F32)
    fresh = kept[0]
    state = jnp.zeros(out.shape[1:], F32)
    if given:
        taps, near, next_one, over, between = given
        (near, rows_near), (next_one, rows_next) = unpack(near[...]), unpack(next_one[...])
        (over, rows_over), (between, rows) = unpack(over[...]), unpack(between[...])
        opening = rim_state(rows_over, rows, taps)
        state = between + spread_rows(rows, 4, per, size) * opening + spread_rows(rows, 0, per, size) * over
        state = state + near + next_one
        fresh = fresh + rim_state(rows_near + rows_next + rows, own, taps)
    out[0] = state.astype(BF16)
    for r in range(1, LO):
        state = fresh + spread_rows(meta[r - 1].astype(F32), 0, per, size) * state
        out[r] = state.astype(BF16)
        fresh = kept[r]


def copy_kernel(*refs):
    half = len(refs) // 2
    for source, target in zip(refs[:half], refs[half:]):
        target[...] = source[...]


def blank_kernel(*refs):
    for ref in refs:
        ref[...] = jnp.zeros(ref.shape, ref.dtype)


def intra_kernel(*refs, count):
    rims, (xc, bcc, first, x_taps, bc_taps, cum_in, less_in, per_head, out, c_out) = refs[:count], refs[count:]
    heads = cum_in.shape[0]
    channels = xc.shape[0]
    width = channels // heads
    states = bcc.shape[0] // 2
    cum, less = cum_in[...], less_in[...]
    less_cols = jnp.concatenate([less[:, :128].T, less[:, 128:].T], axis=0)
    skips = per_head[2][:, :1]
    lines = lax.broadcasted_iota(jnp.int32, first.shape, 0)
    given = sum(r[...].astype(F32) for r in rims)
    edges = jnp.where(lines < 3, given, pltpu.roll(first[...].astype(F32), 3, 0))
    begun = [early(edges[:, :channels], x_taps[...]), early(edges[:, channels:], bc_taps[...])]
    placed = dot(jnp.concatenate(begun, axis=1), picks(0), 0, 0).astype(BF16)

    def mended(values, rows):
        lanes = lax.broadcasted_iota(jnp.int32, rows.shape, 1)
        return jnp.concatenate([jnp.where(lanes < 3, rows, values[:, :128]), values[:, 128:]], axis=1)

    both = mended(bcc[...], placed[channels:])
    c_out[...] = both[states:]
    gram = dot(both[:states], both[states:], 0, 0)
    keep = lax.broadcasted_iota(jnp.int32, (128, 128), 0) <= lax.broadcasted_iota(jnp.int32, (128, 128), 1)
    for h in range(heads):
        at = pl.ds(h * width, width)
        values = mended(xc[at, :], placed[h * width : (h + 1) * width])
        row = cum[h : h + 1]
        col = less_cols[:, h : h + 1]

        def mix(s, t, masked):
            spread = row[:, t : t + 128] - col[s : s + 128]
            if masked:
                spread = jnp.where(keep, spread, -1e30)
            return (gram[s : s + 128, t : t + 128] * jnp.exp(spread)).astype(BF16)

        near = dot(values[:, :128], mix(0, 0, True), 1, 0)
        late = dot(values, jnp.concatenate([mix(0, 128, False), mix(128, 128, True)], axis=0), 1, 0)
        out[at, :] = jnp.concatenate([near, late], axis=1) + skips[h : h + 1] * values.astype(F32)


def output_kernel(inner, c_rows, cum, state, z, out, held, done):
    heads = cum.shape[0]
    width = inner.shape[0] // heads
    per = heads // LO
    grown = jnp.exp(cum[...])
    copies = []
    for h in range(heads):
        at = pl.ds(h * width, width)
        y = inner[at, :] + grown[h : h + 1] * dot(state[at, :], c_rows[...], 1, 0)
        y = y.astype(BF16).astype(F32)
        held[at, :] = (y * silu(z[at, :].astype(F32))).astype(BF16)
        if h % per == per - 1:
            part = pl.ds((h + 1 - per) * width, per * width)
            copies.append(pltpu.make_async_copy(held.at[part], out.at[part], done.at[h // per]))
            copies[-1].start()
    for copy in copies:
        copy.wait()


def shape(*dims, dtype=F32):
    return pltpu.VMEM(dims, dtype)


VMEM = pl.BlockSpec(memory_space=pltpu.VMEM)


def run(kernel, outs, *args):
    args = [pltpu.with_memory_space_constraint(a, pltpu.VMEM) for a in args]
    return pl.pallas_call(kernel, out_shape=outs, in_specs=[VMEM] * len(args), out_specs=[VMEM] * len(outs))(*args)


def local(x_in, z_gate, bc_in, dt_raw, conv_x_w, conv_x_b, conv_bc_w, conv_bc_b, dt_bias, a_log, d_skip):
    heads, length = dt_raw.shape
    channels = x_in.shape[0]
    rows = bc_in.shape[1]
    states = rows // 2
    per = heads // LO
    quarter = channels // LO
    group = (lax.axis_index("tensor") // (GROUP_HEADS // heads)).astype(jnp.int32).reshape(1)
    member = lax.axis_index("near").astype(jnp.int32).reshape(1)
    far = lax.axis_index("far")
    cp = ("far", "near")
    count = lax.axis_size(cp)

    strip = shape(8, channels + rows, dtype=BF16)
    block_shape = shape(quarter + META, states, dtype=BF16)
    kept_shapes = [shape(LO, quarter, states), shape(LO, META, states, dtype=BF16)]
    state_shape = shape(LO, quarter, states, dtype=BF16)
    series = shape(channels, length, dtype=BF16)
    pairs = shape(rows, length, dtype=BF16)
    taps = jnp.swapaxes(conv_bc_w, 1, 2)
    small = [dt_raw, conv_x_w.T, conv_x_b[None], conv_bc_b, dt_bias[None], a_log[None], d_skip[None]]
    outs = [strip, strip, series, pairs, shape(heads, length, dtype=BF16), shape(8, channels), shape(8, rows)]
    outs += [shape(2, 8, 128), shape(3, heads, 128)]
    last, first, x, bc, dt, x_taps, bc_taps, own_taps, per_head = pl.pallas_call(
        load_kernel,
        grid_spec=pltpu.PrefetchScalarGridSpec(
            num_scalar_prefetch=2,
            grid=(1,),
            in_specs=[pl.BlockSpec((1,) + a.shape[1:], lambda i, g, m: (g[0], 0, 0)) for a in (bc_in, taps)]
            + [pl.BlockSpec(a.shape, lambda i, g, m: (0, 0)) for a in [x_in] + small],
            out_specs=[VMEM] * len(outs),
        ),
        out_shape=outs,
        name="load",
    )(group, member, bc_in, taps, x_in, *small)
    inputs = [pltpu.with_memory_space_constraint(a, pltpu.VMEM) for a in (x, bc, dt, x_taps, bc_taps, per_head, last, first)]
    outs = [shape(LO, quarter + META, states, dtype=BF16), series, pairs]
    outs += [shape(heads, length), shape(heads, length), series]
    pay, xc, bcc, cum, less, z = pl.pallas_call(
        state_kernel,
        out_shape=outs,
        in_specs=[pl.BlockSpec(memory_space=pl.ANY)] + [VMEM] * len(inputs),
        out_specs=[VMEM] * len(outs),
        scratch_shapes=[pltpu.SemaphoreType.DMA],
        name="states",
    )(z_gate, *inputs)

    def gather(*rest, opening=False):
        got = lax.all_to_all(pay, "near", 0, 0, tiled=True)
        kernel = lambda *refs: group_kernel(*refs, per=per, opening=opening)
        return tuple(run(kernel, [*kept_shapes, *rest], got, own_taps))

    def blank(*outs):
        return tuple(run(blank_kernel, list(outs)))

    def exchange(*given, blanks=()):
        kernel = lambda *refs: entering_kernel(*refs, per=per, blanks=len(blanks))
        entering, *rest = run(kernel, [state_shape, *blanks], *given)
        return tuple(rest) + (lax.all_to_all(entering, "near", 0, 0, tiled=True),)

    def sent(block, source, target):
        route = [(source * LO + i, target * LO + i) for i in range(LO)]
        return lax.ppermute(block, cp, route)

    def kept_on(*arrays):
        return tuple(run(copy_kernel, [shape(*a.shape, dtype=a.dtype) for a in arrays], *arrays))

    def inside(*rims):
        outs = [shape(channels, length), shape(states, length, dtype=BF16)]
        args = (first, x_taps, bc_taps, cum, less, per_head)
        kernel = lambda *refs: intra_kernel(*refs, count=len(rims))
        return tuple(run(kernel, outs, *rims, xc, bcc, *args))

    def shifted(begin, end):
        return lax.ppermute(kept_on(last)[0], cp, [(i, i + 1) for i in range(begin, end)])

    inner_shapes = [shape(channels, length), shape(states, length, dtype=BF16)]

    def low_part():
        kept = lax.cond(
            far == 0, lambda: gather(block_shape, opening=True), lambda: blank(*kept_shapes, block_shape)
        )
        near = sent(kept[2], 0, 1)
        rims = shifted(0, 2 * LO - 1)
        *kept, begin = lax.cond(
            far == 0,
            lambda *kept: exchange(*kept[:2], blanks=(*kept_shapes, block_shape)),
            lambda *kept: gather(block_shape, state_shape),
            *kept,
        )
        inner = inside(rims)
        (joined,) = run(lambda *refs: join_kernel(*refs, per=per), [block_shape], near, kept[2], own_taps)
        kept, meta, near, begin = kept_on(*kept[:2], near, begin)
        return (kept, meta, joined, near, begin, *inner)

    def high_part(*kept):
        rims = shifted(2 * LO, count - 1)
        kept = lax.cond(far == 2, lambda *kept: gather(block_shape), lambda *kept: blank(*kept_shapes, block_shape), *kept)
        between = sent(kept[2], 2, 3)
        kept = lax.cond(far == 3, lambda *kept: gather(), kept_on, *kept[:2])
        return kept_on(*kept, between, rims)

    def later_part(kept, meta, joined, near, begin, *inner):
        (joined,) = kept_on(joined)
        over = sent(joined, 1, 3)
        next_one = sent(joined, 1, 2)
        rims_mid = shifted(2 * LO - 1, 2 * LO)
        *kept, between, rims = lax.cond(
            far >= 2, high_part, lambda *kept: kept_on(*kept) + blank(block_shape, strip), kept, meta
        )
        inner = lax.cond(
            far >= 2, lambda rims, rims_mid, *inner: inside(rims, rims_mid),
            lambda rims, rims_mid, *inner: kept_on(*inner), rims, rims_mid, *inner
        )
        between, *inner = lax.optimization_barrier((between, *inner))
        (state,) = exchange(*kept_on(*kept), own_taps, near, next_one, over, between)
        return (state, *inner)

    parts = lax.cond(
        far < 2, low_part, lambda: blank(*kept_shapes, block_shape, block_shape, state_shape, *inner_shapes)
    )
    parts = list(parts)
    parts[2], parts[4] = kept_on(parts[2], parts[4])
    state, inner, c_rows = lax.cond(far == 0, lambda *parts: kept_on(*parts[4:]), later_part, *parts)
    inputs = [inner, c_rows, cum, state.reshape(channels, states), z]
    return pl.pallas_call(
        output_kernel,
        out_shape=jax.ShapeDtypeStruct((channels, length), BF16),
        in_specs=[VMEM] * len(inputs),
        out_specs=pl.BlockSpec(memory_space=pl.ANY),
        scratch_shapes=[pltpu.VMEM((channels, length), BF16), pltpu.SemaphoreType.DMA((LO,))],
        name="gated",
    )(*[pltpu.with_memory_space_constraint(a, pltpu.VMEM) for a in inputs])


def solution(mesh):
    dp, cp, tensor = mesh.devices.shape
    finer = Mesh(mesh.devices.reshape(dp, cp // LO, LO, tensor), ("dp", "far", "near", "tensor"))
    along = ("dp", "far", "near")
    return jax.shard_map(
        local,
        mesh=finer,
        in_specs=(
            P("tensor", along),
            P("tensor", along),
            P(None, None, along),
            P("tensor", along),
            P("tensor", None),
            P("tensor"),
            P(),
            P(),
            P("tensor"),
            P("tensor"),
            P("tensor"),
        ),
        out_specs=P("tensor", along),
        check_vma=False,
    )
```

```python
import jax
import jax.numpy as jnp
from jax import lax
from jax.experimental import pallas as pl
from jax.experimental.pallas import tpu as pltpu
from jax.sharding import Mesh, PartitionSpec as P


HEADS = 128
GROUPS = 8
GROUP_HEADS = HEADS // GROUPS
LO = 4
META = 32

F32 = jnp.float32
BF16 = jnp.bfloat16


def dot(a, b, ca, cb):
    return lax.dot_general(a, b, (((ca,), (cb,)), ((), ())), preferred_element_type=F32)


def silu(v):
    return v / (1.0 + jnp.exp(-v))


def log1p(u):
    return jnp.where(u < 1e-3, u * (1.0 - u * (0.5 - u * (1.0 / 3.0))), jnp.log(1.0 + u))


def softplus(v):
    return jnp.maximum(v, 0.0) + log1p(jnp.exp(-jnp.abs(v)))


def picks(first_lane):
    rows = lax.broadcasted_iota(jnp.int32, (8, 128), 0)
    lanes = lax.broadcasted_iota(jnp.int32, (8, 128), 1)
    return jnp.where(jnp.logical_and(lanes == rows + first_lane, rows < 3), 1.0, 0.0).astype(BF16)


def load_kernel(
    group, member, bc, bw, x, dt, xw, xb, bb, bias, a_log, skip,
    last, first, x_out, bc_out, dt_out, x_taps, bc_taps, own_taps, per_head,
):
    channels = x.shape[0]
    heads = dt.shape[0]
    begin, finish = picks(0), picks(125)
    series, mine = x[...], bc[0]
    last[:, :channels] = dot(finish, series[:, 128:], 1, 1).astype(BF16)
    last[:, channels:] = dot(finish, mine[:, 128:], 1, 1).astype(BF16)
    first[:, :channels] = dot(begin, series[:, :128], 1, 1).astype(BF16)
    first[:, channels:] = dot(begin, mine[:, :128], 1, 1).astype(BF16)
    x_out[...] = series
    bc_out[...] = mine
    dt_out[...] = dt[...]
    x_taps[:4, :] = xw[...]
    x_taps[4:, :] = jnp.broadcast_to(xb[...], (4, channels))
    own = jnp.zeros(own_taps.shape[1:], F32)
    for q in range(LO):
        own = jnp.where(member[0] == q, x_taps[:, q * 128 : (q + 1) * 128], own)
    own_taps[0] = own
    bc_taps[:4, :] = bw[0]
    bc_taps[4:, :] = jnp.broadcast_to(chosen(bb[...], group[0]), (4, mine.shape[0]))
    own_taps[1] = bc_taps[:, :128]
    for i, row in enumerate((bias, a_log, skip)):
        per_head[i] = jnp.broadcast_to(column(row[...]), (heads, 128))


def filtered(series, taps):
    lanes = lax.broadcasted_iota(jnp.int32, (series.shape[0], 128), 1)
    first, second = series[:, :128].astype(F32), series[:, 128:].astype(F32)
    a = taps[:, 4:5] + taps[:, 3:4] * first
    b = taps[:, 4:5] + taps[:, 3:4] * second
    for back in (1, 2, 3):
        moved = pltpu.roll(first, back, 1)
        tap = taps[:, 3 - back : 4 - back]
        a = a + tap * moved
        b = b + tap * jnp.where(lanes < back, moved, pltpu.roll(second, back, 1))
    return jnp.concatenate([silu(a), silu(b)], axis=1).astype(BF16)


def column(row):
    size = row.shape[1]
    same = lax.broadcasted_iota(jnp.int32, (size, size), 0) == lax.broadcasted_iota(jnp.int32, (size, size), 1)
    return jnp.sum(jnp.where(same, row, 0.0), axis=1, keepdims=True)


def chosen(table, group):
    rows = lax.broadcasted_iota(jnp.int32, table.shape, 0)
    return jnp.sum(jnp.where(rows == group, table, 0.0), axis=0, keepdims=True)


def split(value):
    high = value.astype(BF16)
    return high, (value - high.astype(F32)).astype(BF16)


def state_kernel(x, bc, dt, x_taps, bc_taps, per_head, last, first, pay, xc, bcc, cum_out, less_out):
    channels = x.shape[0]
    heads = dt.shape[0]
    width = channels // heads
    states = bc.shape[0] // 2

    delta = softplus(dt[...].astype(F32) + per_head[0][:, :1])
    scaled = delta * -jnp.exp(per_head[1][:, :1])
    high = scaled.astype(BF16)
    mid, low = split(scaled - high.astype(F32))
    size = scaled.shape[1]
    upto = jnp.where(
        lax.broadcasted_iota(jnp.int32, (size, size), 0) <= lax.broadcasted_iota(jnp.int32, (size, size), 1), 1.0, 0.0
    ).astype(BF16)
    cum = dot(low, upto, 1, 0) + dot(mid, upto, 1, 0) + dot(high, upto, 1, 0)
    cum_out[...] = cum
    less_out[...] = cum - jnp.log(delta)
    end = cum[:, size - 1 :]
    gain = delta * jnp.exp(end - cum)
    total_high, total_low = split(jnp.exp(end))
    total_high, total_low = total_high.astype(F32), total_low.astype(F32)

    spread = jnp.where(
        lax.broadcasted_iota(jnp.int32, (heads, channels), 1) // width
        == lax.broadcasted_iota(jnp.int32, (heads, channels), 0),
        1.0,
        0.0,
    ).astype(BF16)
    gain_high, gain_low = split(gain[:, :128])
    lines = lax.broadcasted_iota(jnp.int32, (8, channels), 0)
    gains = jnp.where(lines < 4, dot(gain_high, spread, 0, 0)[:8], pltpu.roll(dot(gain_low, spread, 0, 0)[:8], 4, 0))
    lines = lax.broadcasted_iota(jnp.int32, last.shape, 0)
    edges = jnp.where(lines < 3, last[...].astype(F32), pltpu.roll(first[...].astype(F32), 3, 0))

    bcc[...] = filtered(bc[...], bc_taps[...].T)
    b_rows = bcc[:states, :]
    x_cols = x_taps[...].T
    late = jnp.where(lax.broadcasted_iota(jnp.int32, gain.shape, 1) < 3, 0.0, gain)
    lines = lax.broadcasted_iota(jnp.int32, (8, 128), 0)
    per = heads // LO
    for quarter in range(LO):
        tail = jnp.zeros((8, 128), F32)
        for j in range(per):
            h = quarter * per + j
            at = pl.ds(h * width, width)
            values = filtered(x[at, :], x_cols[h * width : (h + 1) * width])
            xc[at, :] = values
            weighted = (values.astype(F32) * late[h : h + 1]).astype(BF16)
            pay[quarter, pl.ds(j * width, width), :] = dot(weighted, b_rows, 1, 1).astype(BF16)
            tail = jnp.where(lines == 2 * j, total_high[h : h + 1], tail)
            tail = jnp.where(lines == 2 * j + 1, total_low[h : h + 1], tail)
        here = slice(quarter * 128, (quarter + 1) * 128)
        rows = jnp.concatenate([tail, edges[:, here], edges[:, channels : channels + 128], gains[:, here]], axis=0)
        pay[quarter, pl.ds(per * width, META), :] = rows.astype(BF16)


def early(series, taps):
    rows = lax.broadcasted_iota(jnp.int32, series.shape, 0)
    total = taps[4:5] + taps[0:1] * series
    for k in (1, 2, 3):
        total = total + taps[k : k + 1] * pltpu.roll(series, 8 - k, 0)
    return jnp.where(rows < 3, silu(total), 0.0).astype(BF16)


def rim_state(before, after, taps):
    rows = lax.broadcasted_iota(jnp.int32, (8, 128), 0)
    x_rows = early(jnp.where(rows < 3, before[8:16], after[8:16]), taps[0])
    b_rows = early(jnp.where(rows < 3, before[16:24], after[16:24]), taps[1])
    gains = after[24:32] + pltpu.roll(after[24:32], 4, 0)
    return dot((x_rows.astype(F32) * gains).astype(BF16), b_rows, 0, 0)


def spread_rows(rows, start, per, size):
    width = size // per
    values = [rows[start + 2 * j : start + 2 * j + 1] + rows[start + 2 * j + 1 : start + 2 * j + 2] for j in range(per)]
    return jnp.concatenate([jnp.broadcast_to(v, (width, 128)) for v in values], axis=0)


def unpack(block):
    size = block.shape[0] - META
    return block[:size].astype(F32), block[size:].astype(F32)


def packed_rows(decay, start, rows, per):
    width = decay.shape[0] // per
    lines = lax.broadcasted_iota(jnp.int32, (8, 128), 0)
    for j in range(per):
        d = decay[j * width : j * width + 1]
        high = d.astype(BF16).astype(F32)
        rows = jnp.where(lines == start + 2 * j, high, rows)
        rows = jnp.where(lines == start + 2 * j + 1, d - high, rows)
    return rows


def group_kernel(got, taps, kept, meta, *refs, per, opening):
    blank_kernel(*refs[1:])
    size = kept.shape[1]
    members = [unpack(got[r]) for r in range(LO)]
    lines = lax.broadcasted_iota(jnp.int32, (META, 128), 0)
    state, rows = members[0]
    if opening:
        state = state + rim_state(jnp.zeros_like(rows), rows, taps)
    kept[0] = state
    decay = spread_rows(rows, 0, per, size)
    suffix = jnp.ones_like(decay)
    for r in range(1, LO):
        fresh, now = members[r]
        fresh = fresh + rim_state(members[r - 1][1], now, taps)
        kept[r] = fresh
        d = spread_rows(now, 0, per, size)
        state = fresh + d * state
        decay, suffix = decay * d, suffix * d
    meta[...] = got[:, size:, :]
    if not refs:
        return
    out = refs[0]
    out[:size, :] = state.astype(BF16)
    head = packed_rows(suffix, 4, packed_rows(decay, 0, jnp.zeros((8, 128), F32), per), per)
    edge = lax.broadcasted_iota(jnp.int32, (16, 128), 0) % 8 < 3
    edges = jnp.where(edge, members[LO - 1][1][8:24], rows[8:24])
    out[size:, :] = jnp.concatenate([head, edges, rows[24:32]], axis=0).astype(BF16)


def join_kernel(earlier, later, taps, out, *, per):
    size = out.shape[0] - META
    before, rows_before = unpack(earlier[...])
    after, rows = unpack(later[...])
    opening = rim_state(rows_before, rows, taps)
    state = after + spread_rows(rows, 4, per, size) * opening + spread_rows(rows, 0, per, size) * before
    out[:size, :] = state.astype(BF16)
    out[size:, :] = later[size:, :]


def entering_kernel(kept, meta, *refs, per, blanks):
    blank_kernel(*refs[len(refs) - blanks :])
    *given, out = refs[: len(refs) - blanks]
    size = kept.shape[1]
    own = meta[0].astype(F32)
    fresh = kept[0]
    state = jnp.zeros(out.shape[1:], F32)
    if given:
        taps, near, next_one, over, between = given
        (near, rows_near), (next_one, rows_next) = unpack(near[...]), unpack(next_one[...])
        (over, rows_over), (between, rows) = unpack(over[...]), unpack(between[...])
        opening = rim_state(rows_over, rows, taps)
        state = between + spread_rows(rows, 4, per, size) * opening + spread_rows(rows, 0, per, size) * over
        state = state + near + next_one
        fresh = fresh + rim_state(rows_near + rows_next + rows, own, taps)
    out[0] = state.astype(BF16)
    for r in range(1, LO):
        state = fresh + spread_rows(meta[r - 1].astype(F32), 0, per, size) * state
        out[r] = state.astype(BF16)
        fresh = kept[r]


def copy_kernel(*refs):
    half = len(refs) // 2
    for source, target in zip(refs[:half], refs[half:]):
        target[...] = source[...]


def pack_kernel(kept, begin, meta, joined, near, kept_out, rows):
    kept_out[...] = kept[...] + begin[...].astype(F32)
    at = 0
    for r in range(LO):
        rows[at : at + META, :] = meta[r]
        at += META
    for block in (joined, near):
        rows[at : at + block.shape[0], :] = block[...]
        at += block.shape[0]


def unpack_kernel(rows, meta, joined, near):
    at = 0
    for r in range(LO):
        meta[r] = rows[at : at + META, :]
        at += META
    for block in (joined, near):
        block[...] = rows[at : at + block.shape[0], :]
        at += block.shape[0]


def begin_kernel(kept, inner, later, state, inner_out, later_out):
    state[...] = kept[...].astype(BF16)
    inner_out[...] = inner[...]
    later_out[...] = later[...]


def blank_kernel(*refs):
    for ref in refs:
        ref[...] = jnp.zeros(ref.shape, ref.dtype)


def intra_kernel(z, *refs, count):
    rims, refs = refs[:count], refs[count:]
    xc, bcc, first, x_taps, bc_taps, cum_in, less_in, per_head, out, later, done = refs
    fetch = pltpu.make_async_copy(z, later.at[pl.ds(bcc.shape[0] // 2, z.shape[0])], done)
    fetch.start()
    heads = cum_in.shape[0]
    channels = xc.shape[0]
    width = channels // heads
    states = bcc.shape[0] // 2
    cum, less = cum_in[...], less_in[...]
    less_cols = jnp.concatenate([less[:, :128].T, less[:, 128:].T], axis=0)
    skips = per_head[2][:, :1]
    lines = lax.broadcasted_iota(jnp.int32, first.shape, 0)
    given = sum(r[...].astype(F32) for r in rims)
    edges = jnp.where(lines < 3, given, pltpu.roll(first[...].astype(F32), 3, 0))
    begun = [early(edges[:, :channels], x_taps[...]), early(edges[:, channels:], bc_taps[...])]
    placed = dot(jnp.concatenate(begun, axis=1), picks(0), 0, 0).astype(BF16)

    def mended(values, rows):
        lanes = lax.broadcasted_iota(jnp.int32, rows.shape, 1)
        return jnp.concatenate([jnp.where(lanes < 3, rows, values[:, :128]), values[:, 128:]], axis=1)

    both = mended(bcc[...], placed[channels:])
    later[:states, :] = both[states:]
    gram = dot(both[:states], both[states:], 0, 0)
    keep = lax.broadcasted_iota(jnp.int32, (128, 128), 0) <= lax.broadcasted_iota(jnp.int32, (128, 128), 1)
    for h in range(heads):
        at = pl.ds(h * width, width)
        values = mended(xc[at, :], placed[h * width : (h + 1) * width])
        row = cum[h : h + 1]
        col = less_cols[:, h : h + 1]

        def mix(s, t, masked):
            spread = row[:, t : t + 128] - col[s : s + 128]
            if masked:
                spread = jnp.where(keep, spread, -1e30)
            return (gram[s : s + 128, t : t + 128] * jnp.exp(spread)).astype(BF16)

        near = dot(values[:, :128], mix(0, 0, True), 1, 0)
        late = dot(values, jnp.concatenate([mix(0, 128, False), mix(128, 128, True)], axis=0), 1, 0)
        out[at, :] = jnp.concatenate([near, late], axis=1) + skips[h : h + 1] * values.astype(F32)
    fetch.wait()


def output_kernel(inner, later, cum, state, out, held, done):
    heads = cum.shape[0]
    width = inner.shape[0] // heads
    per = heads // LO
    states = state.shape[1]
    c_rows = later[:states, :]
    grown = jnp.exp(cum[...])
    copies = []
    for h in range(heads):
        at = pl.ds(h * width, width)
        y = inner[at, :] + grown[h : h + 1] * dot(state[at, :], c_rows, 1, 0)
        y = y.astype(BF16).astype(F32)
        held[at, :] = (y * silu(later[pl.ds(states + h * width, width), :].astype(F32))).astype(BF16)
        if h % per == per - 1:
            part = pl.ds((h + 1 - per) * width, per * width)
            copies.append(pltpu.make_async_copy(held.at[part], out.at[part], done.at[h // per]))
            copies[-1].start()
    for copy in copies:
        copy.wait()


def shape(*dims, dtype=F32):
    return pltpu.VMEM(dims, dtype)


VMEM = pl.BlockSpec(memory_space=pltpu.VMEM)
GRANT = pltpu.CompilerParams(vmem_limit_bytes=12 << 20)


def run(kernel, outs, *args):
    args = [pltpu.with_memory_space_constraint(a, pltpu.VMEM) for a in args]
    return pl.pallas_call(
        kernel, out_shape=outs, in_specs=[VMEM] * len(args), out_specs=[VMEM] * len(outs), compiler_params=GRANT
    )(*args)


def local(x_in, z_gate, bc_in, dt_raw, conv_x_w, conv_x_b, conv_bc_w, conv_bc_b, dt_bias, a_log, d_skip):
    heads, length = dt_raw.shape
    channels = x_in.shape[0]
    rows = bc_in.shape[1]
    states = rows // 2
    per = heads // LO
    quarter = channels // LO
    group = (lax.axis_index("tensor") // (GROUP_HEADS // heads)).astype(jnp.int32).reshape(1)
    member = lax.axis_index("near").astype(jnp.int32).reshape(1)
    far = lax.axis_index("far")
    cp = ("far", "near")
    count = lax.axis_size(cp)

    strip = shape(8, channels + rows, dtype=BF16)
    block_shape = shape(quarter + META, states, dtype=BF16)
    kept_shapes = [shape(LO, quarter, states), shape(LO, META, states, dtype=BF16)]
    state_shape = shape(LO, quarter, states, dtype=BF16)
    series = shape(channels, length, dtype=BF16)
    pairs = shape(rows, length, dtype=BF16)
    taps = jnp.swapaxes(conv_bc_w, 1, 2)
    small = [dt_raw, conv_x_w.T, conv_x_b[None], conv_bc_b, dt_bias[None], a_log[None], d_skip[None]]
    outs = [strip, strip, series, pairs, shape(heads, length, dtype=BF16), shape(8, channels), shape(8, rows)]
    outs += [shape(2, 8, 128), shape(3, heads, 128)]
    last, first, x, bc, dt, x_taps, bc_taps, own_taps, per_head = pl.pallas_call(
        load_kernel,
        grid_spec=pltpu.PrefetchScalarGridSpec(
            num_scalar_prefetch=2,
            grid=(1,),
            in_specs=[pl.BlockSpec((1,) + a.shape[1:], lambda i, g, m: (g[0], 0, 0)) for a in (bc_in, taps)]
            + [pl.BlockSpec(a.shape, lambda i, g, m: (0, 0)) for a in [x_in] + small],
            out_specs=[VMEM] * len(outs),
        ),
        out_shape=outs,
        name="load",
        compiler_params=GRANT,
    )(group, member, *[pltpu.with_memory_space_constraint(a, pltpu.HBM) for a in (bc_in, taps, x_in, *small)])
    outs = [shape(LO, quarter + META, states, dtype=BF16), series, pairs]
    outs += [shape(heads, length), shape(heads, length)]
    pay, xc, bcc, cum, less = run(state_kernel, outs, x, bc, dt, x_taps, bc_taps, per_head, last, first)

    def gather(*rest, opening=False):
        got = lax.all_to_all(pay, "near", 0, 0, tiled=True)
        kernel = lambda *refs: group_kernel(*refs, per=per, opening=opening)
        return tuple(run(kernel, [*kept_shapes, *rest], got, own_taps))

    def blank(*outs):
        return tuple(run(blank_kernel, list(outs)))

    def exchange(*given, blanks=()):
        kernel = lambda *refs: entering_kernel(*refs, per=per, blanks=len(blanks))
        entering, *rest = run(kernel, [state_shape, *blanks], *given)
        return tuple(rest) + (lax.all_to_all(entering, "near", 0, 0, tiled=True),)

    def sent(block, source, target):
        route = [(source * LO + i, target * LO + i) for i in range(LO)]
        return lax.ppermute(block, cp, route)

    def kept_on(*arrays):
        return tuple(run(copy_kernel, [shape(*a.shape, dtype=a.dtype) for a in arrays], *arrays))

    def inside(*rims):
        args = [*rims, xc, bcc, first, x_taps, bc_taps, cum, less, per_head]
        return tuple(
            pl.pallas_call(
                lambda *refs: intra_kernel(*refs, count=len(rims)),
                out_shape=inner_shapes,
                in_specs=[pl.BlockSpec(memory_space=pl.ANY)] + [VMEM] * len(args),
                out_specs=[VMEM] * 2,
                scratch_shapes=[pltpu.SemaphoreType.DMA],
                name="intra",
        compiler_params=GRANT,
            )(pltpu.with_memory_space_constraint(z_gate, pltpu.HBM), *[pltpu.with_memory_space_constraint(a, pltpu.VMEM) for a in args])
        )

    def shifted(begin, end):
        return lax.ppermute(kept_on(last)[0], cp, [(i, i + 1) for i in range(begin, end)])

    inner_shapes = [shape(channels, length), shape(states + channels, length, dtype=BF16)]

    packed_rows_count = LO * META + 2 * (quarter + META)
    packed_shapes = [kept_shapes[0], shape(packed_rows_count, states, dtype=BF16)]

    def low_part():
        kept = lax.cond(
            far == 0, lambda: gather(block_shape, opening=True), lambda: blank(*kept_shapes, block_shape)
        )
        near = sent(kept[2], 0, 1)
        rims = shifted(0, 2 * LO - 1)
        *kept, begin = lax.cond(
            far == 0,
            lambda *kept: exchange(*kept[:2], blanks=(*kept_shapes, block_shape)),
            lambda *kept: gather(block_shape, state_shape),
            *kept,
        )
        inner = inside(rims)
        (joined,) = run(lambda *refs: join_kernel(*refs, per=per), [block_shape], near, kept[2], own_taps)
        packed = run(pack_kernel, packed_shapes, kept[0], begin, kept[1], joined, near)
        return (*packed, *inner)

    def high_part(*kept):
        rims = shifted(2 * LO, count - 1)
        kept = lax.cond(far == 2, lambda *kept: gather(block_shape), lambda *kept: blank(*kept_shapes, block_shape), *kept)
        between = sent(kept[2], 2, 3)
        kept = lax.cond(far == 3, lambda *kept: gather(), kept_on, *kept[:2])
        return kept_on(*kept, between, rims)

    def later_part(kept, packed, *inner):
        meta, joined, near = run(unpack_kernel, [kept_shapes[1], block_shape, block_shape], packed)
        over = sent(joined, 1, 3)
        next_one = sent(joined, 1, 2)
        rims_mid = shifted(2 * LO - 1, 2 * LO)
        *kept, between, rims = lax.cond(
            far >= 2, high_part, lambda *kept: kept_on(*kept) + blank(block_shape, strip), kept, meta
        )
        inner = lax.cond(
            far >= 2, lambda rims, rims_mid, *inner: inside(rims, rims_mid),
            lambda rims, rims_mid, *inner: kept_on(*inner), rims, rims_mid, *inner
        )
        between, *inner = lax.optimization_barrier((between, *inner))
        (state,) = exchange(*kept_on(*kept), own_taps, near, next_one, over, between)
        return (state, *inner)

    parts = lax.cond(far < 2, low_part, lambda: blank(*packed_shapes, *inner_shapes))
    state, inner, later = lax.cond(
        far == 0,
        lambda kept, packed, *inner: tuple(run(begin_kernel, [state_shape, *inner_shapes], kept, *inner)),
        later_part,
        *parts,
    )
    inputs = [inner, later, cum, state.reshape(channels, states)]
    return pl.pallas_call(
        output_kernel,
        out_shape=jax.ShapeDtypeStruct((channels, length), BF16),
        in_specs=[VMEM] * len(inputs),
        out_specs=pl.BlockSpec(memory_space=pl.ANY),
        scratch_shapes=[pltpu.VMEM((channels, length), BF16), pltpu.SemaphoreType.DMA((LO,))],
        name="gated",
    compiler_params=GRANT,
    )(*[pltpu.with_memory_space_constraint(a, pltpu.VMEM) for a in inputs])


def solution(mesh):
    dp, cp, tensor = mesh.devices.shape
    finer = Mesh(mesh.devices.reshape(dp, cp // LO, LO, tensor), ("dp", "far", "near", "tensor"))
    along = ("dp", "far", "near")
    return jax.shard_map(
        local,
        mesh=finer,
        in_specs=(
            P("tensor", along),
            P("tensor", along),
            P(None, None, along),
            P("tensor", along),
            P("tensor", None),
            P("tensor"),
            P(),
            P(),
            P("tensor"),
            P("tensor"),
            P("tensor"),
        ),
        out_specs=P("tensor", along),
        check_vma=False,
    )
```

```python
import jax
import jax.numpy as jnp
from jax import lax
from jax.experimental import pallas as pl
from jax.experimental.pallas import tpu as pltpu
from jax.sharding import Mesh, PartitionSpec as P


HEADS = 128
GROUPS = 8
GROUP_HEADS = HEADS // GROUPS
LO = 4
META = 32

F32 = jnp.float32
BF16 = jnp.bfloat16


def dot(a, b, ca, cb):
    return lax.dot_general(a, b, (((ca,), (cb,)), ((), ())), preferred_element_type=F32)


def silu(v):
    half = 0.5 * v
    return half + half * jnp.tanh(half)


def log1p(u):
    return jnp.where(u < 1e-3, u * (1.0 - u * (0.5 - u * (1.0 / 3.0))), jnp.log(1.0 + u))


def softplus(v):
    return jnp.maximum(v, 0.0) + log1p(jnp.exp(-jnp.abs(v)))


def picks(first_lane):
    rows = lax.broadcasted_iota(jnp.int32, (8, 128), 0)
    lanes = lax.broadcasted_iota(jnp.int32, (8, 128), 1)
    return jnp.where(jnp.logical_and(lanes == rows + first_lane, rows < 3), 1.0, 0.0).astype(BF16)


def load_kernel(
    group, member, bc, bw, x, dt, xw, xb, bb, bias, a_log, skip,
    last, first, x_out, bc_out, dt_out, x_taps, bc_taps, own_taps, per_head,
):
    channels = x.shape[0]
    heads = dt.shape[0]
    begin, finish = picks(0), picks(125)
    series, mine = x[...], bc[0]
    last[:, :channels] = dot(finish, series[:, 128:], 1, 1).astype(BF16)
    last[:, channels:] = dot(finish, mine[:, 128:], 1, 1).astype(BF16)
    first[:, :channels] = dot(begin, series[:, :128], 1, 1).astype(BF16)
    first[:, channels:] = dot(begin, mine[:, :128], 1, 1).astype(BF16)
    x_out[...] = series
    bc_out[...] = mine
    dt_out[...] = dt[...]
    x_taps[:4, :] = xw[...]
    x_taps[4:, :] = jnp.broadcast_to(xb[...], (4, channels))
    own = jnp.zeros(own_taps.shape[1:], F32)
    for q in range(LO):
        own = jnp.where(member[0] == q, x_taps[:, q * 128 : (q + 1) * 128], own)
    own_taps[0] = own
    bc_taps[:4, :] = bw[0]
    bc_taps[4:, :] = jnp.broadcast_to(chosen(bb[...], group[0]), (4, mine.shape[0]))
    own_taps[1] = bc_taps[:, :128]
    for i, row in enumerate((bias, a_log, skip)):
        per_head[i] = jnp.broadcast_to(column(row[...]), (heads, 128))


def filtered(series, taps):
    lanes = lax.broadcasted_iota(jnp.int32, (series.shape[0], 128), 1)
    first, second = series[:, :128].astype(F32), series[:, 128:].astype(F32)
    a = taps[:, 4:5] + taps[:, 3:4] * first
    b = taps[:, 4:5] + taps[:, 3:4] * second
    for back in (1, 2, 3):
        moved = pltpu.roll(first, back, 1)
        tap = taps[:, 3 - back : 4 - back]
        a = a + tap * moved
        b = b + tap * jnp.where(lanes < back, moved, pltpu.roll(second, back, 1))
    return jnp.concatenate([silu(a), silu(b)], axis=1).astype(BF16)


def column(row):
    size = row.shape[1]
    same = lax.broadcasted_iota(jnp.int32, (size, size), 0) == lax.broadcasted_iota(jnp.int32, (size, size), 1)
    return jnp.sum(jnp.where(same, row, 0.0), axis=1, keepdims=True)


def chosen(table, group):
    rows = lax.broadcasted_iota(jnp.int32, table.shape, 0)
    return jnp.sum(jnp.where(rows == group, table, 0.0), axis=0, keepdims=True)


def split(value):
    high = value.astype(BF16)
    return high, (value - high.astype(F32)).astype(BF16)


def state_kernel(x, bc, dt, x_taps, bc_taps, per_head, last, first, pay, xc, bcc, cum_out, less_out):
    channels = x.shape[0]
    heads = dt.shape[0]
    width = channels // heads
    states = bc.shape[0] // 2

    delta = softplus(dt[...].astype(F32) + per_head[0][:, :1])
    scaled = delta * -jnp.exp(per_head[1][:, :1])
    high = scaled.astype(BF16).astype(F32)
    mid = (scaled - high).astype(BF16).astype(F32)
    size = scaled.shape[1]
    upto = jnp.where(
        lax.broadcasted_iota(jnp.int32, (size, size), 0) <= lax.broadcasted_iota(jnp.int32, (size, size), 1), 1.0, 0.0
    ).astype(BF16)
    sums = dot(jnp.concatenate([scaled - high - mid, mid, high], axis=0).astype(BF16), upto, 1, 0)
    cum = sums[:heads] + sums[heads : 2 * heads] + sums[2 * heads :]
    cum_out[...] = cum
    less_out[...] = cum - jnp.log(delta)
    end = cum[:, size - 1 :]
    gain = delta * jnp.exp(end - cum)
    total_high, total_low = split(jnp.exp(end))
    total_high, total_low = total_high.astype(F32), total_low.astype(F32)

    opening = gain[:, :128].T[:8]
    gains = jnp.concatenate([jnp.broadcast_to(opening[:, h : h + 1], (8, width)) for h in range(heads)], axis=1)
    gain_high = gains.astype(BF16).astype(F32)
    lines = lax.broadcasted_iota(jnp.int32, (8, channels), 0)
    gains = jnp.where(lines < 4, gain_high, pltpu.roll(gains - gain_high, 4, 0))
    lines = lax.broadcasted_iota(jnp.int32, last.shape, 0)
    edges = jnp.where(lines < 3, last[...].astype(F32), pltpu.roll(first[...].astype(F32), 3, 0))

    bcc[...] = filtered(bc[...], bc_taps[...].T)
    b_rows = bcc[:states, :]
    x_cols = x_taps[...].T
    late = jnp.where(lax.broadcasted_iota(jnp.int32, gain.shape, 1) < 3, 0.0, gain)
    lines = lax.broadcasted_iota(jnp.int32, (8, 128), 0)
    per = heads // LO
    for quarter in range(LO):
        tail = jnp.zeros((8, 128), F32)
        for j in range(per):
            h = quarter * per + j
            at = pl.ds(h * width, width)
            values = filtered(x[at, :], x_cols[h * width : (h + 1) * width])
            xc[at, :] = values
            weighted = (values.astype(F32) * late[h : h + 1]).astype(BF16)
            pay[quarter, pl.ds(j * width, width), :] = dot(weighted, b_rows, 1, 1).astype(BF16)
            tail = jnp.where(lines == 2 * j, total_high[h : h + 1], tail)
            tail = jnp.where(lines == 2 * j + 1, total_low[h : h + 1], tail)
        here = slice(quarter * 128, (quarter + 1) * 128)
        rows = jnp.concatenate([tail, edges[:, here], edges[:, channels : channels + 128], gains[:, here]], axis=0)
        pay[quarter, pl.ds(per * width, META), :] = rows.astype(BF16)


def early(series, taps):
    rows = lax.broadcasted_iota(jnp.int32, series.shape, 0)
    total = taps[4:5] + taps[0:1] * series
    for k in (1, 2, 3):
        total = total + taps[k : k + 1] * pltpu.roll(series, 8 - k, 0)
    return jnp.where(rows < 3, silu(total), 0.0).astype(BF16)


def rim_state(before, after, taps):
    rows = lax.broadcasted_iota(jnp.int32, (8, 128), 0)
    x_rows = early(jnp.where(rows < 3, before[8:16], after[8:16]), taps[0])
    b_rows = early(jnp.where(rows < 3, before[16:24], after[16:24]), taps[1])
    gains = after[24:32] + pltpu.roll(after[24:32], 4, 0)
    return dot((x_rows.astype(F32) * gains).astype(BF16), b_rows, 0, 0)


def spread_rows(rows, start, per, size):
    width = size // per
    values = [rows[start + 2 * j : start + 2 * j + 1] + rows[start + 2 * j + 1 : start + 2 * j + 2] for j in range(per)]
    return jnp.concatenate([jnp.broadcast_to(v, (width, 128)) for v in values], axis=0)


def unpack(block):
    size = block.shape[0] - META
    return block[:size].astype(F32), block[size:].astype(F32)


def packed_rows(decay, start, rows, per):
    width = decay.shape[0] // per
    lines = lax.broadcasted_iota(jnp.int32, (8, 128), 0)
    for j in range(per):
        d = decay[j * width : j * width + 1]
        high = d.astype(BF16).astype(F32)
        rows = jnp.where(lines == start + 2 * j, high, rows)
        rows = jnp.where(lines == start + 2 * j + 1, d - high, rows)
    return rows


def group_kernel(got, taps, kept, meta, *refs, per, opening):
    blank_kernel(*refs[1:])
    size = kept.shape[1]
    members = [unpack(got[r]) for r in range(LO)]
    lines = lax.broadcasted_iota(jnp.int32, (META, 128), 0)
    state, rows = members[0]
    if opening:
        state = state + rim_state(jnp.zeros_like(rows), rows, taps)
    kept[0] = state
    decay = spread_rows(rows, 0, per, size)
    suffix = jnp.ones_like(decay)
    for r in range(1, LO):
        fresh, now = members[r]
        fresh = fresh + rim_state(members[r - 1][1], now, taps)
        kept[r] = fresh
        d = spread_rows(now, 0, per, size)
        state = fresh + d * state
        decay, suffix = decay * d, suffix * d
    meta[...] = got[:, size:, :]
    if not refs:
        return
    out = refs[0]
    out[:size, :] = state.astype(BF16)
    head = packed_rows(suffix, 4, packed_rows(decay, 0, jnp.zeros((8, 128), F32), per), per)
    edge = lax.broadcasted_iota(jnp.int32, (16, 128), 0) % 8 < 3
    edges = jnp.where(edge, members[LO - 1][1][8:24], rows[8:24])
    out[size:, :] = jnp.concatenate([head, edges, rows[24:32]], axis=0).astype(BF16)


def join_kernel(earlier, later, taps, out, *, per):
    size = out.shape[0] - META
    before, rows_before = unpack(earlier[...])
    after, rows = unpack(later[...])
    opening = rim_state(rows_before, rows, taps)
    state = after + spread_rows(rows, 4, per, size) * opening + spread_rows(rows, 0, per, size) * before
    out[:size, :] = state.astype(BF16)
    out[size:, :] = later[size:, :]


def entering_kernel(kept, meta, *refs, per, blanks):
    blank_kernel(*refs[len(refs) - blanks :])
    *given, out = refs[: len(refs) - blanks]
    size = kept.shape[1]
    own = meta[0].astype(F32)
    fresh = kept[0]
    state = jnp.zeros(out.shape[1:], F32)
    if given:
        taps, near, next_one, over, between = given
        (near, rows_near), (next_one, rows_next) = unpack(near[...]), unpack(next_one[...])
        (over, rows_over), (between, rows) = unpack(over[...]), unpack(between[...])
        opening = rim_state(rows_over, rows, taps)
        state = between + spread_rows(rows, 4, per, size) * opening + spread_rows(rows, 0, per, size) * over
        state = state + near + next_one
        fresh = fresh + rim_state(rows_near + rows_next + rows, own, taps)
    out[0] = state.astype(BF16)
    for r in range(1, LO):
        state = fresh + spread_rows(meta[r - 1].astype(F32), 0, per, size) * state
        out[r] = state.astype(BF16)
        fresh = kept[r]


def copy_kernel(*refs):
    half = len(refs) // 2
    for source, target in zip(refs[:half], refs[half:]):
        target[...] = source[...]


def pack_kernel(kept, begin, meta, joined, near, kept_out, rows):
    kept_out[...] = kept[...] + begin[...].astype(F32)
    at = 0
    for r in range(LO):
        rows[at : at + META, :] = meta[r]
        at += META
    for block in (joined, near):
        rows[at : at + block.shape[0], :] = block[...]
        at += block.shape[0]


def unpack_kernel(rows, meta, joined, near):
    at = 0
    for r in range(LO):
        meta[r] = rows[at : at + META, :]
        at += META
    for block in (joined, near):
        block[...] = rows[at : at + block.shape[0], :]
        at += block.shape[0]


def begin_kernel(kept, state):
    state[...] = kept[...].astype(BF16)


def blank_kernel(*refs):
    for ref in refs:
        ref[...] = jnp.zeros(ref.shape, ref.dtype)


def intra_kernel(z, *refs, count):
    rims, refs = refs[:count], refs[count:]
    xc, bcc, first, x_taps, bc_taps, cum_in, less_in, per_head, out, later, done = refs
    fetch = pltpu.make_async_copy(z, later.at[pl.ds(bcc.shape[0] // 2, z.shape[0])], done)
    fetch.start()
    heads = cum_in.shape[0]
    channels = xc.shape[0]
    width = channels // heads
    states = bcc.shape[0] // 2
    cum, less = cum_in[...], less_in[...]
    less_cols = jnp.concatenate([less[:, :128].T, less[:, 128:].T], axis=0)
    skips = per_head[2][:, :1]
    lines = lax.broadcasted_iota(jnp.int32, first.shape, 0)
    given = sum(r[...].astype(F32) for r in rims)
    edges = jnp.where(lines < 3, given, pltpu.roll(first[...].astype(F32), 3, 0))
    begun = [early(edges[:, :channels], x_taps[...]), early(edges[:, channels:], bc_taps[...])]
    placed = dot(jnp.concatenate(begun, axis=1), picks(0), 0, 0).astype(BF16)

    def mended(values, rows):
        lanes = lax.broadcasted_iota(jnp.int32, rows.shape, 1)
        return jnp.concatenate([jnp.where(lanes < 3, rows, values[:, :128]), values[:, 128:]], axis=1)

    both = mended(bcc[...], placed[channels:])
    later[:states, :] = both[states:]
    gram = dot(both[:states], both[states:], 0, 0)
    keep = lax.broadcasted_iota(jnp.int32, (128, 128), 0) <= lax.broadcasted_iota(jnp.int32, (128, 128), 1)
    for h in range(heads):
        at = pl.ds(h * width, width)
        values = mended(xc[at, :], placed[h * width : (h + 1) * width])
        row = cum[h : h + 1]
        col = less_cols[:, h : h + 1]

        def mix(s, t, masked):
            spread = row[:, t : t + 128] - col[s : s + 128]
            if masked:
                spread = jnp.where(keep, spread, -1e30)
            return (gram[s : s + 128, t : t + 128] * jnp.exp(spread)).astype(BF16)

        near = dot(values[:, :128], mix(0, 0, True), 1, 0)
        late = dot(values, jnp.concatenate([mix(0, 128, False), mix(128, 128, True)], axis=0), 1, 0)
        out[at, :] = jnp.concatenate([near, late], axis=1) + skips[h : h + 1] * values.astype(F32)
    fetch.wait()


def output_kernel(inner, later, cum, state, out, held, done):
    heads = cum.shape[0]
    width = inner.shape[0] // heads
    per = heads // LO
    states = state.shape[1]
    c_rows = later[:states, :]
    grown = jnp.exp(cum[...])
    copies = []
    for h in range(heads):
        at = pl.ds(h * width, width)
        y = inner[at, :] + grown[h : h + 1] * dot(state[at, :], c_rows, 1, 0)
        y = y.astype(BF16).astype(F32)
        held[at, :] = (y * silu(later[pl.ds(states + h * width, width), :].astype(F32))).astype(BF16)
        if h % per == per - 1:
            part = pl.ds((h + 1 - per) * width, per * width)
            copies.append(pltpu.make_async_copy(held.at[part], out.at[part], done.at[h // per]))
            copies[-1].start()
    for copy in copies:
        copy.wait()


def shape(*dims, dtype=F32):
    return pltpu.VMEM(dims, dtype)


VMEM = pl.BlockSpec(memory_space=pltpu.VMEM)
GRANT = pltpu.CompilerParams(vmem_limit_bytes=12 << 20)


def run(kernel, outs, *args):
    args = [pltpu.with_memory_space_constraint(a, pltpu.VMEM) for a in args]
    return pl.pallas_call(
        kernel, out_shape=outs, in_specs=[VMEM] * len(args), out_specs=[VMEM] * len(outs), compiler_params=GRANT
    )(*args)


def local(x_in, z_gate, bc_in, dt_raw, conv_x_w, conv_x_b, conv_bc_w, conv_bc_b, dt_bias, a_log, d_skip):
    heads, length = dt_raw.shape
    channels = x_in.shape[0]
    rows = bc_in.shape[1]
    states = rows // 2
    per = heads // LO
    quarter = channels // LO
    group = (lax.axis_index("tensor") // (GROUP_HEADS // heads)).astype(jnp.int32).reshape(1)
    member = lax.axis_index("near").astype(jnp.int32).reshape(1)
    far = lax.axis_index("far")
    cp = ("far", "near")
    count = lax.axis_size(cp)

    strip = shape(8, channels + rows, dtype=BF16)
    block_shape = shape(quarter + META, states, dtype=BF16)
    kept_shapes = [shape(LO, quarter, states), shape(LO, META, states, dtype=BF16)]
    state_shape = shape(LO, quarter, states, dtype=BF16)
    series = shape(channels, length, dtype=BF16)
    pairs = shape(rows, length, dtype=BF16)
    taps = jnp.swapaxes(conv_bc_w, 1, 2)
    small = [dt_raw, conv_x_w.T, conv_x_b[None], conv_bc_b, dt_bias[None], a_log[None], d_skip[None]]
    outs = [strip, strip, series, pairs, shape(heads, length, dtype=BF16), shape(8, channels), shape(8, rows)]
    outs += [shape(2, 8, 128), shape(3, heads, 128)]
    last, first, x, bc, dt, x_taps, bc_taps, own_taps, per_head = pl.pallas_call(
        load_kernel,
        grid_spec=pltpu.PrefetchScalarGridSpec(
            num_scalar_prefetch=2,
            grid=(1,),
            in_specs=[pl.BlockSpec((1,) + a.shape[1:], lambda i, g, m: (g[0], 0, 0)) for a in (bc_in, taps)]
            + [pl.BlockSpec(a.shape, lambda i, g, m: (0, 0)) for a in [x_in] + small],
            out_specs=[VMEM] * len(outs),
        ),
        out_shape=outs,
        name="load",
        compiler_params=GRANT,
    )(group, member, *[pltpu.with_memory_space_constraint(a, pltpu.HBM) for a in (bc_in, taps, x_in, *small)])
    outs = [shape(LO, quarter + META, states, dtype=BF16), series, pairs]
    outs += [shape(heads, length), shape(heads, length)]
    pay, xc, bcc, cum, less = run(state_kernel, outs, x, bc, dt, x_taps, bc_taps, per_head, last, first)

    def gather(*rest, opening=False):
        got = lax.all_to_all(pay, "near", 0, 0, tiled=True)
        kernel = lambda *refs: group_kernel(*refs, per=per, opening=opening)
        return tuple(run(kernel, [*kept_shapes, *rest], got, own_taps))

    def blank(*outs):
        return tuple(run(blank_kernel, list(outs)))

    def exchange(*given, blanks=()):
        kernel = lambda *refs: entering_kernel(*refs, per=per, blanks=len(blanks))
        entering, *rest = run(kernel, [state_shape, *blanks], *given)
        return tuple(rest) + (lax.all_to_all(entering, "near", 0, 0, tiled=True),)

    def sent(block, source, target):
        route = [(source * LO + i, target * LO + i) for i in range(LO)]
        return lax.ppermute(block, cp, route)

    def kept_on(*arrays):
        return tuple(run(copy_kernel, [shape(*a.shape, dtype=a.dtype) for a in arrays], *arrays))

    def inside(*rims):
        args = [*rims, xc, bcc, first, x_taps, bc_taps, cum, less, per_head]
        return tuple(
            pl.pallas_call(
                lambda *refs: intra_kernel(*refs, count=len(rims)),
                out_shape=inner_shapes,
                in_specs=[pl.BlockSpec(memory_space=pl.ANY)] + [VMEM] * len(args),
                out_specs=[VMEM] * 2,
                scratch_shapes=[pltpu.SemaphoreType.DMA],
                name="intra",
        compiler_params=GRANT,
            )(pltpu.with_memory_space_constraint(z_gate, pltpu.HBM), *[pltpu.with_memory_space_constraint(a, pltpu.VMEM) for a in args])
        )

    def shifted(begin, end):
        return lax.ppermute(kept_on(last)[0], cp, [(i, i + 1) for i in range(begin, end)])

    inner_shapes = [shape(channels, length), shape(states + channels, length, dtype=BF16)]

    packed_rows_count = LO * META + 2 * (quarter + META)
    packed_shapes = [kept_shapes[0], shape(packed_rows_count, states, dtype=BF16)]

    def low_part():
        kept = lax.cond(
            far == 0, lambda: gather(block_shape, opening=True), lambda: blank(*kept_shapes, block_shape)
        )
        near = sent(kept[2], 0, 1)
        rims = shifted(0, 2 * LO - 1)
        *kept, begin = lax.cond(
            far == 0,
            lambda *kept: exchange(*kept[:2], blanks=(*kept_shapes, block_shape)),
            lambda *kept: gather(block_shape, state_shape),
            *kept,
        )
        (joined,) = run(lambda *refs: join_kernel(*refs, per=per), [block_shape], near, kept[2], own_taps)
        packed = run(pack_kernel, packed_shapes, kept[0], begin, kept[1], joined, near)
        return (*packed, *kept_on(rims))

    def high_part(*kept):
        rims = shifted(2 * LO, count - 1)
        kept = lax.cond(far == 2, lambda *kept: gather(block_shape), lambda *kept: blank(*kept_shapes, block_shape), *kept)
        between = sent(kept[2], 2, 3)
        kept = lax.cond(far == 3, lambda *kept: gather(), kept_on, *kept[:2])
        return kept_on(*kept, between, rims)

    def later_part(kept, packed, rims_low):
        meta, joined, near = run(unpack_kernel, [kept_shapes[1], block_shape, block_shape], packed)
        over = sent(joined, 1, 3)
        next_one = sent(joined, 1, 2)
        rims_mid = shifted(2 * LO - 1, 2 * LO)
        *kept, between, rims = lax.cond(
            far >= 2,
            high_part,
            lambda *kept: kept_on(*kept[:2]) + blank(block_shape) + kept_on(kept[2]),
            kept,
            meta,
            rims_low,
        )
        inner = inside(rims, rims_mid)
        between, *inner = lax.optimization_barrier((between, *inner))
        (state,) = exchange(*kept_on(*kept), own_taps, near, next_one, over, between)
        return (state, *inner)

    parts = lax.cond(far < 2, low_part, lambda: blank(*packed_shapes, strip))
    state, inner, later = lax.cond(
        far == 0,
        lambda kept, packed, rims: tuple(run(begin_kernel, [state_shape], kept)) + inside(rims),
        later_part,
        *parts,
    )
    inputs = [inner, later, cum, state.reshape(channels, states)]
    return pl.pallas_call(
        output_kernel,
        out_shape=jax.ShapeDtypeStruct((channels, length), BF16),
        in_specs=[VMEM] * len(inputs),
        out_specs=pl.BlockSpec(memory_space=pl.ANY),
        scratch_shapes=[pltpu.VMEM((channels, length), BF16), pltpu.SemaphoreType.DMA((LO,))],
        name="gated",
    compiler_params=GRANT,
    )(*[pltpu.with_memory_space_constraint(a, pltpu.VMEM) for a in inputs])


def solution(mesh):
    dp, cp, tensor = mesh.devices.shape
    finer = Mesh(mesh.devices.reshape(dp, cp // LO, LO, tensor), ("dp", "far", "near", "tensor"))
    along = ("dp", "far", "near")
    return jax.shard_map(
        local,
        mesh=finer,
        in_specs=(
            P("tensor", along),
            P("tensor", along),
            P(None, None, along),
            P("tensor", along),
            P("tensor", None),
            P("tensor"),
            P(),
            P(),
            P("tensor"),
            P("tensor"),
            P("tensor"),
        ),
        out_specs=P("tensor", along),
        check_vma=False,
    )
```

```python
import jax
import jax.numpy as jnp
from jax import lax
from jax.experimental import pallas as pl
from jax.experimental.pallas import tpu as pltpu
from jax.sharding import Mesh, PartitionSpec as P


HEADS = 128
GROUPS = 8
GROUP_HEADS = HEADS // GROUPS
LO = 4
META = 32

F32 = jnp.float32
BF16 = jnp.bfloat16


def dot(a, b, ca, cb):
    return lax.dot_general(a, b, (((ca,), (cb,)), ((), ())), preferred_element_type=F32)


def silu(v):
    half = 0.5 * v
    return half + half * jnp.tanh(half)


def log1p(u):
    return jnp.where(u < 1e-3, u * (1.0 - u * (0.5 - u * (1.0 / 3.0))), jnp.log(1.0 + u))


def softplus(v):
    return jnp.maximum(v, 0.0) + log1p(jnp.exp(-jnp.abs(v)))


def picks(first_lane):
    rows = lax.broadcasted_iota(jnp.int32, (8, 128), 0)
    lanes = lax.broadcasted_iota(jnp.int32, (8, 128), 1)
    return jnp.where(jnp.logical_and(lanes == rows + first_lane, rows < 3), 1.0, 0.0).astype(BF16)


def load_kernel(
    group, member, bc, bw, x, dt, xw, xb, bb, bias, a_log, skip,
    last, first, x_out, bc_out, dt_out, x_taps, bc_taps, own_taps, per_head,
):
    channels = x.shape[0]
    heads = dt.shape[0]
    begin, finish = picks(0), picks(125)
    series, mine = x[...], bc[0]
    last[:, :channels] = dot(finish, series[:, 128:], 1, 1).astype(BF16)
    last[:, channels:] = dot(finish, mine[:, 128:], 1, 1).astype(BF16)
    first[:, :channels] = dot(begin, series[:, :128], 1, 1).astype(BF16)
    first[:, channels:] = dot(begin, mine[:, :128], 1, 1).astype(BF16)
    x_out[...] = series
    bc_out[...] = mine
    dt_out[...] = dt[...]
    x_taps[:4, :] = xw[...]
    x_taps[4:, :] = jnp.broadcast_to(xb[...], (4, channels))
    own = jnp.zeros(own_taps.shape[1:], F32)
    for q in range(LO):
        own = jnp.where(member[0] == q, x_taps[:, q * 128 : (q + 1) * 128], own)
    own_taps[0] = own
    bc_taps[:4, :] = bw[0]
    bc_taps[4:, :] = jnp.broadcast_to(chosen(bb[...], group[0]), (4, mine.shape[0]))
    own_taps[1] = bc_taps[:, :128]
    for i, row in enumerate((bias, a_log, skip)):
        per_head[i] = jnp.broadcast_to(column(row[...]), (heads, 128))


def filtered(series, taps):
    lanes = lax.broadcasted_iota(jnp.int32, (series.shape[0], 128), 1)
    first, second = series[:, :128].astype(F32), series[:, 128:].astype(F32)
    a = taps[:, 4:5] + taps[:, 3:4] * first
    b = taps[:, 4:5] + taps[:, 3:4] * second
    for back in (1, 2, 3):
        moved = pltpu.roll(first, back, 1)
        tap = taps[:, 3 - back : 4 - back]
        a = a + tap * moved
        b = b + tap * jnp.where(lanes < back, moved, pltpu.roll(second, back, 1))
    return jnp.concatenate([silu(a), silu(b)], axis=1).astype(BF16)


def column(row):
    size = row.shape[1]
    same = lax.broadcasted_iota(jnp.int32, (size, size), 0) == lax.broadcasted_iota(jnp.int32, (size, size), 1)
    return jnp.sum(jnp.where(same, row, 0.0), axis=1, keepdims=True)


def chosen(table, group):
    rows = lax.broadcasted_iota(jnp.int32, table.shape, 0)
    return jnp.sum(jnp.where(rows == group, table, 0.0), axis=0, keepdims=True)


def split(value):
    high = value.astype(BF16)
    return high, (value - high.astype(F32)).astype(BF16)


def state_kernel(
    z, x, bc, dt, x_taps, bc_taps, per_head, last, first, pay, xc, bcc, cum_out, less_out, z_out, done
):
    fetch = pltpu.make_async_copy(z, z_out, done)
    fetch.start()
    channels = x.shape[0]
    heads = dt.shape[0]
    width = channels // heads
    states = bc.shape[0] // 2

    delta = softplus(dt[...].astype(F32) + per_head[0][:, :1])
    scaled = delta * -jnp.exp(per_head[1][:, :1])
    high = scaled.astype(BF16).astype(F32)
    mid = (scaled - high).astype(BF16).astype(F32)
    size = scaled.shape[1]
    upto = jnp.where(
        lax.broadcasted_iota(jnp.int32, (size, size), 0) <= lax.broadcasted_iota(jnp.int32, (size, size), 1), 1.0, 0.0
    ).astype(BF16)
    sums = dot(jnp.concatenate([scaled - high - mid, mid, high], axis=0).astype(BF16), upto, 1, 0)
    cum = sums[:heads] + sums[heads : 2 * heads] + sums[2 * heads :]
    cum_out[...] = cum
    less_out[...] = cum - jnp.log(delta)
    end = cum[:, size - 1 :]
    gain = delta * jnp.exp(end - cum)
    total_high, total_low = split(jnp.exp(end))
    total_high, total_low = total_high.astype(F32), total_low.astype(F32)

    opening = gain[:, :128].T[:8]
    gains = jnp.concatenate([jnp.broadcast_to(opening[:, h : h + 1], (8, width)) for h in range(heads)], axis=1)
    gain_high = gains.astype(BF16).astype(F32)
    lines = lax.broadcasted_iota(jnp.int32, (8, channels), 0)
    gains = jnp.where(lines < 4, gain_high, pltpu.roll(gains - gain_high, 4, 0))
    lines = lax.broadcasted_iota(jnp.int32, last.shape, 0)
    edges = jnp.where(lines < 3, last[...].astype(F32), pltpu.roll(first[...].astype(F32), 3, 0))

    bcc[...] = filtered(bc[...], bc_taps[...].T)
    b_rows = bcc[:states, :]
    x_cols = x_taps[...].T
    late = jnp.where(lax.broadcasted_iota(jnp.int32, gain.shape, 1) < 3, 0.0, gain)
    lines = lax.broadcasted_iota(jnp.int32, (8, 128), 0)
    per = heads // LO
    for quarter in range(LO):
        tail = jnp.zeros((8, 128), F32)
        for j in range(per):
            h = quarter * per + j
            at = pl.ds(h * width, width)
            values = filtered(x[at, :], x_cols[h * width : (h + 1) * width])
            xc[at, :] = values
            weighted = (values.astype(F32) * late[h : h + 1]).astype(BF16)
            pay[quarter, pl.ds(j * width, width), :] = dot(weighted, b_rows, 1, 1).astype(BF16)
            tail = jnp.where(lines == 2 * j, total_high[h : h + 1], tail)
            tail = jnp.where(lines == 2 * j + 1, total_low[h : h + 1], tail)
        here = slice(quarter * 128, (quarter + 1) * 128)
        rows = jnp.concatenate([tail, edges[:, here], edges[:, channels : channels + 128], gains[:, here]], axis=0)
        pay[quarter, pl.ds(per * width, META), :] = rows.astype(BF16)
    fetch.wait()


def early(series, taps):
    rows = lax.broadcasted_iota(jnp.int32, series.shape, 0)
    total = taps[4:5] + taps[0:1] * series
    for k in (1, 2, 3):
        total = total + taps[k : k + 1] * pltpu.roll(series, 8 - k, 0)
    return jnp.where(rows < 3, silu(total), 0.0).astype(BF16)


def rim_state(before, after, taps):
    rows = lax.broadcasted_iota(jnp.int32, (8, 128), 0)
    x_rows = early(jnp.where(rows < 3, before[8:16], after[8:16]), taps[0])
    b_rows = early(jnp.where(rows < 3, before[16:24], after[16:24]), taps[1])
    gains = after[24:32] + pltpu.roll(after[24:32], 4, 0)
    return dot((x_rows.astype(F32) * gains).astype(BF16), b_rows, 0, 0)


def spread_rows(rows, start, per, size):
    width = size // per
    values = [rows[start + 2 * j : start + 2 * j + 1] + rows[start + 2 * j + 1 : start + 2 * j + 2] for j in range(per)]
    return jnp.concatenate([jnp.broadcast_to(v, (width, 128)) for v in values], axis=0)


def unpack(block):
    size = block.shape[0] - META
    return block[:size].astype(F32), block[size:].astype(F32)


def packed_rows(decay, start, rows, per):
    width = decay.shape[0] // per
    lines = lax.broadcasted_iota(jnp.int32, (8, 128), 0)
    for j in range(per):
        d = decay[j * width : j * width + 1]
        high = d.astype(BF16).astype(F32)
        rows = jnp.where(lines == start + 2 * j, high, rows)
        rows = jnp.where(lines == start + 2 * j + 1, d - high, rows)
    return rows


def group_kernel(got, taps, kept, meta, *refs, per, opening):
    blank_kernel(*refs[1:])
    size = kept.shape[1]
    members = [unpack(got[r]) for r in range(LO)]
    lines = lax.broadcasted_iota(jnp.int32, (META, 128), 0)
    state, rows = members[0]
    if opening:
        state = state + rim_state(jnp.zeros_like(rows), rows, taps)
    kept[0] = state
    decay = spread_rows(rows, 0, per, size)
    suffix = jnp.ones_like(decay)
    for r in range(1, LO):
        fresh, now = members[r]
        fresh = fresh + rim_state(members[r - 1][1], now, taps)
        kept[r] = fresh
        d = spread_rows(now, 0, per, size)
        state = fresh + d * state
        decay, suffix = decay * d, suffix * d
    meta[...] = got[:, size:, :]
    if not refs:
        return
    out = refs[0]
    out[:size, :] = state.astype(BF16)
    head = packed_rows(suffix, 4, packed_rows(decay, 0, jnp.zeros((8, 128), F32), per), per)
    edge = lax.broadcasted_iota(jnp.int32, (16, 128), 0) % 8 < 3
    edges = jnp.where(edge, members[LO - 1][1][8:24], rows[8:24])
    out[size:, :] = jnp.concatenate([head, edges, rows[24:32]], axis=0).astype(BF16)


def join_kernel(earlier, later, taps, out, *, per):
    size = out.shape[0] - META
    before, rows_before = unpack(earlier[...])
    after, rows = unpack(later[...])
    opening = rim_state(rows_before, rows, taps)
    state = after + spread_rows(rows, 4, per, size) * opening + spread_rows(rows, 0, per, size) * before
    out[:size, :] = state.astype(BF16)
    out[size:, :] = later[size:, :]


def entering_kernel(kept, meta, *refs, per, blanks):
    blank_kernel(*refs[len(refs) - blanks :])
    *given, out = refs[: len(refs) - blanks]
    size = kept.shape[1]
    own = meta[0].astype(F32)
    fresh = kept[0]
    state = jnp.zeros(out.shape[1:], F32)
    if len(given) == 2:
        taps, near = given
        state, rows = unpack(near[...])
        fresh = fresh + rim_state(rows, own, taps)
    elif given:
        taps, next_one, over, between = given
        next_one, rows_next = unpack(next_one[...])
        (over, rows_over), (between, rows) = unpack(over[...]), unpack(between[...])
        opening = rim_state(rows_over, rows, taps)
        state = between + spread_rows(rows, 4, per, size) * opening + spread_rows(rows, 0, per, size) * over
        state = state + next_one
        fresh = fresh + rim_state(rows_next + rows, own, taps)
    out[0] = state.astype(BF16)
    for r in range(1, LO):
        state = fresh + spread_rows(meta[r - 1].astype(F32), 0, per, size) * state
        out[r] = state.astype(BF16)
        fresh = kept[r]


def copy_kernel(*refs):
    half = len(refs) // 2
    for source, target in zip(refs[:half], refs[half:]):
        target[...] = source[...]


def pack_kernel(kept, begin, meta, joined, near, kept_out, rows):
    kept_out[...] = kept[...] + begin[...].astype(F32)
    at = 0
    for r in range(LO):
        rows[at : at + META, :] = meta[r]
        at += META
    for block in (joined, near):
        rows[at : at + block.shape[0], :] = block[...]
        at += block.shape[0]


def unpack_kernel(rows, meta, joined, near):
    at = 0
    for r in range(LO):
        meta[r] = rows[at : at + META, :]
        at += META
    for block in (joined, near):
        block[...] = rows[at : at + block.shape[0], :]
        at += block.shape[0]


def begin_kernel(kept, state):
    state[...] = kept[...].astype(BF16)


def blank_kernel(*refs):
    for ref in refs:
        ref[...] = jnp.zeros(ref.shape, ref.dtype)


def intra_kernel(*refs, count):
    rims, refs = refs[:count], refs[count:]
    xc, bcc, first, x_taps, bc_taps, cum_in, less_in, per_head, out, c_out = refs
    heads = cum_in.shape[0]
    channels = xc.shape[0]
    width = channels // heads
    states = bcc.shape[0] // 2
    cum, less = cum_in[...], less_in[...]
    less_cols = jnp.concatenate([less[:, :128].T, less[:, 128:].T], axis=0)
    skips = per_head[2][:, :1]
    lines = lax.broadcasted_iota(jnp.int32, first.shape, 0)
    given = sum(r[...].astype(F32) for r in rims)
    edges = jnp.where(lines < 3, given, pltpu.roll(first[...].astype(F32), 3, 0))
    begun = [early(edges[:, :channels], x_taps[...]), early(edges[:, channels:], bc_taps[...])]
    placed = dot(jnp.concatenate(begun, axis=1), picks(0), 0, 0).astype(BF16)

    def mended(values, rows):
        lanes = lax.broadcasted_iota(jnp.int32, rows.shape, 1)
        return jnp.concatenate([jnp.where(lanes < 3, rows, values[:, :128]), values[:, 128:]], axis=1)

    both = mended(bcc[...], placed[channels:])
    c_out[...] = both[states:]
    gram = dot(both[:states], both[states:], 0, 0)
    keep = lax.broadcasted_iota(jnp.int32, (128, 128), 0) <= lax.broadcasted_iota(jnp.int32, (128, 128), 1)
    for h in range(heads):
        at = pl.ds(h * width, width)
        values = mended(xc[at, :], placed[h * width : (h + 1) * width])
        row = cum[h : h + 1]
        col = less_cols[:, h : h + 1]

        def mix(s, t, masked):
            spread = row[:, t : t + 128] - col[s : s + 128]
            if masked:
                spread = jnp.where(keep, spread, -1e30)
            return (gram[s : s + 128, t : t + 128] * jnp.exp(spread)).astype(BF16)

        near = dot(values[:, :128], mix(0, 0, True), 1, 0)
        late = dot(values, jnp.concatenate([mix(0, 128, False), mix(128, 128, True)], axis=0), 1, 0)
        out[at, :] = jnp.concatenate([near, late], axis=1) + skips[h : h + 1] * values.astype(F32)


def output_kernel(inner, c_rows, cum, state, z, out, held, done):
    heads = cum.shape[0]
    width = inner.shape[0] // heads
    per = heads // LO
    grown = jnp.exp(cum[...])
    copies = []
    for h in range(heads):
        at = pl.ds(h * width, width)
        y = inner[at, :] + grown[h : h + 1] * dot(state[at, :], c_rows[...], 1, 0)
        y = y.astype(BF16).astype(F32)
        held[at, :] = (y * silu(z[at, :].astype(F32))).astype(BF16)
        if h % per == per - 1:
            part = pl.ds((h + 1 - per) * width, per * width)
            copies.append(pltpu.make_async_copy(held.at[part], out.at[part], done.at[h // per]))
            copies[-1].start()
    for copy in copies:
        copy.wait()


def shape(*dims, dtype=F32):
    return pltpu.VMEM(dims, dtype)


VMEM = pl.BlockSpec(memory_space=pltpu.VMEM)
GRANT = pltpu.CompilerParams(vmem_limit_bytes=12 << 20)


def run(kernel, outs, *args):
    args = [pltpu.with_memory_space_constraint(a, pltpu.VMEM) for a in args]
    return pl.pallas_call(
        kernel, out_shape=outs, in_specs=[VMEM] * len(args), out_specs=[VMEM] * len(outs), compiler_params=GRANT
    )(*args)


def local(x_in, z_gate, bc_in, dt_raw, conv_x_w, conv_x_b, conv_bc_w, conv_bc_b, dt_bias, a_log, d_skip):
    heads, length = dt_raw.shape
    channels = x_in.shape[0]
    rows = bc_in.shape[1]
    states = rows // 2
    per = heads // LO
    quarter = channels // LO
    group = (lax.axis_index("tensor") // (GROUP_HEADS // heads)).astype(jnp.int32).reshape(1)
    member = lax.axis_index("near").astype(jnp.int32).reshape(1)
    far = lax.axis_index("far")
    cp = ("far", "near")
    count = lax.axis_size(cp)

    strip = shape(8, channels + rows, dtype=BF16)
    block_shape = shape(quarter + META, states, dtype=BF16)
    kept_shapes = [shape(LO, quarter, states), shape(LO, META, states, dtype=BF16)]
    state_shape = shape(LO, quarter, states, dtype=BF16)
    series = shape(channels, length, dtype=BF16)
    pairs = shape(rows, length, dtype=BF16)
    taps = jnp.swapaxes(conv_bc_w, 1, 2)
    small = [dt_raw, conv_x_w.T, conv_x_b[None], conv_bc_b, dt_bias[None], a_log[None], d_skip[None]]
    outs = [strip, strip, series, pairs, shape(heads, length, dtype=BF16), shape(8, channels), shape(8, rows)]
    outs += [shape(2, 8, 128), shape(3, heads, 128)]
    last, first, x, bc, dt, x_taps, bc_taps, own_taps, per_head = pl.pallas_call(
        load_kernel,
        grid_spec=pltpu.PrefetchScalarGridSpec(
            num_scalar_prefetch=2,
            grid=(1,),
            in_specs=[pl.BlockSpec((1,) + a.shape[1:], lambda i, g, m: (g[0], 0, 0)) for a in (bc_in, taps)]
            + [pl.BlockSpec(a.shape, lambda i, g, m: (0, 0)) for a in [x_in] + small],
            out_specs=[VMEM] * len(outs),
        ),
        out_shape=outs,
        name="load",
        compiler_params=GRANT,
    )(group, member, *[pltpu.with_memory_space_constraint(a, pltpu.HBM) for a in (bc_in, taps, x_in, *small)])
    outs = [shape(LO, quarter + META, states, dtype=BF16), series, pairs]
    outs += [shape(heads, length), shape(heads, length), series]
    args = [x, bc, dt, x_taps, bc_taps, per_head, last, first]
    pay, xc, bcc, cum, less, z = pl.pallas_call(
        state_kernel,
        out_shape=outs,
        in_specs=[pl.BlockSpec(memory_space=pl.ANY)] + [VMEM] * len(args),
        out_specs=[VMEM] * len(outs),
        scratch_shapes=[pltpu.SemaphoreType.DMA],
        name="states",
        compiler_params=GRANT,
    )(
        pltpu.with_memory_space_constraint(z_gate, pltpu.HBM),
        *[pltpu.with_memory_space_constraint(a, pltpu.VMEM) for a in args],
    )

    def gather(*rest, opening=False):
        got = lax.all_to_all(pay, "near", 0, 0, tiled=True)
        kernel = lambda *refs: group_kernel(*refs, per=per, opening=opening)
        return tuple(run(kernel, [*kept_shapes, *rest], got, own_taps))

    def blank(*outs):
        return tuple(run(blank_kernel, list(outs)))

    def exchange(*given, blanks=()):
        kernel = lambda *refs: entering_kernel(*refs, per=per, blanks=len(blanks))
        entering, *rest = run(kernel, [state_shape, *blanks], *given)
        return tuple(rest) + (lax.all_to_all(entering, "near", 0, 0, tiled=True),)

    def sent(block, source, target):
        route = [(source * LO + i, target * LO + i) for i in range(LO)]
        return lax.ppermute(block, cp, route)

    def kept_on(*arrays):
        return tuple(run(copy_kernel, [shape(*a.shape, dtype=a.dtype) for a in arrays], *arrays))

    def inside(*rims):
        args = [*rims, xc, bcc, first, x_taps, bc_taps, cum, less, per_head]
        return tuple(run(lambda *refs: intra_kernel(*refs, count=len(rims)), inner_shapes, *args))

    def shifted(begin, end):
        return lax.ppermute(kept_on(last)[0], cp, [(i, i + 1) for i in range(begin, end)])

    inner_shapes = [shape(channels, length), shape(states, length, dtype=BF16)]

    packed_rows_count = LO * META + 2 * (quarter + META)
    packed_shapes = [kept_shapes[0], shape(packed_rows_count, states, dtype=BF16)]

    def low_part():
        kept = lax.cond(
            far == 0, lambda: gather(block_shape, opening=True), lambda: blank(*kept_shapes, block_shape)
        )
        near = sent(kept[2], 0, 1)
        rims = shifted(0, 2 * LO - 1)
        *kept, begin = lax.cond(
            far == 0,
            lambda *kept: exchange(*kept[:2], blanks=(*kept_shapes, block_shape)),
            lambda *kept: gather(block_shape, state_shape),
            *kept,
        )
        packed = run(pack_kernel, packed_shapes, kept[0], begin, kept[1], kept[2], near)
        return (*packed, *kept_on(rims))

    def high_part(*kept):
        rims = shifted(2 * LO, count - 1)
        kept = lax.cond(far == 2, lambda *kept: gather(block_shape), lambda *kept: blank(*kept_shapes, block_shape), *kept)
        between = sent(kept[2], 2, 3)
        kept = lax.cond(far == 3, lambda *kept: gather(), kept_on, *kept[:2])
        return kept_on(*kept, between, rims) + blank(state_shape)

    def later_part(kept, packed, rims_low):
        meta, block, near = run(unpack_kernel, [kept_shapes[1], block_shape, block_shape], packed)
        (joined,) = run(lambda *refs: join_kernel(*refs, per=per), [block_shape], near, block, own_taps)
        over = sent(joined, 1, 3)
        next_one = sent(joined, 1, 2)
        rims_mid = shifted(2 * LO - 1, 2 * LO)
        *kept, between, rims, state = lax.cond(
            far >= 2,
            lambda *kept: high_part(*kept),
            lambda *kept: exchange(*kept, own_taps, near, blanks=(*kept_shapes, block_shape, strip)),
            kept,
            meta,
        )
        inner = inside(rims_low, rims_mid, rims)
        between, *inner = lax.optimization_barrier((between, *inner))
        (state,) = lax.cond(
            far >= 2,
            lambda state, *given: exchange(*given),
            lambda state, *given: kept_on(state),
            state,
            *kept,
            own_taps,
            next_one,
            over,
            between,
        )
        return (state, *inner)

    parts = lax.cond(far < 2, low_part, lambda: blank(*packed_shapes, strip))
    state, inner, c_rows = lax.cond(
        far == 0,
        lambda kept, packed, rims: tuple(run(begin_kernel, [state_shape], kept)) + inside(rims),
        later_part,
        *parts,
    )
    inputs = [inner, c_rows, cum, state.reshape(channels, states), z]
    return pl.pallas_call(
        output_kernel,
        out_shape=jax.ShapeDtypeStruct((channels, length), BF16),
        in_specs=[VMEM] * len(inputs),
        out_specs=pl.BlockSpec(memory_space=pl.ANY),
        scratch_shapes=[pltpu.VMEM((channels, length), BF16), pltpu.SemaphoreType.DMA((LO,))],
        name="gated",
    compiler_params=GRANT,
    )(*[pltpu.with_memory_space_constraint(a, pltpu.VMEM) for a in inputs])


def solution(mesh):
    dp, cp, tensor = mesh.devices.shape
    finer = Mesh(mesh.devices.reshape(dp, cp // LO, LO, tensor), ("dp", "far", "near", "tensor"))
    along = ("dp", "far", "near")
    return jax.shard_map(
        local,
        mesh=finer,
        in_specs=(
            P("tensor", along),
            P("tensor", along),
            P(None, None, along),
            P("tensor", along),
            P("tensor", None),
            P("tensor"),
            P(),
            P(),
            P("tensor"),
            P("tensor"),
            P("tensor"),
        ),
        out_specs=P("tensor", along),
        check_vma=False,
    )
```

```python
import jax
import jax.numpy as jnp
from jax import lax
from jax.experimental import pallas as pl
from jax.experimental.pallas import tpu as pltpu
from jax.sharding import Mesh, PartitionSpec as P


HEADS = 128
GROUPS = 8
GROUP_HEADS = HEADS // GROUPS
LO = 4
META = 32

F32 = jnp.float32
BF16 = jnp.bfloat16


def dot(a, b, ca, cb):
    return lax.dot_general(a, b, (((ca,), (cb,)), ((), ())), preferred_element_type=F32)


def silu(v):
    half = 0.5 * v
    return half + half * jnp.tanh(half)


def log1p(u):
    return jnp.where(u < 1e-3, u * (1.0 - u * (0.5 - u * (1.0 / 3.0))), jnp.log(1.0 + u))


def softplus(v):
    return jnp.maximum(v, 0.0) + log1p(jnp.exp(-jnp.abs(v)))


def picks(first_lane):
    rows = lax.broadcasted_iota(jnp.int32, (8, 128), 0)
    lanes = lax.broadcasted_iota(jnp.int32, (8, 128), 1)
    return jnp.where(jnp.logical_and(lanes == rows + first_lane, rows < 3), 1.0, 0.0).astype(BF16)


def load_kernel(
    group, member, bc, bw, x, dt, xw, xb, bb, bias, a_log, skip,
    last, first, x_out, bc_out, dt_out, x_taps, bc_taps, own_taps, per_head,
):
    channels = x.shape[0]
    heads = dt.shape[0]
    begin, finish = picks(0), picks(125)
    series, mine = x[...], bc[0]
    last[:, :channels] = dot(finish, series[:, 128:], 1, 1).astype(BF16)
    last[:, channels:] = dot(finish, mine[:, 128:], 1, 1).astype(BF16)
    first[:, :channels] = dot(begin, series[:, :128], 1, 1).astype(BF16)
    first[:, channels:] = dot(begin, mine[:, :128], 1, 1).astype(BF16)
    x_out[...] = series
    bc_out[...] = mine
    dt_out[...] = dt[...]
    x_taps[:4, :] = xw[...]
    x_taps[4:, :] = jnp.broadcast_to(xb[...], (4, channels))
    own = jnp.zeros(own_taps.shape[1:], F32)
    for q in range(LO):
        own = jnp.where(member[0] == q, x_taps[:, q * 128 : (q + 1) * 128], own)
    own_taps[0] = own
    bc_taps[:4, :] = bw[0]
    bc_taps[4:, :] = jnp.broadcast_to(chosen(bb[...], group[0]), (4, mine.shape[0]))
    own_taps[1] = bc_taps[:, :128]
    for i, row in enumerate((bias, a_log, skip)):
        per_head[i] = jnp.broadcast_to(column(row[...]), (heads, 128))


def filtered(series, taps):
    lanes = lax.broadcasted_iota(jnp.int32, (series.shape[0], 128), 1)
    first, second = series[:, :128].astype(F32), series[:, 128:].astype(F32)
    wide = [taps[:, k * 128 : (k + 1) * 128] for k in range(5)]
    a = wide[4] + wide[3] * first
    b = wide[4] + wide[3] * second
    for back in (1, 2, 3):
        moved = pltpu.roll(first, back, 1)
        a = a + wide[3 - back] * moved
        b = b + wide[3 - back] * jnp.where(lanes < back, moved, pltpu.roll(second, back, 1))
    return jnp.concatenate([silu(a), silu(b)], axis=1)


def thirds(value):
    high = value.astype(BF16).astype(F32)
    mid = (value - high).astype(BF16).astype(F32)
    return jnp.concatenate([high, mid, value - high - mid], axis=0).astype(BF16)


def column(row):
    size = row.shape[1]
    same = lax.broadcasted_iota(jnp.int32, (size, size), 0) == lax.broadcasted_iota(jnp.int32, (size, size), 1)
    return jnp.sum(jnp.where(same, row, 0.0), axis=1, keepdims=True)


def chosen(table, group):
    rows = lax.broadcasted_iota(jnp.int32, table.shape, 0)
    return jnp.sum(jnp.where(rows == group, table, 0.0), axis=0, keepdims=True)


def split(value):
    high = value.astype(BF16)
    return high, (value - high.astype(F32)).astype(BF16)


def state_kernel(
    z, x, bc, dt, x_taps, bc_taps, per_head, last, first, pay, xc, bcc, cum_out, less_out, z_out, done, weighted, cols
):
    fetch = pltpu.make_async_copy(z, z_out, done)
    fetch.start()
    channels = x.shape[0]
    heads = dt.shape[0]
    width = channels // heads
    states = bc.shape[0] // 2

    delta = softplus(dt[...].astype(F32) + per_head[0][:, :1])
    scaled = delta * -jnp.exp(per_head[1][:, :1])
    size = scaled.shape[1]
    upto = jnp.where(
        lax.broadcasted_iota(jnp.int32, (size, size), 0) <= lax.broadcasted_iota(jnp.int32, (size, size), 1), 1.0, 0.0
    ).astype(BF16)
    sums = dot(thirds(scaled), upto, 1, 0)
    cum = sums[2 * heads :] + sums[heads : 2 * heads] + sums[:heads]
    cum_out[...] = cum
    less_out[...] = cum - jnp.log(delta)
    end = cum[:, size - 1 :]
    gain = delta * jnp.exp(end - cum)
    total_high, total_low = split(jnp.exp(end))
    total_high, total_low = total_high.astype(F32), total_low.astype(F32)

    opening = gain[:, :128].T[:8]
    gains = jnp.concatenate([jnp.broadcast_to(opening[:, h : h + 1], (8, width)) for h in range(heads)], axis=1)
    gain_high = gains.astype(BF16).astype(F32)
    lines = lax.broadcasted_iota(jnp.int32, (8, channels), 0)
    gains = jnp.where(lines < 4, gain_high, pltpu.roll(gains - gain_high, 4, 0))
    lines = lax.broadcasted_iota(jnp.int32, last.shape, 0)
    edges = jnp.where(lines < 3, last[...].astype(F32), pltpu.roll(first[...].astype(F32), 3, 0))

    kinds = lax.broadcasted_iota(jnp.int32, (24, 5 * 128), 1) // 128
    picked = jnp.where(lax.broadcasted_iota(jnp.int32, (24, 5 * 128), 0) % 8 == kinds, 1.0, 0.0).astype(BF16)
    cols[...] = dot(thirds(jnp.concatenate([x_taps[...], bc_taps[...]], axis=1)), picked, 0, 0)
    for start in range(0, 2 * states, width):
        at = pl.ds(start, width)
        bcc[at, :] = filtered(bc[at, :], cols[pl.ds(channels + start, width), :]).astype(BF16)
    late = jnp.where(lax.broadcasted_iota(jnp.int32, gain.shape, 1) < 3, 0.0, gain)
    lines = lax.broadcasted_iota(jnp.int32, (8, 128), 0)
    per = heads // LO
    for quarter in range(LO):
        tail = jnp.zeros((8, 128), F32)
        for j in range(per):
            h = quarter * per + j
            at = pl.ds(h * width, width)
            values = filtered(x[at, :], cols[at, :])
            xc[at, :] = values.astype(BF16)
            weighted[at, :] = (values * late[h : h + 1]).astype(BF16)
            tail = jnp.where(lines == 2 * j, total_high[h : h + 1], tail)
            tail = jnp.where(lines == 2 * j + 1, total_low[h : h + 1], tail)
        here = slice(quarter * 128, (quarter + 1) * 128)
        rows = jnp.concatenate([tail, edges[:, here], edges[:, channels : channels + 128], gains[:, here]], axis=0)
        pay[quarter, pl.ds(per * width, META), :] = rows.astype(BF16)
    fresh = dot(weighted[...], bcc[:states, :], 1, 1).astype(BF16)
    for quarter in range(LO):
        size = per * width
        pay[quarter, pl.ds(0, size), :] = fresh[quarter * size : (quarter + 1) * size]
    fetch.wait()


def early(series, taps):
    rows = lax.broadcasted_iota(jnp.int32, series.shape, 0)
    total = taps[4:5] + taps[0:1] * series
    for k in (1, 2, 3):
        total = total + taps[k : k + 1] * pltpu.roll(series, 8 - k, 0)
    return jnp.where(rows < 3, silu(total), 0.0).astype(BF16)


def rim_state(before, after, taps):
    rows = lax.broadcasted_iota(jnp.int32, (8, 128), 0)
    x_rows = early(jnp.where(rows < 3, before[8:16], after[8:16]), taps[0])
    b_rows = early(jnp.where(rows < 3, before[16:24], after[16:24]), taps[1])
    gains = after[24:32] + pltpu.roll(after[24:32], 4, 0)
    return dot((x_rows.astype(F32) * gains).astype(BF16), b_rows, 0, 0)


def spread_rows(rows, start, per, size):
    width = size // per
    values = [rows[start + 2 * j : start + 2 * j + 1] + rows[start + 2 * j + 1 : start + 2 * j + 2] for j in range(per)]
    return jnp.concatenate([jnp.broadcast_to(v, (width, 128)) for v in values], axis=0)


def unpack(block):
    size = block.shape[0] - META
    return block[:size].astype(F32), block[size:].astype(F32)


def packed_rows(decay, start, rows, per):
    width = decay.shape[0] // per
    lines = lax.broadcasted_iota(jnp.int32, (8, 128), 0)
    for j in range(per):
        d = decay[j * width : j * width + 1]
        high = d.astype(BF16).astype(F32)
        rows = jnp.where(lines == start + 2 * j, high, rows)
        rows = jnp.where(lines == start + 2 * j + 1, d - high, rows)
    return rows


def group_kernel(got, taps, kept, meta, *refs, per, opening):
    blank_kernel(*refs[1:])
    size = kept.shape[1]
    members = [unpack(got[r]) for r in range(LO)]
    lines = lax.broadcasted_iota(jnp.int32, (META, 128), 0)
    state, rows = members[0]
    if opening:
        state = state + rim_state(jnp.zeros_like(rows), rows, taps)
    kept[0] = state
    decay = spread_rows(rows, 0, per, size)
    suffix = jnp.ones_like(decay)
    for r in range(1, LO):
        fresh, now = members[r]
        fresh = fresh + rim_state(members[r - 1][1], now, taps)
        kept[r] = fresh
        d = spread_rows(now, 0, per, size)
        state = fresh + d * state
        decay, suffix = decay * d, suffix * d
    meta[...] = got[:, size:, :]
    if not refs:
        return
    out = refs[0]
    out[:size, :] = state.astype(BF16)
    head = packed_rows(suffix, 4, packed_rows(decay, 0, jnp.zeros((8, 128), F32), per), per)
    edge = lax.broadcasted_iota(jnp.int32, (16, 128), 0) % 8 < 3
    edges = jnp.where(edge, members[LO - 1][1][8:24], rows[8:24])
    out[size:, :] = jnp.concatenate([head, edges, rows[24:32]], axis=0).astype(BF16)


def join_kernel(earlier, later, taps, out, *, per):
    size = out.shape[0] - META
    before, rows_before = unpack(earlier[...])
    after, rows = unpack(later[...])
    opening = rim_state(rows_before, rows, taps)
    state = after + spread_rows(rows, 4, per, size) * opening + spread_rows(rows, 0, per, size) * before
    out[:size, :] = state.astype(BF16)
    out[size:, :] = later[size:, :]


def entering_kernel(kept, meta, *refs, per, blanks):
    blank_kernel(*refs[len(refs) - blanks :])
    *given, out = refs[: len(refs) - blanks]
    size = kept.shape[1]
    own = meta[0].astype(F32)
    fresh = kept[0]
    state = jnp.zeros(out.shape[1:], F32)
    if len(given) == 2:
        taps, near = given
        state, rows = unpack(near[...])
        fresh = fresh + rim_state(rows, own, taps)
    elif given:
        taps, next_one, over, between = given
        next_one, rows_next = unpack(next_one[...])
        (over, rows_over), (between, rows) = unpack(over[...]), unpack(between[...])
        opening = rim_state(rows_over, rows, taps)
        state = between + spread_rows(rows, 4, per, size) * opening + spread_rows(rows, 0, per, size) * over
        state = state + next_one
        fresh = fresh + rim_state(rows_next + rows, own, taps)
    out[0] = state.astype(BF16)
    for r in range(1, LO):
        state = fresh + spread_rows(meta[r - 1].astype(F32), 0, per, size) * state
        out[r] = state.astype(BF16)
        fresh = kept[r]


def copy_kernel(*refs):
    half = len(refs) // 2
    for source, target in zip(refs[:half], refs[half:]):
        target[...] = source[...]


def pack_kernel(kept, begin, meta, joined, near, kept_out, rows):
    kept_out[...] = kept[...] + begin[...].astype(F32)
    at = 0
    for r in range(LO):
        rows[at : at + META, :] = meta[r]
        at += META
    for block in (joined, near):
        rows[at : at + block.shape[0], :] = block[...]
        at += block.shape[0]


def unpack_kernel(rows, meta, joined, near):
    at = 0
    for r in range(LO):
        meta[r] = rows[at : at + META, :]
        at += META
    for block in (joined, near):
        block[...] = rows[at : at + block.shape[0], :]
        at += block.shape[0]


def begin_kernel(kept, unused, state, *blanks):
    state[...] = kept[...].astype(BF16)
    blank_kernel(*blanks)


def blank_kernel(*refs):
    for ref in refs:
        ref[...] = jnp.zeros(ref.shape, ref.dtype)


def intra_kernel(xc, bcc, cum_in, less_in, per_head, out):
    heads = cum_in.shape[0]
    width = xc.shape[0] // heads
    states = bcc.shape[0] // 2
    cum, less = cum_in[...], less_in[...]
    less_cols = jnp.concatenate([less[:, :128].T, less[:, 128:].T], axis=0)
    skips = per_head[2][:, :1]
    gram = dot(bcc[:states, :], bcc[states:, :], 0, 0)
    gram = jnp.where(lax.broadcasted_iota(jnp.int32, gram.shape, 0) < 3, 0.0, gram)
    keep = lax.broadcasted_iota(jnp.int32, (128, 128), 0) <= lax.broadcasted_iota(jnp.int32, (128, 128), 1)
    lanes = lax.broadcasted_iota(jnp.int32, (width, 256), 1)
    for h in range(heads):
        at = pl.ds(h * width, width)
        values = xc[at, :]
        row = cum[h : h + 1]
        col = less_cols[:, h : h + 1]

        def mix(s, t, masked):
            spread = row[:, t : t + 128] - col[s : s + 128]
            if masked:
                spread = jnp.where(keep, spread, -1e30)
            return (gram[s : s + 128, t : t + 128] * jnp.exp(spread)).astype(BF16)

        near = dot(values[:, :128], mix(0, 0, True), 1, 0)
        late = dot(values, jnp.concatenate([mix(0, 128, False), mix(128, 128, True)], axis=0), 1, 0)
        kept = jnp.where(lanes < 3, 0.0, values.astype(F32))
        out[at, :] = jnp.concatenate([near, late], axis=1) + skips[h : h + 1] * kept


def output_kernel(
    low, high, bcc, rims_low, rims_mid, rims_high, first, x_taps, bc_taps, cum_in, less, per_head, state, z, out, held, done
):
    heads = cum_in.shape[0]
    channels = low.shape[0]
    width = channels // heads
    states = state.shape[1]
    per = heads // LO
    lines = lax.broadcasted_iota(jnp.int32, first.shape, 0)
    given = rims_low[...].astype(F32) + rims_mid[...].astype(F32) + rims_high[...].astype(F32)
    edges = jnp.where(lines < 3, given, pltpu.roll(first[...].astype(F32), 3, 0))
    x_rows = early(edges[:, :channels], x_taps[...])
    bc_rows = early(edges[:, channels:], bc_taps[...])
    x_placed = dot(x_rows, picks(0), 0, 0)
    c_placed = dot(bc_rows[:, states:], picks(0), 0, 0).astype(BF16)
    lanes = lax.broadcasted_iota(jnp.int32, c_placed.shape, 1)
    c_rows = bcc[states:, :]
    c_rows = jnp.concatenate([jnp.where(lanes < 3, c_placed, c_rows[:, :128]), c_rows[:, 128:]], axis=1)
    gram = dot(bc_rows[:, :states], c_rows, 1, 0)
    cum = cum_in[...]
    grown = jnp.exp(cum)
    less_cols = less[:, :128].T[:8]
    keep = lax.broadcasted_iota(jnp.int32, gram.shape, 0) <= lax.broadcasted_iota(jnp.int32, gram.shape, 1)
    skips = per_head[2][:, :1]
    copies = []
    for h in range(heads):
        at = pl.ds(h * width, width)
        spread = jnp.where(keep, cum[h : h + 1] - less_cols[:, h : h + 1], -1e30)
        mixing = (gram * jnp.exp(spread)).astype(BF16)
        opening = dot(x_rows[:, h * width : (h + 1) * width], mixing, 0, 0)
        skipped = skips[h : h + 1] * x_placed[h * width : (h + 1) * width]
        y = low[at, :] + high[at, :] + opening + grown[h : h + 1] * dot(state[at, :], c_rows, 1, 0)
        y = jnp.concatenate([y[:, :128] + skipped, y[:, 128:]], axis=1)
        y = y.astype(BF16).astype(F32)
        held[at, :] = (y * silu(z[at, :].astype(F32))).astype(BF16)
        if h % per == per - 1:
            part = pl.ds((h + 1 - per) * width, per * width)
            copies.append(pltpu.make_async_copy(held.at[part], out.at[part], done.at[h // per]))
            copies[-1].start()
    for copy in copies:
        copy.wait()


def shape(*dims, dtype=F32):
    return pltpu.VMEM(dims, dtype)


VMEM = pl.BlockSpec(memory_space=pltpu.VMEM)
GRANT = pltpu.CompilerParams(vmem_limit_bytes=12 << 20)


def run(kernel, outs, *args):
    args = [pltpu.with_memory_space_constraint(a, pltpu.VMEM) for a in args]
    return pl.pallas_call(
        kernel, out_shape=outs, in_specs=[VMEM] * len(args), out_specs=[VMEM] * len(outs), compiler_params=GRANT
    )(*args)


def local(x_in, z_gate, bc_in, dt_raw, conv_x_w, conv_x_b, conv_bc_w, conv_bc_b, dt_bias, a_log, d_skip):
    heads, length = dt_raw.shape
    channels = x_in.shape[0]
    rows = bc_in.shape[1]
    states = rows // 2
    per = heads // LO
    quarter = channels // LO
    group = (lax.axis_index("tensor") // (GROUP_HEADS // heads)).astype(jnp.int32).reshape(1)
    member = lax.axis_index("near").astype(jnp.int32).reshape(1)
    far = lax.axis_index("far")
    cp = ("far", "near")
    count = lax.axis_size(cp)

    strip = shape(8, channels + rows, dtype=BF16)
    block_shape = shape(quarter + META, states, dtype=BF16)
    kept_shapes = [shape(LO, quarter, states), shape(LO, META, states, dtype=BF16)]
    state_shape = shape(LO, quarter, states, dtype=BF16)
    series = shape(channels, length, dtype=BF16)
    pairs = shape(rows, length, dtype=BF16)
    taps = jnp.swapaxes(conv_bc_w, 1, 2)
    small = [dt_raw, conv_x_w.T, conv_x_b[None], conv_bc_b, dt_bias[None], a_log[None], d_skip[None]]
    outs = [strip, strip, series, pairs, shape(heads, length, dtype=BF16), shape(8, channels), shape(8, rows)]
    outs += [shape(2, 8, 128), shape(3, heads, 128)]
    last, first, x, bc, dt, x_taps, bc_taps, own_taps, per_head = pl.pallas_call(
        load_kernel,
        grid_spec=pltpu.PrefetchScalarGridSpec(
            num_scalar_prefetch=2,
            grid=(1,),
            in_specs=[pl.BlockSpec((1,) + a.shape[1:], lambda i, g, m: (g[0], 0, 0)) for a in (bc_in, taps)]
            + [pl.BlockSpec(a.shape, lambda i, g, m: (0, 0)) for a in [x_in] + small],
            out_specs=[VMEM] * len(outs),
        ),
        out_shape=outs,
        name="load",
        compiler_params=GRANT,
    )(group, member, *[pltpu.with_memory_space_constraint(a, pltpu.HBM) for a in (bc_in, taps, x_in, *small)])
    outs = [shape(LO, quarter + META, states, dtype=BF16), series, pairs]
    outs += [shape(heads, length), shape(heads, length), series]
    args = [x, bc, dt, x_taps, bc_taps, per_head, last, first]
    pay, xc, bcc, cum, less, z = pl.pallas_call(
        state_kernel,
        out_shape=outs,
        in_specs=[pl.BlockSpec(memory_space=pl.ANY)] + [VMEM] * len(args),
        out_specs=[VMEM] * len(outs),
        scratch_shapes=[
            pltpu.SemaphoreType.DMA,
            pltpu.VMEM((channels, length), BF16),
            pltpu.VMEM((channels + rows, 5 * 128), F32),
        ],
        name="states",
        compiler_params=GRANT,
    )(
        pltpu.with_memory_space_constraint(z_gate, pltpu.HBM),
        *[pltpu.with_memory_space_constraint(a, pltpu.VMEM) for a in args],
    )

    def gather(*rest, opening=False):
        got = lax.all_to_all(pay, "near", 0, 0, tiled=True)
        kernel = lambda *refs: group_kernel(*refs, per=per, opening=opening)
        return tuple(run(kernel, [*kept_shapes, *rest], got, own_taps))

    def blank(*outs):
        return tuple(run(blank_kernel, list(outs)))

    def exchange(*given, blanks=()):
        kernel = lambda *refs: entering_kernel(*refs, per=per, blanks=len(blanks))
        entering, *rest = run(kernel, [state_shape, *blanks], *given)
        return tuple(rest) + (lax.all_to_all(entering, "near", 0, 0, tiled=True),)

    def sent(block, source, target):
        route = [(source * LO + i, target * LO + i) for i in range(LO)]
        return lax.ppermute(block, cp, route)

    def kept_on(*arrays):
        return tuple(run(copy_kernel, [shape(*a.shape, dtype=a.dtype) for a in arrays], *arrays))

    def inside(after):
        _, values = lax.optimization_barrier((after, xc))
        return run(intra_kernel, [inner_shape], values, bcc, cum, less, per_head)[0]

    def shifted(begin, end):
        return lax.ppermute(kept_on(last)[0], cp, [(i, i + 1) for i in range(begin, end)])

    inner_shape = shape(channels, length)

    packed_rows_count = LO * META + 2 * (quarter + META)
    packed_shapes = [kept_shapes[0], shape(packed_rows_count, states, dtype=BF16)]

    def low_part():
        kept = lax.cond(
            far == 0, lambda: gather(block_shape, opening=True), lambda: blank(*kept_shapes, block_shape)
        )
        near = sent(kept[2], 0, 1)
        rims = shifted(0, 2 * LO - 1)
        *kept, begin = lax.cond(
            far == 0,
            lambda *kept: exchange(*kept[:2], blanks=(*kept_shapes, block_shape)),
            lambda *kept: gather(block_shape, state_shape),
            *kept,
        )
        inner = inside(begin)
        packed = run(pack_kernel, packed_shapes, kept[0], begin, kept[1], kept[2], near)
        return (*packed, *kept_on(rims), inner)

    def high_part(*kept):
        rims = shifted(2 * LO, count - 1)
        kept = lax.cond(far == 2, lambda *kept: gather(block_shape), lambda *kept: blank(*kept_shapes, block_shape), *kept)
        between = sent(kept[2], 2, 3)
        kept = lax.cond(far == 3, lambda *kept: gather(), kept_on, *kept[:2])
        inner = inside(kept[0])
        return kept_on(*kept, between, rims) + (inner,) + blank(state_shape)

    def later_part(kept, packed):
        meta, block, near = run(unpack_kernel, [kept_shapes[1], block_shape, block_shape], packed)
        (joined,) = run(lambda *refs: join_kernel(*refs, per=per), [block_shape], near, block, own_taps)
        over = sent(joined, 1, 3)
        next_one = sent(joined, 1, 2)
        rims_mid = shifted(2 * LO - 1, 2 * LO)
        *kept, between, rims, inner, state = lax.cond(
            far >= 2,
            high_part,
            lambda *kept: exchange(*kept, own_taps, near, blanks=(*kept_shapes, block_shape, strip, inner_shape)),
            kept,
            meta,
        )
        (state,) = lax.cond(
            far >= 2,
            lambda state, *given: exchange(*given),
            lambda state, *given: kept_on(state),
            state,
            *kept,
            own_taps,
            next_one,
            over,
            between,
        )
        return (state, inner, rims_mid, rims)

    kept, packed, rims_low, inner_low = lax.cond(far < 2, low_part, lambda: blank(*packed_shapes, strip, inner_shape))
    state, inner, rims_mid, rims = lax.cond(
        far == 0,
        lambda kept, packed: tuple(run(begin_kernel, [state_shape, inner_shape, strip, strip], kept, packed)),
        later_part,
        kept,
        packed,
    )
    inputs = [inner_low, inner, bcc, rims_low, rims_mid, rims, first, x_taps, bc_taps, cum, less, per_head]
    inputs += [state.reshape(channels, states), z]
    return pl.pallas_call(
        output_kernel,
        out_shape=jax.ShapeDtypeStruct((channels, length), BF16),
        in_specs=[VMEM] * len(inputs),
        out_specs=pl.BlockSpec(memory_space=pl.ANY),
        scratch_shapes=[pltpu.VMEM((channels, length), BF16), pltpu.SemaphoreType.DMA((LO,))],
        name="gated",
    compiler_params=GRANT,
    )(*[pltpu.with_memory_space_constraint(a, pltpu.VMEM) for a in inputs])


def solution(mesh):
    dp, cp, tensor = mesh.devices.shape
    finer = Mesh(mesh.devices.reshape(dp, cp // LO, LO, tensor), ("dp", "far", "near", "tensor"))
    along = ("dp", "far", "near")
    return jax.shard_map(
        local,
        mesh=finer,
        in_specs=(
            P("tensor", along),
            P("tensor", along),
            P(None, None, along),
            P("tensor", along),
            P("tensor", None),
            P("tensor"),
            P(),
            P(),
            P("tensor"),
            P("tensor"),
            P("tensor"),
        ),
        out_specs=P("tensor", along),
        check_vma=False,
    )
```

```python
import jax
import jax.numpy as jnp
from jax import lax
from jax.experimental import pallas as pl
from jax.experimental.pallas import tpu as pltpu
from jax.sharding import Mesh, PartitionSpec as P


HEADS = 128
GROUPS = 8
GROUP_HEADS = HEADS // GROUPS
LO = 4
META = 32

F32 = jnp.float32
BF16 = jnp.bfloat16


def dot(a, b, ca, cb):
    return lax.dot_general(a, b, (((ca,), (cb,)), ((), ())), preferred_element_type=F32)


def silu(v):
    half = 0.5 * v
    return half + half * jnp.tanh(half)


def log1p(u):
    return jnp.where(u < 1e-3, u * (1.0 - u * (0.5 - u * (1.0 / 3.0))), jnp.log(1.0 + u))


def softplus(v):
    return jnp.maximum(v, 0.0) + log1p(jnp.exp(-jnp.abs(v)))


def picks(first_lane):
    rows = lax.broadcasted_iota(jnp.int32, (8, 128), 0)
    lanes = lax.broadcasted_iota(jnp.int32, (8, 128), 1)
    return jnp.where(jnp.logical_and(lanes == rows + first_lane, rows < 3), 1.0, 0.0).astype(BF16)


def load_kernel(
    group, member, bc_0, bc_1, x_0, x_1, x_2, x_3, bw, dt, xw, xb, bb, bias, a_log, skip,
    last, first, x_out, bc_out, dt_out, x_taps, bc_taps, own_taps, per_head,
):
    channels = x_out.shape[0]
    heads = dt.shape[0]
    begin, finish = picks(0), picks(125)
    series = jnp.concatenate([x_0[...], x_1[...], x_2[...], x_3[...]], axis=0)
    mine = jnp.concatenate([bc_0[0], bc_1[0]], axis=0)
    last[:, :channels] = dot(finish, series[:, 128:], 1, 1).astype(BF16)
    last[:, channels:] = dot(finish, mine[:, 128:], 1, 1).astype(BF16)
    first[:, :channels] = dot(begin, series[:, :128], 1, 1).astype(BF16)
    first[:, channels:] = dot(begin, mine[:, :128], 1, 1).astype(BF16)
    x_out[...] = series
    bc_out[...] = mine
    dt_out[...] = dt[...]
    x_taps[:4, :] = xw[...]
    x_taps[4:, :] = jnp.broadcast_to(xb[...], (4, channels))
    own = jnp.zeros(own_taps.shape[1:], F32)
    for q in range(LO):
        own = jnp.where(member[0] == q, x_taps[:, q * 128 : (q + 1) * 128], own)
    own_taps[0] = own
    bc_taps[:4, :] = bw[0]
    bc_taps[4:, :] = jnp.broadcast_to(chosen(bb[...], group[0]), (4, mine.shape[0]))
    own_taps[1] = bc_taps[:, :128]
    for i, row in enumerate((bias, a_log, skip)):
        per_head[i] = jnp.broadcast_to(column(row[...]), (heads, 128))


def filtered(series, taps):
    lanes = lax.broadcasted_iota(jnp.int32, (series.shape[0], 128), 1)
    first, second = series[:, :128].astype(F32), series[:, 128:].astype(F32)
    wide = [taps[:, k * 128 : (k + 1) * 128] for k in range(5)]
    a = wide[4] + wide[3] * first
    b = wide[4] + wide[3] * second
    for back in (1, 2, 3):
        moved = pltpu.roll(first, back, 1)
        a = a + wide[3 - back] * moved
        b = b + wide[3 - back] * jnp.where(lanes < back, moved, pltpu.roll(second, back, 1))
    return jnp.concatenate([silu(a), silu(b)], axis=1)


def thirds(value):
    high = value.astype(BF16).astype(F32)
    mid = (value - high).astype(BF16).astype(F32)
    return jnp.concatenate([high, mid, value - high - mid], axis=0).astype(BF16)


def column(row):
    size = row.shape[1]
    same = lax.broadcasted_iota(jnp.int32, (size, size), 0) == lax.broadcasted_iota(jnp.int32, (size, size), 1)
    return jnp.sum(jnp.where(same, row, 0.0), axis=1, keepdims=True)


def chosen(table, group):
    rows = lax.broadcasted_iota(jnp.int32, table.shape, 0)
    return jnp.sum(jnp.where(rows == group, table, 0.0), axis=0, keepdims=True)


def split(value):
    high = value.astype(BF16)
    return high, (value - high.astype(F32)).astype(BF16)


def state_kernel(
    z, x, bc, dt, x_taps, bc_taps, per_head, last, first, pay, xc, bcc, cum_out, less_out, z_out, done, weighted, cols
):
    fetch = pltpu.make_async_copy(z, z_out, done)
    fetch.start()
    channels = x.shape[0]
    heads = dt.shape[0]
    width = channels // heads
    states = bc.shape[0] // 2

    delta = softplus(dt[...].astype(F32) + per_head[0][:, :1])
    scaled = delta * -jnp.exp(per_head[1][:, :1])
    size = scaled.shape[1]
    upto = jnp.where(
        lax.broadcasted_iota(jnp.int32, (size, size), 0) <= lax.broadcasted_iota(jnp.int32, (size, size), 1), 1.0, 0.0
    ).astype(BF16)
    sums = dot(thirds(scaled), upto, 1, 0)
    cum = sums[2 * heads :] + sums[heads : 2 * heads] + sums[:heads]
    cum_out[...] = cum
    less_out[...] = cum - jnp.log(delta)
    end = cum[:, size - 1 :]
    gain = delta * jnp.exp(end - cum)
    total_high, total_low = split(jnp.exp(end))
    total_high, total_low = total_high.astype(F32), total_low.astype(F32)

    opening = gain[:, :128].T[:8]
    gains = jnp.concatenate([jnp.broadcast_to(opening[:, h : h + 1], (8, width)) for h in range(heads)], axis=1)
    gain_high = gains.astype(BF16).astype(F32)
    lines = lax.broadcasted_iota(jnp.int32, (8, channels), 0)
    gains = jnp.where(lines < 4, gain_high, pltpu.roll(gains - gain_high, 4, 0))
    lines = lax.broadcasted_iota(jnp.int32, last.shape, 0)
    edges = jnp.where(lines < 3, last[...].astype(F32), pltpu.roll(first[...].astype(F32), 3, 0))

    kinds = lax.broadcasted_iota(jnp.int32, (24, 5 * 128), 1) // 128
    picked = jnp.where(lax.broadcasted_iota(jnp.int32, (24, 5 * 128), 0) % 8 == kinds, 1.0, 0.0).astype(BF16)
    cols[...] = dot(thirds(jnp.concatenate([x_taps[...], bc_taps[...]], axis=1)), picked, 0, 0)
    for start in range(0, 2 * states, width):
        at = pl.ds(start, width)
        bcc[at, :] = filtered(bc[at, :], cols[pl.ds(channels + start, width), :]).astype(BF16)
    late = jnp.where(lax.broadcasted_iota(jnp.int32, gain.shape, 1) < 3, 0.0, gain)
    lines = lax.broadcasted_iota(jnp.int32, (8, 128), 0)
    per = heads // LO
    for quarter in range(LO):
        tail = jnp.zeros((8, 128), F32)
        for j in range(per):
            h = quarter * per + j
            at = pl.ds(h * width, width)
            values = filtered(x[at, :], cols[at, :])
            xc[at, :] = values.astype(BF16)
            weighted[at, :] = (values * late[h : h + 1]).astype(BF16)
            tail = jnp.where(lines == 2 * j, total_high[h : h + 1], tail)
            tail = jnp.where(lines == 2 * j + 1, total_low[h : h + 1], tail)
        here = slice(quarter * 128, (quarter + 1) * 128)
        rows = jnp.concatenate([tail, edges[:, here], edges[:, channels : channels + 128], gains[:, here]], axis=0)
        pay[quarter, pl.ds(per * width, META), :] = rows.astype(BF16)
    fresh = dot(weighted[...], bcc[:states, :], 1, 1).astype(BF16)
    for quarter in range(LO):
        size = per * width
        pay[quarter, pl.ds(0, size), :] = fresh[quarter * size : (quarter + 1) * size]
    fetch.wait()


def early(series, taps):
    rows = lax.broadcasted_iota(jnp.int32, series.shape, 0)
    total = taps[4:5] + taps[0:1] * series
    for k in (1, 2, 3):
        total = total + taps[k : k + 1] * pltpu.roll(series, 8 - k, 0)
    return jnp.where(rows < 3, silu(total), 0.0).astype(BF16)


def rim_state(before, after, taps):
    rows = lax.broadcasted_iota(jnp.int32, (8, 128), 0)
    x_rows = early(jnp.where(rows < 3, before[8:16], after[8:16]), taps[0])
    b_rows = early(jnp.where(rows < 3, before[16:24], after[16:24]), taps[1])
    gains = after[24:32] + pltpu.roll(after[24:32], 4, 0)
    return dot((x_rows.astype(F32) * gains).astype(BF16), b_rows, 0, 0)


def spread_rows(rows, start, per, size):
    width = size // per
    values = [rows[start + 2 * j : start + 2 * j + 1] + rows[start + 2 * j + 1 : start + 2 * j + 2] for j in range(per)]
    return jnp.concatenate([jnp.broadcast_to(v, (width, 128)) for v in values], axis=0)


def unpack(block):
    size = block.shape[0] - META
    return block[:size].astype(F32), block[size:].astype(F32)


def packed_rows(decay, start, rows, per):
    width = decay.shape[0] // per
    lines = lax.broadcasted_iota(jnp.int32, (8, 128), 0)
    for j in range(per):
        d = decay[j * width : j * width + 1]
        high = d.astype(BF16).astype(F32)
        rows = jnp.where(lines == start + 2 * j, high, rows)
        rows = jnp.where(lines == start + 2 * j + 1, d - high, rows)
    return rows


def group_kernel(got, taps, kept, meta, *refs, per, opening):
    blank_kernel(*refs[1:])
    size = kept.shape[1]
    members = [unpack(got[r]) for r in range(LO)]
    lines = lax.broadcasted_iota(jnp.int32, (META, 128), 0)
    state, rows = members[0]
    if opening:
        state = state + rim_state(jnp.zeros_like(rows), rows, taps)
    kept[0] = state
    decay = spread_rows(rows, 0, per, size)
    suffix = jnp.ones_like(decay)
    for r in range(1, LO):
        fresh, now = members[r]
        fresh = fresh + rim_state(members[r - 1][1], now, taps)
        kept[r] = fresh
        d = spread_rows(now, 0, per, size)
        state = fresh + d * state
        decay, suffix = decay * d, suffix * d
    meta[...] = got[:, size:, :]
    if not refs:
        return
    out = refs[0]
    out[:size, :] = state.astype(BF16)
    head = packed_rows(suffix, 4, packed_rows(decay, 0, jnp.zeros((8, 128), F32), per), per)
    edge = lax.broadcasted_iota(jnp.int32, (16, 128), 0) % 8 < 3
    edges = jnp.where(edge, members[LO - 1][1][8:24], rows[8:24])
    out[size:, :] = jnp.concatenate([head, edges, rows[24:32]], axis=0).astype(BF16)


def join_kernel(earlier, later, taps, out, *, per):
    size = out.shape[0] - META
    before, rows_before = unpack(earlier[...])
    after, rows = unpack(later[...])
    opening = rim_state(rows_before, rows, taps)
    state = after + spread_rows(rows, 4, per, size) * opening + spread_rows(rows, 0, per, size) * before
    out[:size, :] = state.astype(BF16)
    out[size:, :] = later[size:, :]


def entering_kernel(kept, meta, *refs, per, blanks):
    blank_kernel(*refs[len(refs) - blanks :])
    *given, out = refs[: len(refs) - blanks]
    size = kept.shape[1]
    own = meta[0].astype(F32)
    fresh = kept[0]
    state = jnp.zeros(out.shape[1:], F32)
    if len(given) == 2:
        taps, near = given
        state, rows = unpack(near[...])
        fresh = fresh + rim_state(rows, own, taps)
    elif given:
        taps, next_one, over, between = given
        next_one, rows_next = unpack(next_one[...])
        (over, rows_over), (between, rows) = unpack(over[...]), unpack(between[...])
        opening = rim_state(rows_over, rows, taps)
        state = between + spread_rows(rows, 4, per, size) * opening + spread_rows(rows, 0, per, size) * over
        state = state + next_one
        fresh = fresh + rim_state(rows_next + rows, own, taps)
    out[0] = state.astype(BF16)
    for r in range(1, LO):
        state = fresh + spread_rows(meta[r - 1].astype(F32), 0, per, size) * state
        out[r] = state.astype(BF16)
        fresh = kept[r]


def copy_kernel(*refs):
    half = len(refs) // 2
    for source, target in zip(refs[:half], refs[half:]):
        target[...] = source[...]


def pack_kernel(kept, begin, meta, joined, near, kept_out, rows):
    kept_out[...] = kept[...] + begin[...].astype(F32)
    at = 0
    for r in range(LO):
        rows[at : at + META, :] = meta[r]
        at += META
    for block in (joined, near):
        rows[at : at + block.shape[0], :] = block[...]
        at += block.shape[0]


def unpack_kernel(rows, meta, joined, near):
    at = 0
    for r in range(LO):
        meta[r] = rows[at : at + META, :]
        at += META
    for block in (joined, near):
        block[...] = rows[at : at + block.shape[0], :]
        at += block.shape[0]


def begin_kernel(kept, unused, state, *blanks):
    state[...] = kept[...].astype(BF16)
    blank_kernel(*blanks)


def blank_kernel(*refs):
    for ref in refs:
        ref[...] = jnp.zeros(ref.shape, ref.dtype)


def intra_kernel(xc, bcc, cum_in, less_in, per_head, out):
    heads = cum_in.shape[0]
    width = xc.shape[0] // heads
    states = bcc.shape[0] // 2
    cum, less = cum_in[...], less_in[...]
    less_cols = jnp.concatenate([less[:, :128].T, less[:, 128:].T], axis=0)
    skips = per_head[2][:, :1]
    gram = dot(bcc[:states, :], bcc[states:, :], 0, 0)
    gram = jnp.where(lax.broadcasted_iota(jnp.int32, gram.shape, 0) < 3, 0.0, gram)
    keep = lax.broadcasted_iota(jnp.int32, (128, 128), 0) <= lax.broadcasted_iota(jnp.int32, (128, 128), 1)
    lanes = lax.broadcasted_iota(jnp.int32, (width, 256), 1)
    for h in range(heads):
        at = pl.ds(h * width, width)
        values = xc[at, :]
        row = cum[h : h + 1]
        col = less_cols[:, h : h + 1]

        def mix(s, t, masked):
            spread = row[:, t : t + 128] - col[s : s + 128]
            if masked:
                spread = jnp.where(keep, spread, -1e30)
            return (gram[s : s + 128, t : t + 128] * jnp.exp(spread)).astype(BF16)

        near = dot(values[:, :128], mix(0, 0, True), 1, 0)
        late = dot(values, jnp.concatenate([mix(0, 128, False), mix(128, 128, True)], axis=0), 1, 0)
        kept = jnp.where(lanes < 3, 0.0, values.astype(F32))
        out[at, :] = jnp.concatenate([near, late], axis=1) + skips[h : h + 1] * kept


def output_kernel(
    low, high, bcc, rims_low, rims_mid, rims_high, first, x_taps, bc_taps, cum_in, less, per_head, state, z, out, held, done
):
    heads = cum_in.shape[0]
    channels = low.shape[0]
    width = channels // heads
    states = state.shape[1]
    per = heads // LO
    lines = lax.broadcasted_iota(jnp.int32, first.shape, 0)
    given = rims_low[...].astype(F32) + rims_mid[...].astype(F32) + rims_high[...].astype(F32)
    edges = jnp.where(lines < 3, given, pltpu.roll(first[...].astype(F32), 3, 0))
    x_rows = early(edges[:, :channels], x_taps[...])
    bc_rows = early(edges[:, channels:], bc_taps[...])
    x_placed = dot(x_rows, picks(0), 0, 0)
    c_placed = dot(bc_rows[:, states:], picks(0), 0, 0).astype(BF16)
    lanes = lax.broadcasted_iota(jnp.int32, c_placed.shape, 1)
    c_rows = bcc[states:, :]
    c_rows = jnp.concatenate([jnp.where(lanes < 3, c_placed, c_rows[:, :128]), c_rows[:, 128:]], axis=1)
    gram = dot(bc_rows[:, :states], c_rows, 1, 0)
    cum = cum_in[...]
    grown = jnp.exp(cum)
    less_cols = less[:, :128].T[:8]
    keep = lax.broadcasted_iota(jnp.int32, gram.shape, 0) <= lax.broadcasted_iota(jnp.int32, gram.shape, 1)
    skips = per_head[2][:, :1]
    copies = []
    for h in range(heads):
        at = pl.ds(h * width, width)
        spread = jnp.where(keep, cum[h : h + 1] - less_cols[:, h : h + 1], -1e30)
        mixing = (gram * jnp.exp(spread)).astype(BF16)
        opening = dot(x_rows[:, h * width : (h + 1) * width], mixing, 0, 0)
        skipped = skips[h : h + 1] * x_placed[h * width : (h + 1) * width]
        y = low[at, :] + high[at, :] + opening + grown[h : h + 1] * dot(state[at, :], c_rows, 1, 0)
        y = jnp.concatenate([y[:, :128] + skipped, y[:, 128:]], axis=1)
        y = y.astype(BF16).astype(F32)
        held[at, :] = (y * silu(z[at, :].astype(F32))).astype(BF16)
        if h % per == per - 1:
            part = pl.ds((h + 1 - per) * width, per * width)
            copies.append(pltpu.make_async_copy(held.at[part], out.at[part], done.at[h // per]))
            copies[-1].start()
    for copy in copies:
        copy.wait()


def shape(*dims, dtype=F32):
    return pltpu.VMEM(dims, dtype)


VMEM = pl.BlockSpec(memory_space=pltpu.VMEM)
GRANT = pltpu.CompilerParams(vmem_limit_bytes=12 << 20)


def run(kernel, outs, *args):
    args = [pltpu.with_memory_space_constraint(a, pltpu.VMEM) for a in args]
    return pl.pallas_call(
        kernel, out_shape=outs, in_specs=[VMEM] * len(args), out_specs=[VMEM] * len(outs), compiler_params=GRANT
    )(*args)


def local(x_in, z_gate, bc_in, dt_raw, conv_x_w, conv_x_b, conv_bc_w, conv_bc_b, dt_bias, a_log, d_skip):
    heads, length = dt_raw.shape
    channels = x_in.shape[0]
    rows = bc_in.shape[1]
    states = rows // 2
    per = heads // LO
    quarter = channels // LO
    group = (lax.axis_index("tensor") // (GROUP_HEADS // heads)).astype(jnp.int32).reshape(1)
    member = lax.axis_index("near").astype(jnp.int32).reshape(1)
    far = lax.axis_index("far")
    cp = ("far", "near")
    count = lax.axis_size(cp)

    strip = shape(8, channels + rows, dtype=BF16)
    block_shape = shape(quarter + META, states, dtype=BF16)
    kept_shapes = [shape(LO, quarter, states), shape(LO, META, states, dtype=BF16)]
    state_shape = shape(LO, quarter, states, dtype=BF16)
    series = shape(channels, length, dtype=BF16)
    pairs = shape(rows, length, dtype=BF16)
    taps = jnp.swapaxes(conv_bc_w, 1, 2)
    small = [dt_raw, conv_x_w.T, conv_x_b[None], conv_bc_b, dt_bias[None], a_log[None], d_skip[None]]
    outs = [strip, strip, series, pairs, shape(heads, length, dtype=BF16), shape(8, channels), shape(8, rows)]
    outs += [shape(2, 8, 128), shape(3, heads, 128)]
    last, first, x, bc, dt, x_taps, bc_taps, own_taps, per_head = pl.pallas_call(
        load_kernel,
        grid_spec=pltpu.PrefetchScalarGridSpec(
            num_scalar_prefetch=2,
            grid=(1,),
            in_specs=[pl.BlockSpec((1, states, length), lambda i, g, m, p=p: (g[0], p, 0)) for p in range(2)]
            + [pl.BlockSpec((quarter, length), lambda i, g, m, p=p: (p, 0)) for p in range(LO)]
            + [pl.BlockSpec((1,) + taps.shape[1:], lambda i, g, m: (g[0], 0, 0))]
            + [pl.BlockSpec(a.shape, lambda i, g, m: (0, 0)) for a in small],
            out_specs=[VMEM] * len(outs),
        ),
        out_shape=outs,
        name="load",
        compiler_params=GRANT,
    )(group, member, *[pltpu.with_memory_space_constraint(a, pltpu.HBM) for a in (bc_in, bc_in, *[x_in] * LO, taps, *small)])
    outs = [shape(LO, quarter + META, states, dtype=BF16), series, pairs]
    outs += [shape(heads, length), shape(heads, length), series]
    args = [x, bc, dt, x_taps, bc_taps, per_head, last, first]
    pay, xc, bcc, cum, less, z = pl.pallas_call(
        state_kernel,
        out_shape=outs,
        in_specs=[pl.BlockSpec(memory_space=pl.ANY)] + [VMEM] * len(args),
        out_specs=[VMEM] * len(outs),
        scratch_shapes=[
            pltpu.SemaphoreType.DMA,
            pltpu.VMEM((channels, length), BF16),
            pltpu.VMEM((channels + rows, 5 * 128), F32),
        ],
        name="states",
        compiler_params=GRANT,
    )(
        pltpu.with_memory_space_constraint(z_gate, pltpu.HBM),
        *[pltpu.with_memory_space_constraint(a, pltpu.VMEM) for a in args],
    )

    def gather(*rest, opening=False):
        got = lax.all_to_all(pay, "near", 0, 0, tiled=True)
        kernel = lambda *refs: group_kernel(*refs, per=per, opening=opening)
        return tuple(run(kernel, [*kept_shapes, *rest], got, own_taps))

    def blank(*outs):
        return tuple(run(blank_kernel, list(outs)))

    def exchange(*given, blanks=()):
        kernel = lambda *refs: entering_kernel(*refs, per=per, blanks=len(blanks))
        entering, *rest = run(kernel, [state_shape, *blanks], *given)
        return tuple(rest) + (lax.all_to_all(entering, "near", 0, 0, tiled=True),)

    def sent(block, source, target):
        route = [(source * LO + i, target * LO + i) for i in range(LO)]
        return lax.ppermute(block, cp, route)

    def kept_on(*arrays):
        return tuple(run(copy_kernel, [shape(*a.shape, dtype=a.dtype) for a in arrays], *arrays))

    def inside(after):
        _, values = lax.optimization_barrier((after, xc))
        return run(intra_kernel, [inner_shape], values, bcc, cum, less, per_head)[0]

    def shifted(begin, end):
        return lax.ppermute(kept_on(last)[0], cp, [(i, i + 1) for i in range(begin, end)])

    inner_shape = shape(channels, length)

    packed_rows_count = LO * META + 2 * (quarter + META)
    packed_shapes = [kept_shapes[0], shape(packed_rows_count, states, dtype=BF16)]

    def low_part():
        kept = lax.cond(
            far == 0, lambda: gather(block_shape, opening=True), lambda: blank(*kept_shapes, block_shape)
        )
        near = sent(kept[2], 0, 1)
        rims = shifted(0, 2 * LO - 1)
        *kept, begin = lax.cond(
            far == 0,
            lambda *kept: exchange(*kept[:2], blanks=(*kept_shapes, block_shape)),
            lambda *kept: gather(block_shape, state_shape),
            *kept,
        )
        inner = inside(begin)
        packed = run(pack_kernel, packed_shapes, kept[0], begin, kept[1], kept[2], near)
        return (*packed, *kept_on(rims), inner)

    def high_part(*kept):
        rims = shifted(2 * LO, count - 1)
        kept = lax.cond(far == 2, lambda *kept: gather(block_shape), lambda *kept: blank(*kept_shapes, block_shape), *kept)
        between = sent(kept[2], 2, 3)
        kept = lax.cond(far == 3, lambda *kept: gather(), kept_on, *kept[:2])
        inner = inside(kept[0])
        return kept_on(*kept, between, rims) + (inner,) + blank(state_shape)

    def later_part(kept, packed):
        meta, block, near = run(unpack_kernel, [kept_shapes[1], block_shape, block_shape], packed)
        (joined,) = run(lambda *refs: join_kernel(*refs, per=per), [block_shape], near, block, own_taps)
        over = sent(joined, 1, 3)
        next_one = sent(joined, 1, 2)
        rims_mid = shifted(2 * LO - 1, 2 * LO)
        *kept, between, rims, inner, state = lax.cond(
            far >= 2,
            high_part,
            lambda *kept: exchange(*kept, own_taps, near, blanks=(*kept_shapes, block_shape, strip, inner_shape)),
            kept,
            meta,
        )
        (state,) = lax.cond(
            far >= 2,
            lambda state, *given: exchange(*given),
            lambda state, *given: kept_on(state),
            state,
            *kept,
            own_taps,
            next_one,
            over,
            between,
        )
        return (state, inner, rims_mid, rims)

    kept, packed, rims_low, inner_low = lax.cond(far < 2, low_part, lambda: blank(*packed_shapes, strip, inner_shape))
    state, inner, rims_mid, rims = lax.cond(
        far == 0,
        lambda kept, packed: tuple(run(begin_kernel, [state_shape, inner_shape, strip, strip], kept, packed)),
        later_part,
        kept,
        packed,
    )
    inputs = [inner_low, inner, bcc, rims_low, rims_mid, rims, first, x_taps, bc_taps, cum, less, per_head]
    inputs += [state.reshape(channels, states), z]
    return pl.pallas_call(
        output_kernel,
        out_shape=jax.ShapeDtypeStruct((channels, length), BF16),
        in_specs=[VMEM] * len(inputs),
        out_specs=pl.BlockSpec(memory_space=pl.ANY),
        scratch_shapes=[pltpu.VMEM((channels, length), BF16), pltpu.SemaphoreType.DMA((LO,))],
        name="gated",
    compiler_params=GRANT,
    )(*[pltpu.with_memory_space_constraint(a, pltpu.VMEM) for a in inputs])


def solution(mesh):
    dp, cp, tensor = mesh.devices.shape
    finer = Mesh(mesh.devices.reshape(dp, cp // LO, LO, tensor), ("dp", "far", "near", "tensor"))
    along = ("dp", "far", "near")
    return jax.shard_map(
        local,
        mesh=finer,
        in_specs=(
            P("tensor", along),
            P("tensor", along),
            P(None, None, along),
            P("tensor", along),
            P("tensor", None),
            P("tensor"),
            P(),
            P(),
            P("tensor"),
            P("tensor"),
            P("tensor"),
        ),
        out_specs=P("tensor", along),
        check_vma=False,
    )
```

```python
import jax
import jax.numpy as jnp
from jax import lax
from jax.experimental import pallas as pl
from jax.experimental.pallas import tpu as pltpu
from jax.sharding import Mesh, PartitionSpec as P


HEADS = 128
GROUPS = 8
GROUP_HEADS = HEADS // GROUPS
LO = 4
META = 32

F32 = jnp.float32
BF16 = jnp.bfloat16


def dot(a, b, ca, cb):
    return lax.dot_general(a, b, (((ca,), (cb,)), ((), ())), preferred_element_type=F32)


def silu(v):
    half = 0.5 * v
    return half + half * jnp.tanh(half)


def log1p(u):
    return jnp.where(u < 1e-3, u * (1.0 - u * (0.5 - u * (1.0 / 3.0))), jnp.log(1.0 + u))


def softplus(v):
    return jnp.maximum(v, 0.0) + log1p(jnp.exp(-jnp.abs(v)))


def picks(first_lane):
    rows = lax.broadcasted_iota(jnp.int32, (8, 128), 0)
    lanes = lax.broadcasted_iota(jnp.int32, (8, 128), 1)
    return jnp.where(jnp.logical_and(lanes == rows + first_lane, rows < 3), 1.0, 0.0).astype(BF16)


def load_kernel(
    group, member, bc_0, bc_1, x_0, x_1, x_2, x_3, bw, dt, xw, xb, bb, bias, a_log, skip,
    last, first, x_out, bc_out, dt_out, x_taps, bc_taps, own_taps, per_head,
):
    channels = x_out.shape[0]
    heads = dt.shape[0]
    begin, finish = picks(0), picks(125)
    series = jnp.concatenate([x_0[...], x_1[...], x_2[...], x_3[...]], axis=0)
    mine = jnp.concatenate([bc_0[0], bc_1[0]], axis=0)
    last[:, :channels] = dot(finish, series[:, 128:], 1, 1).astype(BF16)
    last[:, channels:] = dot(finish, mine[:, 128:], 1, 1).astype(BF16)
    first[:, :channels] = dot(begin, series[:, :128], 1, 1).astype(BF16)
    first[:, channels:] = dot(begin, mine[:, :128], 1, 1).astype(BF16)
    x_out[...] = series
    bc_out[...] = mine
    dt_out[...] = dt[...]
    x_taps[:4, :] = xw[...]
    x_taps[4:, :] = jnp.broadcast_to(xb[...], (4, channels))
    own = jnp.zeros(own_taps.shape[1:], F32)
    for q in range(LO):
        own = jnp.where(member[0] == q, x_taps[:, q * 128 : (q + 1) * 128], own)
    own_taps[0] = own
    bc_taps[:4, :] = bw[0]
    bc_taps[4:, :] = jnp.broadcast_to(chosen(bb[...], group[0]), (4, mine.shape[0]))
    own_taps[1] = bc_taps[:, :128]
    for i, row in enumerate((bias, a_log, skip)):
        per_head[i] = jnp.broadcast_to(column(row[...]), (heads, 128))


def filtered(series, taps):
    lanes = lax.broadcasted_iota(jnp.int32, (series.shape[0], 128), 1)
    first, second = series[:, :128].astype(F32), series[:, 128:].astype(F32)
    wide = [taps[:, k * 128 : (k + 1) * 128] for k in range(5)]
    a = wide[4] + wide[3] * first
    b = wide[4] + wide[3] * second
    for back in (1, 2, 3):
        moved = pltpu.roll(first, back, 1)
        a = a + wide[3 - back] * moved
        b = b + wide[3 - back] * jnp.where(lanes < back, moved, pltpu.roll(second, back, 1))
    return jnp.concatenate([silu(a), silu(b)], axis=1)


def thirds(value):
    high = value.astype(BF16).astype(F32)
    mid = (value - high).astype(BF16).astype(F32)
    return jnp.concatenate([high, mid, value - high - mid], axis=0).astype(BF16)


def column(row):
    size = row.shape[1]
    same = lax.broadcasted_iota(jnp.int32, (size, size), 0) == lax.broadcasted_iota(jnp.int32, (size, size), 1)
    return jnp.sum(jnp.where(same, row, 0.0), axis=1, keepdims=True)


def chosen(table, group):
    rows = lax.broadcasted_iota(jnp.int32, table.shape, 0)
    return jnp.sum(jnp.where(rows == group, table, 0.0), axis=0, keepdims=True)


def split(value):
    high = value.astype(BF16)
    return high, (value - high.astype(F32)).astype(BF16)


def state_kernel(
    z, x, bc, dt, x_taps, bc_taps, per_head, last, first, pay, xc, bcc, cum_out, less_out, z_out, done, weighted, cols
):
    fetch = pltpu.make_async_copy(z, z_out, done)
    fetch.start()
    channels = x.shape[0]
    heads = dt.shape[0]
    width = channels // heads
    states = bc.shape[0] // 2

    delta = softplus(dt[...].astype(F32) + per_head[0][:, :1])
    scaled = delta * -jnp.exp(per_head[1][:, :1])
    size = scaled.shape[1]
    upto = jnp.where(
        lax.broadcasted_iota(jnp.int32, (size, size), 0) <= lax.broadcasted_iota(jnp.int32, (size, size), 1), 1.0, 0.0
    ).astype(BF16)
    sums = dot(thirds(scaled), upto, 1, 0)
    cum = sums[2 * heads :] + sums[heads : 2 * heads] + sums[:heads]
    cum_out[...] = cum
    less_out[...] = cum - jnp.log(delta)
    end = cum[:, size - 1 :]
    gain = delta * jnp.exp(end - cum)
    total_high, total_low = split(jnp.exp(end))
    total_high, total_low = total_high.astype(F32), total_low.astype(F32)

    opening = gain[:, :128].T[:8]
    gains = jnp.concatenate([jnp.broadcast_to(opening[:, h : h + 1], (8, width)) for h in range(heads)], axis=1)
    gain_high = gains.astype(BF16).astype(F32)
    lines = lax.broadcasted_iota(jnp.int32, (8, channels), 0)
    gains = jnp.where(lines < 4, gain_high, pltpu.roll(gains - gain_high, 4, 0))
    lines = lax.broadcasted_iota(jnp.int32, last.shape, 0)
    edges = jnp.where(lines < 3, last[...].astype(F32), pltpu.roll(first[...].astype(F32), 3, 0))

    kinds = lax.broadcasted_iota(jnp.int32, (24, 5 * 128), 1) // 128
    picked = jnp.where(lax.broadcasted_iota(jnp.int32, (24, 5 * 128), 0) % 8 == kinds, 1.0, 0.0).astype(BF16)
    cols[...] = dot(thirds(jnp.concatenate([x_taps[...], bc_taps[...]], axis=1)), picked, 0, 0)
    for start in range(0, 2 * states, width):
        at = pl.ds(start, width)
        bcc[at, :] = filtered(bc[at, :], cols[pl.ds(channels + start, width), :]).astype(BF16)
    late = jnp.where(lax.broadcasted_iota(jnp.int32, gain.shape, 1) < 3, 0.0, gain)
    lines = lax.broadcasted_iota(jnp.int32, (8, 128), 0)
    per = heads // LO
    for quarter in range(LO):
        tail = jnp.zeros((8, 128), F32)
        for j in range(per):
            h = quarter * per + j
            at = pl.ds(h * width, width)
            values = filtered(x[at, :], cols[at, :])
            xc[at, :] = values.astype(BF16)
            weighted[at, :] = (values * late[h : h + 1]).astype(BF16)
            tail = jnp.where(lines == 2 * j, total_high[h : h + 1], tail)
            tail = jnp.where(lines == 2 * j + 1, total_low[h : h + 1], tail)
        here = slice(quarter * 128, (quarter + 1) * 128)
        rows = jnp.concatenate([tail, edges[:, here], edges[:, channels : channels + 128], gains[:, here]], axis=0)
        pay[quarter, pl.ds(per * width, META), :] = rows.astype(BF16)
    fresh = dot(weighted[...], bcc[:states, :], 1, 1).astype(BF16)
    for quarter in range(LO):
        size = per * width
        pay[quarter, pl.ds(0, size), :] = fresh[quarter * size : (quarter + 1) * size]
    fetch.wait()


def early(series, taps):
    rows = lax.broadcasted_iota(jnp.int32, series.shape, 0)
    total = taps[4:5] + taps[0:1] * series
    for k in (1, 2, 3):
        total = total + taps[k : k + 1] * pltpu.roll(series, 8 - k, 0)
    return jnp.where(rows < 3, silu(total), 0.0).astype(BF16)


def rim_state(before, after, taps):
    rows = lax.broadcasted_iota(jnp.int32, (8, 128), 0)
    x_rows = early(jnp.where(rows < 3, before[8:16], after[8:16]), taps[0])
    b_rows = early(jnp.where(rows < 3, before[16:24], after[16:24]), taps[1])
    gains = after[24:32] + pltpu.roll(after[24:32], 4, 0)
    return dot((x_rows.astype(F32) * gains).astype(BF16), b_rows, 0, 0)


def spread_rows(rows, start, per, size):
    width = size // per
    values = [rows[start + 2 * j : start + 2 * j + 1] + rows[start + 2 * j + 1 : start + 2 * j + 2] for j in range(per)]
    return jnp.concatenate([jnp.broadcast_to(v, (width, 128)) for v in values], axis=0)


def unpack(block):
    size = block.shape[0] - META
    return block[:size].astype(F32), block[size:].astype(F32)


def packed_rows(decay, start, rows, per):
    width = decay.shape[0] // per
    lines = lax.broadcasted_iota(jnp.int32, (8, 128), 0)
    for j in range(per):
        d = decay[j * width : j * width + 1]
        high = d.astype(BF16).astype(F32)
        rows = jnp.where(lines == start + 2 * j, high, rows)
        rows = jnp.where(lines == start + 2 * j + 1, d - high, rows)
    return rows


def group_kernel(got, taps, kept, meta, *refs, per, opening):
    blank_kernel(*refs[1:])
    size = kept.shape[1]
    members = [unpack(got[r]) for r in range(LO)]
    lines = lax.broadcasted_iota(jnp.int32, (META, 128), 0)
    state, rows = members[0]
    if opening:
        state = state + rim_state(jnp.zeros_like(rows), rows, taps)
    kept[0] = state
    decay = spread_rows(rows, 0, per, size)
    suffix = jnp.ones_like(decay)
    for r in range(1, LO):
        fresh, now = members[r]
        fresh = fresh + rim_state(members[r - 1][1], now, taps)
        kept[r] = fresh
        d = spread_rows(now, 0, per, size)
        state = fresh + d * state
        decay, suffix = decay * d, suffix * d
    meta[...] = got[:, size:, :]
    if not refs:
        return
    out = refs[0]
    out[:size, :] = state.astype(BF16)
    head = packed_rows(suffix, 4, packed_rows(decay, 0, jnp.zeros((8, 128), F32), per), per)
    edge = lax.broadcasted_iota(jnp.int32, (16, 128), 0) % 8 < 3
    edges = jnp.where(edge, members[LO - 1][1][8:24], rows[8:24])
    out[size:, :] = jnp.concatenate([head, edges, rows[24:32]], axis=0).astype(BF16)


def join_kernel(earlier, later, taps, out, *, per):
    size = out.shape[0] - META
    before, rows_before = unpack(earlier[...])
    after, rows = unpack(later[...])
    opening = rim_state(rows_before, rows, taps)
    state = after + spread_rows(rows, 4, per, size) * opening + spread_rows(rows, 0, per, size) * before
    out[:size, :] = state.astype(BF16)
    out[size:, :] = later[size:, :]


def entering_kernel(kept, meta, *refs, per, blanks):
    blank_kernel(*refs[len(refs) - blanks :])
    *given, out = refs[: len(refs) - blanks]
    size = kept.shape[1]
    own = meta[0].astype(F32)
    fresh = kept[0]
    state = jnp.zeros(out.shape[1:], F32)
    if len(given) == 2:
        taps, near = given
        state, rows = unpack(near[...])
        fresh = fresh + rim_state(rows, own, taps)
    elif given:
        taps, next_one, over, between = given
        next_one, rows_next = unpack(next_one[...])
        (over, rows_over), (between, rows) = unpack(over[...]), unpack(between[...])
        opening = rim_state(rows_over, rows, taps)
        state = between + spread_rows(rows, 4, per, size) * opening + spread_rows(rows, 0, per, size) * over
        state = state + next_one
        fresh = fresh + rim_state(rows_next + rows, own, taps)
    out[0] = state.astype(BF16)
    for r in range(1, LO):
        state = fresh + spread_rows(meta[r - 1].astype(F32), 0, per, size) * state
        out[r] = state.astype(BF16)
        fresh = kept[r]


def copy_kernel(*refs):
    half = len(refs) // 2
    for source, target in zip(refs[:half], refs[half:]):
        target[...] = source[...]


def pack_kernel(kept, begin, meta, joined, near, kept_out, rows):
    kept_out[...] = kept[...] + begin[...].astype(F32)
    at = 0
    for r in range(LO):
        rows[at : at + META, :] = meta[r]
        at += META
    for block in (joined, near):
        rows[at : at + block.shape[0], :] = block[...]
        at += block.shape[0]


def unpack_kernel(rows, meta, joined, near):
    at = 0
    for r in range(LO):
        meta[r] = rows[at : at + META, :]
        at += META
    for block in (joined, near):
        block[...] = rows[at : at + block.shape[0], :]
        at += block.shape[0]


def begin_kernel(kept, unused, state, *blanks):
    state[...] = kept[...].astype(BF16)
    blank_kernel(*blanks)


def blank_kernel(*refs):
    for ref in refs:
        ref[...] = jnp.zeros(ref.shape, ref.dtype)


def intra_kernel(xc, bcc, cum_in, less_in, per_head, out):
    heads = cum_in.shape[0]
    width = xc.shape[0] // heads
    states = bcc.shape[0] // 2
    cum, less = cum_in[...], less_in[...]
    less_cols = jnp.concatenate([less[:, :128].T, less[:, 128:].T], axis=0)
    skips = per_head[2][:, :1]
    gram = dot(bcc[:states, :], bcc[states:, :], 0, 0)
    gram = jnp.where(lax.broadcasted_iota(jnp.int32, gram.shape, 0) < 3, 0.0, gram)
    keep = lax.broadcasted_iota(jnp.int32, (128, 128), 0) <= lax.broadcasted_iota(jnp.int32, (128, 128), 1)
    lanes = lax.broadcasted_iota(jnp.int32, (width, 256), 1)
    for h in range(heads):
        at = pl.ds(h * width, width)
        values = xc[at, :]
        row = cum[h : h + 1]
        col = less_cols[:, h : h + 1]

        def mix(s, t, masked):
            spread = row[:, t : t + 128] - col[s : s + 128]
            if masked:
                spread = jnp.where(keep, spread, -1e30)
            return (gram[s : s + 128, t : t + 128] * jnp.exp(spread)).astype(BF16)

        near = dot(values[:, :128], mix(0, 0, True), 1, 0)
        late = dot(values, jnp.concatenate([mix(0, 128, False), mix(128, 128, True)], axis=0), 1, 0)
        kept = jnp.where(lanes < 3, 0.0, values.astype(F32))
        out[at, :] = jnp.concatenate([near, late], axis=1) + skips[h : h + 1] * kept


def output_kernel(
    low, high, bcc, rims_low, rims_mid, rims_high, first, x_taps, bc_taps, cum_in, less, per_head, state, z, out, held, done
):
    heads = cum_in.shape[0]
    channels = low.shape[0]
    width = channels // heads
    states = state.shape[1]
    per = heads // LO
    lines = lax.broadcasted_iota(jnp.int32, first.shape, 0)
    given = rims_low[...].astype(F32) + rims_mid[...].astype(F32) + rims_high[...].astype(F32)
    edges = jnp.where(lines < 3, given, pltpu.roll(first[...].astype(F32), 3, 0))
    x_rows = early(edges[:, :channels], x_taps[...])
    bc_rows = early(edges[:, channels:], bc_taps[...])
    x_placed = dot(x_rows, picks(0), 0, 0)
    c_placed = dot(bc_rows[:, states:], picks(0), 0, 0).astype(BF16)
    lanes = lax.broadcasted_iota(jnp.int32, c_placed.shape, 1)
    c_rows = bcc[states:, :]
    c_rows = jnp.concatenate([jnp.where(lanes < 3, c_placed, c_rows[:, :128]), c_rows[:, 128:]], axis=1)
    gram = dot(bc_rows[:, :states], c_rows, 1, 0)
    cum = cum_in[...]
    grown = jnp.exp(cum)
    less_cols = less[:, :128].T[:8]
    keep = lax.broadcasted_iota(jnp.int32, gram.shape, 0) <= lax.broadcasted_iota(jnp.int32, gram.shape, 1)
    skips = per_head[2][:, :1]
    copies = []
    for h in range(heads):
        at = pl.ds(h * width, width)
        spread = jnp.where(keep, cum[h : h + 1] - less_cols[:, h : h + 1], -1e30)
        mixing = (gram * jnp.exp(spread)).astype(BF16)
        opening = dot(x_rows[:, h * width : (h + 1) * width], mixing, 0, 0)
        skipped = skips[h : h + 1] * x_placed[h * width : (h + 1) * width]
        y = low[at, :] + high[at, :] + opening + grown[h : h + 1] * dot(state[at, :], c_rows, 1, 0)
        y = jnp.concatenate([y[:, :128] + skipped, y[:, 128:]], axis=1)
        y = y.astype(BF16).astype(F32)
        held[at, :] = (y * silu(z[at, :].astype(F32))).astype(BF16)
        if h % per == per - 1:
            part = pl.ds((h + 1 - per) * width, per * width)
            copies.append(pltpu.make_async_copy(held.at[part], out.at[part], done.at[h // per]))
            copies[-1].start()
    for copy in copies:
        copy.wait()


def shape(*dims, dtype=F32):
    return pltpu.VMEM(dims, dtype)


VMEM = pl.BlockSpec(memory_space=pltpu.VMEM)
GRANT = pltpu.CompilerParams(vmem_limit_bytes=12 << 20)


def run(kernel, outs, *args):
    args = [pltpu.with_memory_space_constraint(a, pltpu.VMEM) for a in args]
    return pl.pallas_call(
        kernel, out_shape=outs, in_specs=[VMEM] * len(args), out_specs=[VMEM] * len(outs), compiler_params=GRANT
    )(*args)


def local(x_in, z_gate, bc_in, dt_raw, conv_x_w, conv_x_b, conv_bc_w, conv_bc_b, dt_bias, a_log, d_skip):
    heads, length = dt_raw.shape
    channels = x_in.shape[0]
    rows = bc_in.shape[1]
    states = rows // 2
    per = heads // LO
    quarter = channels // LO
    group = (lax.axis_index("tensor") // (GROUP_HEADS // heads)).astype(jnp.int32).reshape(1)
    member = lax.axis_index("near").astype(jnp.int32).reshape(1)
    far = lax.axis_index("far")
    cp = ("far", "near")
    count = lax.axis_size(cp)

    strip = shape(8, channels + rows, dtype=BF16)
    block_shape = shape(quarter + META, states, dtype=BF16)
    kept_shapes = [shape(LO, quarter, states), shape(LO, META, states, dtype=BF16)]
    state_shape = shape(LO, quarter, states, dtype=BF16)
    series = shape(channels, length, dtype=BF16)
    pairs = shape(rows, length, dtype=BF16)
    taps = jnp.swapaxes(conv_bc_w, 1, 2)
    small = [dt_raw, conv_x_w.T, conv_x_b[None], conv_bc_b, dt_bias[None], a_log[None], d_skip[None]]
    outs = [strip, strip, series, pairs, shape(heads, length, dtype=BF16), shape(8, channels), shape(8, rows)]
    outs += [shape(2, 8, 128), shape(3, heads, 128)]
    last, first, x, bc, dt, x_taps, bc_taps, own_taps, per_head = pl.pallas_call(
        load_kernel,
        grid_spec=pltpu.PrefetchScalarGridSpec(
            num_scalar_prefetch=2,
            grid=(1,),
            in_specs=[pl.BlockSpec((1, states, length), lambda i, g, m, p=p: (g[0], p, 0)) for p in range(2)]
            + [pl.BlockSpec((quarter, length), lambda i, g, m, p=p: (p, 0)) for p in range(LO)]
            + [pl.BlockSpec((1,) + taps.shape[1:], lambda i, g, m: (g[0], 0, 0))]
            + [pl.BlockSpec(a.shape, lambda i, g, m: (0, 0)) for a in small],
            out_specs=[VMEM] * len(outs),
        ),
        out_shape=outs,
        name="load",
        compiler_params=GRANT,
    )(group, member, *[pltpu.with_memory_space_constraint(a, pltpu.HBM) for a in (bc_in, bc_in, *[x_in] * LO, taps, *small)])
    outs = [shape(LO, quarter + META, states, dtype=BF16), series, pairs]
    outs += [shape(heads, length), shape(heads, length), series]
    args = [x, bc, dt, x_taps, bc_taps, per_head, last, first]
    pay, xc, bcc, cum, less, z = pl.pallas_call(
        state_kernel,
        out_shape=outs,
        in_specs=[pl.BlockSpec(memory_space=pl.ANY)] + [VMEM] * len(args),
        out_specs=[VMEM] * len(outs),
        scratch_shapes=[
            pltpu.SemaphoreType.DMA,
            pltpu.VMEM((channels, length), BF16),
            pltpu.VMEM((channels + rows, 5 * 128), F32),
        ],
        name="states",
        compiler_params=GRANT,
    )(
        pltpu.with_memory_space_constraint(z_gate, pltpu.HBM),
        *[pltpu.with_memory_space_constraint(a, pltpu.VMEM) for a in args],
    )

    def gather(*rest, opening=False, source=pay):
        got = lax.all_to_all(source, "near", 0, 0, tiled=True)
        kernel = lambda *refs: group_kernel(*refs, per=per, opening=opening)
        return tuple(run(kernel, [*kept_shapes, *rest], got, own_taps))

    def blank(*outs):
        return tuple(run(blank_kernel, list(outs)))

    def exchange(*given, blanks=()):
        kernel = lambda *refs: entering_kernel(*refs, per=per, blanks=len(blanks))
        entering, *rest = run(kernel, [state_shape, *blanks], *given)
        return tuple(rest) + (lax.all_to_all(entering, "near", 0, 0, tiled=True),)

    def sent(block, source, target):
        route = [(source * LO + i, target * LO + i) for i in range(LO)]
        return lax.ppermute(block, cp, route)

    def kept_on(*arrays):
        return tuple(run(copy_kernel, [shape(*a.shape, dtype=a.dtype) for a in arrays], *arrays))

    def inside(after):
        _, values = lax.optimization_barrier((after, xc))
        return run(intra_kernel, [inner_shape], values, bcc, cum, less, per_head)[0]

    def shifted(begin, end):
        return lax.ppermute(kept_on(last)[0], cp, [(i, i + 1) for i in range(begin, end)])

    inner_shape = shape(channels, length)

    packed_rows_count = LO * META + 2 * (quarter + META)
    packed_shapes = [kept_shapes[0], shape(packed_rows_count, states, dtype=BF16)]

    def low_part():
        ahead = jnp.logical_and(far == 0, member[0] > 0)
        (begun,) = lax.cond(ahead, lambda: (inside(less),), lambda: blank(inner_shape))
        ready, begun = lax.optimization_barrier((pay, begun))
        kept = lax.cond(
            far == 0,
            lambda ready: gather(block_shape, opening=True, source=ready),
            lambda ready: blank(*kept_shapes, block_shape),
            ready,
        )
        near = sent(kept[2], 0, 1)
        rims = shifted(0, 2 * LO - 1)
        *kept, begin = lax.cond(
            far == 0,
            lambda *kept: exchange(*kept[:2], blanks=(*kept_shapes, block_shape)),
            lambda *kept: gather(block_shape, state_shape),
            *kept,
        )
        begin, begun = lax.optimization_barrier((begin, begun))
        (inner,) = lax.cond(ahead, lambda begun: kept_on(begun), lambda begun: (inside(less),), begun)
        packed = run(pack_kernel, packed_shapes, kept[0], begin, kept[1], kept[2], near)
        return (*packed, *kept_on(rims, inner))

    def high_part(*kept):
        rims = shifted(2 * LO, count - 1)
        kept = lax.cond(far == 2, lambda *kept: gather(block_shape), lambda *kept: blank(*kept_shapes, block_shape), *kept)
        between = sent(kept[2], 2, 3)
        kept = lax.cond(far == 3, lambda *kept: gather(), kept_on, *kept[:2])
        inner = inside(kept[0])
        return kept_on(*kept, between, rims) + (inner,) + blank(state_shape)

    def later_part(kept, packed):
        meta, block, near = run(unpack_kernel, [kept_shapes[1], block_shape, block_shape], packed)
        (joined,) = run(lambda *refs: join_kernel(*refs, per=per), [block_shape], near, block, own_taps)
        over = sent(joined, 1, 3)
        next_one = sent(joined, 1, 2)
        rims_mid = shifted(2 * LO - 1, 2 * LO)
        *kept, between, rims, inner, state = lax.cond(
            far >= 2,
            high_part,
            lambda *kept: exchange(*kept, own_taps, near, blanks=(*kept_shapes, block_shape, strip, inner_shape)),
            kept,
            meta,
        )
        (state,) = lax.cond(
            far >= 2,
            lambda state, *given: exchange(*given),
            lambda state, *given: kept_on(state),
            state,
            *kept,
            own_taps,
            next_one,
            over,
            between,
        )
        return (state, inner, rims_mid, rims)

    kept, packed, rims_low, inner_low = lax.cond(far < 2, low_part, lambda: blank(*packed_shapes, strip, inner_shape))
    state, inner, rims_mid, rims = lax.cond(
        far == 0,
        lambda kept, packed: tuple(run(begin_kernel, [state_shape, inner_shape, strip, strip], kept, packed)),
        later_part,
        kept,
        packed,
    )
    inputs = [inner_low, inner, bcc, rims_low, rims_mid, rims, first, x_taps, bc_taps, cum, less, per_head]
    inputs += [state.reshape(channels, states), z]
    return pl.pallas_call(
        output_kernel,
        out_shape=jax.ShapeDtypeStruct((channels, length), BF16),
        in_specs=[VMEM] * len(inputs),
        out_specs=pl.BlockSpec(memory_space=pl.ANY),
        scratch_shapes=[pltpu.VMEM((channels, length), BF16), pltpu.SemaphoreType.DMA((LO,))],
        name="gated",
    compiler_params=GRANT,
    )(*[pltpu.with_memory_space_constraint(a, pltpu.VMEM) for a in inputs])


def solution(mesh):
    dp, cp, tensor = mesh.devices.shape
    finer = Mesh(mesh.devices.reshape(dp, cp // LO, LO, tensor), ("dp", "far", "near", "tensor"))
    along = ("dp", "far", "near")
    return jax.shard_map(
        local,
        mesh=finer,
        in_specs=(
            P("tensor", along),
            P("tensor", along),
            P(None, None, along),
            P("tensor", along),
            P("tensor", None),
            P("tensor"),
            P(),
            P(),
            P("tensor"),
            P("tensor"),
            P("tensor"),
        ),
        out_specs=P("tensor", along),
        check_vma=False,
    )
```
